8 devices in a mesh: dp: 1 (over z), lon: 2 (over y), lat: 4 (over x, core).
Axes of the slice: x: 2, y: 2, z: 1, core: 2. Of those that a mesh axis runs over, the one named last changes fastest.
Arguments:
- grid_in: bfloat16 [16, 64, 32, 186], P('dp', 'lat', 'lon')
- mesh_in: bfloat16 [64, 3], P(('lat', 'lon'))
- edge_in: bfloat16 [64, 48, 4], P(('lat', 'lon'))
- senders: int32 [64, 48], P(('lat', 'lon'))
- edge_mask: int32 [64, 48], P(('lat', 'lon'))
- w_grid: bfloat16 [186, 512], replicated
- w_mesh: bfloat16 [3, 512], replicated
- w_edge: bfloat16 [4, 512], replicated
- w_msg: bfloat16 [1536, 512], replicated
- w_node: bfloat16 [1024, 512], replicated
- w_gupd: bfloat16 [512, 512], replicated
- w_out: bfloat16 [6, 512, 512], replicated
- bias_gain: float32 [6, 4, 512], replicated
Outputs:
- output 1: bfloat16 [16, 64, 512], P('dp', ('lat', 'lon'))
- output 2: bfloat16 [16, 64, 32, 512], P('dp', 'lat', 'lon')
All inputs are finite; a program needn't handle non-finite values.
Results may differ from the reference program's by a relative error of at most 0.008706.
Values are sent between devices in bfloat16 or wider.
A program may use at most 1 GiB of HBM per device.

```python
import jax
import jax.numpy as jnp
from jax import lax

BATCH = 16
CIN = 186
LATENT = 512
LAT_CELLS = 4
LON_CELLS = 2
CELL = 16
GRID_PER_MESH = 32
SLOTS = 48
REACH = 3

GRID_ROWS = LAT_CELLS * CELL
GRID_COLS = LON_CELLS * CELL
MESH_CELL = CELL * CELL // GRID_PER_MESH
MESH_NODES = LAT_CELLS * LON_CELLS * MESH_CELL
LN_EPS = 1e-5


def draw_graph(graph_key):
    key_list = jax.random.split(graph_key, 11)
    node_ids = jnp.arange(MESH_NODES)
    cell_ids = node_ids // MESH_CELL
    cell_lat = cell_ids // LON_CELLS
    cell_lon = cell_ids % LON_CELLS
    in_cap = (node_ids % MESH_CELL) < MESH_CELL // 2
    top_cap = in_cap & (cell_lat == 0)
    bottom_cap = in_cap & (cell_lat == LAT_CELLS - 1)
    cap_node = top_cap | bottom_cap
    cap_offset = jax.random.randint(key_list[0], (MESH_NODES,), 0, REACH)
    recv_row = cell_lat * CELL + jax.random.randint(key_list[1], (MESH_NODES,), 0, CELL)
    recv_row = jnp.where(top_cap, cap_offset, recv_row)
    recv_row = jnp.where(bottom_cap, GRID_ROWS - 1 - cap_offset, recv_row)
    recv_col = cell_lon * CELL + jax.random.randint(key_list[2], (MESH_NODES,), 0, CELL)
    box_side = 2 * REACH + 1
    box_size = box_side * box_side
    scores = jax.random.randint(key_list[3], (MESH_NODES, box_size), 0, 1048576) * box_size + jnp.arange(box_size)
    picked = jnp.argsort(scores, axis=1)[:, :SLOTS]
    send_row = recv_row[:, None] + picked // box_side - REACH
    send_col = recv_col[:, None] + picked % box_side - REACH
    past_north = send_row < 0
    past_south = send_row >= GRID_ROWS
    send_col = jnp.where(past_north | past_south, send_col + GRID_COLS // 2, send_col)
    send_row = jnp.where(past_north, -1 - send_row, send_row)
    send_row = jnp.where(past_south, 2 * GRID_ROWS - 1 - send_row, send_row)
    cap_slot = cap_node[:, None] & (jnp.arange(SLOTS) >= SLOTS // 4)[None, :]
    cap_row = jax.random.randint(key_list[4], (MESH_NODES, SLOTS), 0, REACH)
    cap_row = jnp.where(top_cap[:, None], cap_row, GRID_ROWS - 1 - cap_row)
    cap_col = jax.random.randint(key_list[5], (MESH_NODES, SLOTS), 0, GRID_COLS)
    send_row = jnp.where(cap_slot, cap_row, send_row)
    send_col = jnp.where(cap_slot, cap_col, send_col) % GRID_COLS
    senders = (send_row * GRID_COLS + send_col).astype(jnp.int32)
    counts = jax.random.randint(key_list[6], (MESH_NODES,), 1, SLOTS + 1)
    few_count = jax.random.randint(key_list[8], (MESH_NODES,), 1, 4)
    small_node = jax.random.randint(key_list[9], (MESH_NODES,), 0, 3) == 0
    counts = jnp.where(small_node, few_count, counts)
    counts = jnp.where(cap_node, SLOTS, counts)
    slot_draw = jax.random.randint(key_list[10], (MESH_NODES, SLOTS), 0, SLOTS)
    edge_mask = ((slot_draw < counts[:, None]) | (jnp.arange(SLOTS)[None, :] == 0)).astype(jnp.int32)
    sub_pos = jax.random.uniform(key_list[7], (MESH_NODES, 2), jnp.float32)
    recv_lat = 0.5 * jnp.pi - (recv_row + sub_pos[:, 0]) * (jnp.pi / GRID_ROWS)
    recv_lon = (recv_col + sub_pos[:, 1]) * (2.0 * jnp.pi / GRID_COLS)
    send_lat = 0.5 * jnp.pi - (send_row + 0.5) * (jnp.pi / GRID_ROWS)
    send_lon = (send_col + 0.5) * (2.0 * jnp.pi / GRID_COLS)
    mesh_feat = jnp.stack([jnp.cos(recv_lat), jnp.sin(recv_lon), jnp.cos(recv_lon)], axis=-1)
    rel_lon = send_lon - recv_lon[:, None]
    sender_x = jnp.cos(send_lat) * jnp.cos(rel_lon)
    sender_y = jnp.cos(send_lat) * jnp.sin(rel_lon)
    sender_z = jnp.sin(send_lat)
    cos_lat = jnp.cos(recv_lat)[:, None]
    sin_lat = jnp.sin(recv_lat)[:, None]
    delta_x = sender_x * cos_lat + sender_z * sin_lat - 1.0
    delta_z = sender_z * cos_lat - sender_x * sin_lat
    distance = jnp.sqrt(delta_x * delta_x + sender_y * sender_y + delta_z * delta_z)
    inv_length = 1.0 / jnp.max(distance)
    edge_feat = jnp.stack([distance, delta_x, sender_y, delta_z], axis=-1) * inv_length
    return mesh_feat.astype(jnp.bfloat16), edge_feat.astype(jnp.bfloat16), senders, edge_mask


def dense_init(sub_key, fan_in, fan_out):
    values = jax.random.normal(sub_key, (fan_in, fan_out), jnp.float32) * fan_in ** -0.5
    return values.astype(jnp.bfloat16)


def setup_inputs(seed: int = 0, part: int = 0) -> dict:
    root_key = jax.random.key(seed)
    graph_key, weight_key, grid_key = jax.random.split(root_key, 3)
    mesh_in, edge_in, senders, edge_mask = draw_graph(graph_key)
    grid_keys = jax.random.split(jax.random.fold_in(grid_key, part), 2)
    row_ids = jnp.arange(GRID_ROWS)
    col_ids = jnp.arange(GRID_COLS)
    row_sign = ((row_ids // CELL) % 2) * 2.0 - 1.0
    col_sign = ((col_ids // CELL) % 2) * 2.0 - 1.0
    fronts = jax.random.normal(grid_keys[1], (2, CIN), jnp.float32)
    front_field = row_sign[:, None, None] * fronts[0] + col_sign[None, :, None] * fronts[1]
    base_field = jax.random.normal(grid_keys[0], (BATCH, GRID_ROWS, GRID_COLS, CIN), jnp.float32)
    grid_in = (base_field + 1.5 * front_field).astype(jnp.bfloat16)
    weight_keys = jax.random.split(weight_key, 8)
    w_out = (jax.random.normal(weight_keys[6], (6, LATENT, LATENT), jnp.float32) * LATENT ** -0.5).astype(jnp.bfloat16)
    spread = jnp.array([0.5, 0.5, 0.3, 0.3], jnp.float32)[None, :, None]
    offset = jnp.array([0.0, 0.0, 1.0, 0.0], jnp.float32)[None, :, None]
    bias_gain = jax.random.normal(weight_keys[7], (6, 4, LATENT), jnp.float32) * spread + offset
    return {
        'grid_in': grid_in,
        'mesh_in': mesh_in,
        'edge_in': edge_in,
        'senders': senders,
        'edge_mask': edge_mask,
        'w_grid': dense_init(weight_keys[0], CIN, LATENT),
        'w_mesh': dense_init(weight_keys[1], 3, LATENT),
        'w_edge': dense_init(weight_keys[2], 4, LATENT),
        'w_msg': dense_init(weight_keys[3], 3 * LATENT, LATENT),
        'w_node': dense_init(weight_keys[4], 2 * LATENT, LATENT),
        'w_gupd': dense_init(weight_keys[5], LATENT, LATENT),
        'w_out': w_out,
        'bias_gain': bias_gain,
    }


def mlp_apply(inputs, w_first, w_second, params):
    lead_shape = inputs.shape[:-1]
    flat_in = inputs.reshape(-1, inputs.shape[-1])
    hidden = jnp.dot(flat_in, w_first, preferred_element_type=jnp.float32) + params[0]
    hidden = jax.nn.silu(hidden).astype(jnp.bfloat16)
    result = jnp.dot(hidden, w_second, preferred_element_type=jnp.float32) + params[1]
    return result.reshape(lead_shape + (w_second.shape[1],))


def layer_norm(values, params):
    centered = values - jnp.mean(values, axis=-1, keepdims=True)
    variance = jnp.mean(centered * centered, axis=-1, keepdims=True)
    return centered * lax.rsqrt(variance + LN_EPS) * params[2] + params[3]


def embed_block(inputs, w_first, w_second, params):
    return layer_norm(mlp_apply(inputs, w_first, w_second, params), params).astype(jnp.bfloat16)


def reference(grid_in, mesh_in, edge_in, senders, edge_mask, w_grid, w_mesh, w_edge, w_msg, w_node, w_gupd, w_out, bias_gain):
    def grid_band(row_band):
        band_lat = embed_block(row_band, w_grid, w_out[0], bias_gain[0])
        band_upd = layer_norm(mlp_apply(band_lat, w_gupd, w_out[5], bias_gain[5]), bias_gain[5])
        return band_lat, (band_lat.astype(jnp.float32) + band_upd).astype(jnp.bfloat16)

    row_bands = jnp.moveaxis(grid_in.reshape(BATCH, LAT_CELLS, CELL, GRID_COLS, CIN), 1, 0)
    band_lat, band_out = lax.map(grid_band, row_bands)
    grid_flat = jnp.moveaxis(band_lat, 0, 1).reshape(BATCH, GRID_ROWS * GRID_COLS, LATENT)
    grid_out = jnp.moveaxis(band_out, 0, 1).reshape(BATCH, GRID_ROWS, GRID_COLS, LATENT)
    mesh_lat = embed_block(mesh_in, w_mesh, w_out[1], bias_gain[1])

    def cell_update(cell_block):
        cell_edges, cell_senders, cell_mask, cell_mesh = cell_block
        edge_lat = embed_block(cell_edges, w_edge, w_out[2], bias_gain[2])
        sender_lat = jnp.take(grid_flat, cell_senders.reshape(-1), axis=1).reshape(BATCH, MESH_CELL, SLOTS, LATENT)
        full_shape = (BATCH, MESH_CELL, SLOTS, LATENT)
        msg_in = jnp.concatenate([
            jnp.broadcast_to(edge_lat[None], full_shape),
            sender_lat,
            jnp.broadcast_to(cell_mesh[None, :, None, :], full_shape)], axis=-1)
        msg_upd = layer_norm(mlp_apply(msg_in, w_msg, w_out[3], bias_gain[3]), bias_gain[3])
        edge_new = (edge_lat.astype(jnp.float32) + msg_upd).astype(jnp.bfloat16)
        weights = cell_mask.astype(jnp.float32)[None, :, :, None]
        agg_sum = jnp.sum(edge_new.astype(jnp.float32) * weights, axis=2).astype(jnp.bfloat16)
        node_in = jnp.concatenate([jnp.broadcast_to(cell_mesh[None], (BATCH, MESH_CELL, LATENT)), agg_sum], axis=-1)
        node_upd = layer_norm(mlp_apply(node_in, w_node, w_out[4], bias_gain[4]), bias_gain[4])
        return (cell_mesh.astype(jnp.float32) + node_upd).astype(jnp.bfloat16)

    cell_count = LAT_CELLS * LON_CELLS
    cell_out = lax.map(cell_update, (
        edge_in.reshape(cell_count, MESH_CELL, SLOTS, 4),
        senders.reshape(cell_count, MESH_CELL, SLOTS),
        edge_mask.reshape(cell_count, MESH_CELL, SLOTS),
        mesh_lat.reshape(cell_count, MESH_CELL, LATENT)))
    mesh_out = jnp.moveaxis(cell_out, 1, 0).reshape(BATCH, MESH_NODES, LATENT)
    return mesh_out, grid_out
```

```python
import functools

import jax
import jax.numpy as jnp
from jax import lax
from jax.experimental import pallas as pl
from jax.experimental.pallas import tpu as pltpu
from jax.sharding import PartitionSpec as P

REACH = 3
LN_EPS = 1e-5
CELL = 16
BATCH = 16
CIN = 186
LAT = 512
HALF = 64
LANES = 128
NODES = 8
SLOTS = 48
NSLOT = NODES * SLOTS
GROUP = 16
ROWS = GROUP * BATCH
EDGE_PTS, POLE_PTS, ROW_PTS = 2 * REACH, CELL - 2 * REACH, CELL
EDGE_BLK, POLE_BLK, ROW_BLK = EDGE_PTS * 3 // 2, POLE_PTS * 3 // 2, ROW_PTS * 3 // 2
BASE_EDGE = 0
BASE_POLE = BASE_EDGE + CELL * EDGE_BLK
BASE_NORTH = BASE_POLE + REACH * POLE_BLK
BASE_SOUTH = BASE_NORTH + REACH * ROW_BLK
BASE_CN = BASE_SOUTH + REACH * ROW_BLK
BASE_CS = BASE_CN + REACH * EDGE_BLK
BLOCKS = BASE_CS + REACH * EDGE_BLK
LIST = 512
bf16, f32, i32 = jnp.bfloat16, jnp.float32, jnp.int32


def dot(a, b):
    return jnp.dot(a, b, preferred_element_type=f32)


def swish(x):
    h = 0.5 * x
    return (h + h * jnp.tanh(h)).astype(bf16)


def norm(y, par):
    y = y - jnp.mean(y, axis=-1, keepdims=True)
    var = jnp.mean(y * y, axis=-1, keepdims=True)
    return y * lax.rsqrt(var + LN_EPS) * par[2:3] + par[3:4]


def finish(pre, w2, par):
    return norm(dot(swish(pre + par[0:1]), w2) + par[1:2], par)


def pack_hi(y):
    half = y.shape[0] // 2
    hi = y[:, LANES:]
    return y[:, :LANES].astype(bf16), (hi[:half] + pltpu.roll(hi[half:], HALF, 1)).astype(bf16)


def pack_kernel(x_ref, edge_ref, pole_ref, north_ref, south_ref, cn_ref, cs_ref, pad_ref):
    lat = lax.axis_index('lat')
    a = lax.broadcasted_iota(i32, (ROWS, ROWS), 0)
    b = lax.broadcasted_iota(i32, (ROWS, ROWS), 1)
    flip = jnp.where((a // BATCH) + (a % BATCH) * CELL == b, 1.0, 0.0).astype(bf16)
    flip_edge = jnp.concatenate([flip[:REACH * BATCH], flip[(CELL - REACH) * BATCH:]], axis=0)
    pad_ref[...] = jnp.zeros_like(pad_ref)
    top_pole = [None] * REACH
    for i in range(CELL):
        slot = i % 2
        pad_ref[slot, :, :CIN] = x_ref[:, i].reshape(ROWS, CIN)
        xi = pad_ref[slot]
        lo, hi = pack_hi(dot(flip_edge, xi))
        n_lo, n_hi = EDGE_PTS * BATCH, EDGE_PTS * BATCH // 2
        dests = [(edge_ref, i)]
        if i < REACH:
            dests.append((cn_ref, i))
        if i >= CELL - REACH:
            dests.append((cs_ref, i - CELL + REACH))
        for ref, row in dests:
            start = row * EDGE_BLK * BATCH
            ref[start:start + n_lo] = lo
            ref[start + n_lo:start + n_lo + n_hi] = hi
        if i < REACH or i >= CELL - REACH:
            full = dot(flip, xi)
            ref, row = (north_ref, i) if i < REACH else (south_ref, i - CELL + REACH)
            lo, hi = pack_hi(full)
            start = row * ROW_BLK * BATCH
            ref[start:start + ROWS] = lo
            ref[start + ROWS:start + ROWS * 3 // 2] = hi
            lo, hi = pack_hi(full[REACH * BATCH:(CELL - REACH) * BATCH])
            if i < REACH:
                top_pole[row] = (lo, hi)
                start = row * POLE_BLK * BATCH
                pole_ref[start:start + POLE_PTS * BATCH] = lo
                pole_ref[start + POLE_PTS * BATCH:start + POLE_BLK * BATCH] = hi
            else:
                @pl.when(lat != 0)
                def _(lo=lo, hi=hi, row=row):
                    start = row * POLE_BLK * BATCH
                    pole_ref[start:start + POLE_PTS * BATCH] = lo
                    pole_ref[start + POLE_PTS * BATCH:start + POLE_BLK * BATCH] = hi


def message(lhs, rows, lp_ref, el_ref, acc_ref, w_msg, w_out3, par):
    pre = dot(lhs, w_msg)
    parts = [pre[u * BATCH:(u + 1) * BATCH] + lp_ref[pl.ds(t, 1), :] for u, (t, _) in enumerate(rows)]
    hid = swish(jnp.concatenate(parts, axis=0))
    upd = norm(dot(hid, w_out3) + par[1:2], par)
    for u, (t, node) in enumerate(rows):
        new = (upd[u * BATCH:(u + 1) * BATCH] + el_ref[pl.ds(t, 1), :]).astype(bf16).astype(f32)
        at = pl.ds(pl.multiple_of(node * BATCH, BATCH), BATCH)
        acc_ref[at, :] = acc_ref[at, :] + new


def local_kernel(senders_ref, mask_ref, x_ref, mesh_ref, edge_ref, wg_ref, wm_ref, we_ref, wmsg_ref, wgu_ref, wo_ref, par_ref,
                 grid_ref, acc_ref, lp_ref, el_ref, vm_ref, rlist_ref,
                 vgt_ref, out_ref, lhs_ref, llist_ref, sem):
    lat = lax.axis_index('lat')
    lon = lax.axis_index('lon')
    a = lax.broadcasted_iota(i32, (ROWS, ROWS), 0)
    b = lax.broadcasted_iota(i32, (ROWS, ROWS), 1)
    flip = jnp.where((a // BATCH) + (a % BATCH) * CELL == b, 1.0, 0.0).astype(bf16)

    def sort_slots(first, count, carry):
        n_loc, n_rem = carry
        for k in range(count):
            t = first + k
            node = t // SLOTS if isinstance(t, int) else lax.div(t, SLOTS)
            s = senders_ref[node, t - node * SLOTS]
            live = mask_ref[node, t - node * SLOTS]
            row, col = s >> 5, s & 31
            r = row - lat * CELL
            c = col & (CELL - 1)
            own_lon = (col >> 4) == lon
            in_band = (r >= 0) & (r < CELL)
            local = in_band & own_lon
            is_edge = (c < REACH) | (c >= CELL - REACH)
            e = jnp.where(c < REACH, c, c - (CELL - 2 * REACH))
            nr = jnp.where(r < 0, r + REACH, r - CELL)
            band_base = jnp.where(r < 0, jnp.where(own_lon, BASE_NORTH, BASE_CN), jnp.where(own_lon, BASE_SOUTH, BASE_CS))
            pole_row = jnp.where(lat == 0, r, r - (CELL - REACH))
            pole = in_band & jnp.logical_not(is_edge)
            base = jnp.where(in_band, jnp.where(pole, BASE_POLE, BASE_EDGE), band_base)
            line = jnp.where(in_band, jnp.where(pole, pole_row, r), nr)
            q = jnp.where(pole, c - REACH, jnp.where(own_lon, c, e))
            half = jnp.where(pole, POLE_PTS // 2, jnp.where(own_lon, ROW_PTS // 2, EDGE_PTS // 2))
            start = base + line * (half * 3)
            upper = jnp.where(q >= half, 1, 0)
            lo = start + q
            hi = start + half * 2 + q - upper * half
            llist_ref[n_loc] = t | ((r * CELL + c) << 16)
            rlist_ref[n_rem] = t | (lo << 9) | (hi << 18) | (upper << 27)
            n_loc = n_loc + jnp.where(local, live, 0)
            n_rem = n_rem + jnp.where(local, 0, live)
        return n_loc, n_rem

    def copy_out(i):
        return pltpu.make_async_copy(out_ref.at[i], grid_ref.at[:, i], sem.at[i])

    per_row = NSLOT // CELL

    def grid_row(i, carry):
        carry = sort_slots(i * per_row, per_row, carry)
        xi = x_ref[:, i].reshape(ROWS, CIN)
        par = par_ref[0]
        vg = finish(dot(xi, wg_ref[...]), wo_ref[0], par).astype(bf16)
        at = pl.ds(pl.multiple_of(i * ROWS, ROWS), ROWS)
        vgt_ref[at, :] = dot(flip, vg).astype(bf16)
        par = par_ref[5]
        upd = finish(dot(vg, wgu_ref[...]), wo_ref[5], par)
        out_ref[i] = (vg.astype(f32) + upd).astype(bf16).reshape(BATCH, CELL, LAT)
        copy_out(i).start()
        return carry

    n_loc, n_rem = lax.fori_loop(0, CELL, grid_row, (jnp.int32(0), jnp.int32(0)))
    rlist_ref[LIST - 1] = n_rem

    vm = finish(dot(mesh_ref[...], wm_ref[...]), wo_ref[1], par_ref[1]).astype(bf16)
    vm_ref[...] = vm.astype(f32)
    el = finish(dot(edge_ref[...], we_ref[...]), wo_ref[2], par_ref[2]).astype(bf16)
    el_ref[...] = el.astype(f32)
    vm_proj = dot(vm, wmsg_ref[2 * LAT:]) + par_ref[3][0:1]
    lp = dot(el, wmsg_ref[:LAT]).reshape(NODES, SLOTS, LAT) + vm_proj[:, None, :]
    lp_ref[...] = lp.reshape(NSLOT, LAT)
    acc_ref[...] = jnp.zeros_like(acc_ref)

    def group(g, carry):
        rows = []
        for u in range(GROUP):
            at = g * GROUP + u
            entry = llist_ref[at]
            ok = at < n_loc
            t = jnp.where(ok, entry & 0xFFFF, 0)
            p = jnp.where(ok, entry >> 16, 0)
            node = jnp.where(ok, lax.div(t, SLOTS), NODES)
            lhs_ref[u * BATCH:(u + 1) * BATCH] = vgt_ref[pl.ds(pl.multiple_of(p * BATCH, BATCH), BATCH), :]
            rows.append((t, node))
        message(lhs_ref[...], rows, lp_ref, el_ref, acc_ref, wmsg_ref[LAT:2 * LAT], wo_ref[3], par_ref[3])
        return carry

    lax.fori_loop(0, (n_loc + GROUP - 1) // GROUP, group, 0)
    for i in range(CELL):
        copy_out(i).wait()


def remote_kernel(rlist_ref, edge_ref, pole_ref, north_ref, south_ref, cn_ref, cs_ref, acc_in_ref, lp_ref, el_ref, vm_ref,
                  wg_ref, wmsg_ref, wnode_ref, wo_ref, par_ref, mesh_ref,
                  rx_ref, wpad_ref, lhs_ref, acc_ref, sem):
    copies = []
    for k, (ref, base) in enumerate([(edge_ref, BASE_EDGE), (pole_ref, BASE_POLE), (north_ref, BASE_NORTH), (south_ref, BASE_SOUTH), (cn_ref, BASE_CN), (cs_ref, BASE_CS)]):
        copies.append(pltpu.make_async_copy(ref, rx_ref.at[pl.ds(base * BATCH, ref.shape[0])], sem.at[k]))
        copies[-1].start()
    wpad_ref[...] = jnp.zeros_like(wpad_ref)
    wpad_ref[:CIN] = wg_ref[...]
    acc_ref[...] = acc_in_ref[...]
    n_rem = rlist_ref[LIST - 1]
    for copy in copies:
        copy.wait()

    def group(g, carry):
        rows = []
        for u in range(GROUP):
            at = g * GROUP + u
            ok = at < n_rem
            entry = jnp.where(ok, rlist_ref[at], 0)
            t = entry & 0x1FF
            lo = (entry >> 9) & 0x1FF
            hi = (entry >> 18) & 0x1FF
            upper = entry >> 27
            node = jnp.where(ok, lax.div(t, SLOTS), NODES)
            dst = slice(u * BATCH, (u + 1) * BATCH)
            lhs_ref[dst, :LANES] = rx_ref[pl.ds(pl.multiple_of(lo * BATCH, BATCH), BATCH), :]
            high = rx_ref[pl.ds(pl.multiple_of(hi * BATCH, BATCH), BATCH), :].astype(f32)
            high = jnp.where(upper == 1, pltpu.roll(high, HALF, 1), high)
            lhs_ref[dst, LANES:] = high.astype(bf16)
            rows.append((t, node))
        vg = finish(dot(lhs_ref[...], wpad_ref[...]), wo_ref[0], par_ref[0]).astype(bf16)
        message(vg, rows, lp_ref, el_ref, acc_ref, wmsg_ref[LAT:2 * LAT], wo_ref[3], par_ref[3])
        return carry

    lax.fori_loop(0, (n_rem + GROUP - 1) // GROUP, group, 0)

    vm = vm_ref[...]
    n_rows = NODES * BATCH
    agg = acc_ref[:n_rows].astype(bf16)
    base = dot(vm.astype(bf16), wnode_ref[:LAT])
    pre = dot(agg, wnode_ref[LAT:]).reshape(NODES, BATCH, LAT) + base[:, None, :]
    upd = finish(pre.reshape(n_rows, LAT), wo_ref[4], par_ref[4])
    out = (upd.reshape(NODES, BATCH, LAT) + vm[:, None, :]).reshape(n_rows, LAT).astype(bf16)
    a = lax.broadcasted_iota(i32, (n_rows, n_rows), 0)
    b = lax.broadcasted_iota(i32, (n_rows, n_rows), 1)
    flip = jnp.where((a // NODES) + (a % NODES) * BATCH == b, 1.0, 0.0).astype(bf16)
    mesh_ref[...] = dot(flip, out).astype(bf16).reshape(BATCH, NODES, LAT)


def solution(mesh):
    n_lat, n_lon = mesh.shape['lat'], mesh.shape['lon']

    def pairs(d_lat, d_lon, keep):
        return [(j * n_lat + i, (j + d_lon) % n_lon * n_lat + i + d_lat)
                for i in range(n_lat) for j in range(n_lon) if 0 <= i + d_lat < n_lat and keep(i)]

    def cell_step(grid_in, mesh_in, edge_in, senders, edge_mask, w_grid, w_mesh, w_edge, w_msg, w_node, w_gupd, w_out, bias_gain):
        vmem = pl.BlockSpec(memory_space=pltpu.VMEM)
        smem = pl.BlockSpec(memory_space=pltpu.SMEM)
        any_ = pl.BlockSpec(memory_space=pl.ANY)
        sizes = [CELL * EDGE_BLK, REACH * POLE_BLK, REACH * ROW_BLK, REACH * ROW_BLK, REACH * EDGE_BLK, REACH * EDGE_BLK]
        halo = pl.pallas_call(
            pack_kernel,
            name='pack',
            out_shape=[jax.ShapeDtypeStruct((n * BATCH, LANES), bf16) for n in sizes],
            in_specs=[vmem],
            out_specs=[vmem] * 6,
            scratch_shapes=[pltpu.VMEM((2, ROWS, 256), bf16)],
            compiler_params=pltpu.CompilerParams(vmem_limit_bytes=24 << 20),
            cost_estimate=pl.CostEstimate(flops=10**9, bytes_accessed=4 << 20, transcendentals=0),
        )(grid_in)
        every = lambda i: True
        pole = lambda i: i in (0, n_lat - 1)
        names = ('lon', 'lat')
        edge, polar, north, south, c_north, c_south = halo
        got_edge = lax.ppermute(edge, names, pairs(0, 1, every))
        from_south = lax.ppermute(north, names, pairs(-1, 0, every))
        from_north = lax.ppermute(south, names, pairs(1, 0, every))
        got_cs = lax.ppermute(c_north, names, pairs(-1, 1, every))
        got_cn = lax.ppermute(c_south, names, pairs(1, 1, every))
        got_pole = lax.ppermute(polar, names, pairs(0, 1, pole))

        grid_out, acc, lp, el, vm, rlist = pl.pallas_call(
            local_kernel,
            name='local',
            out_shape=[
                jax.ShapeDtypeStruct((BATCH, CELL, CELL, LAT), bf16),
                jax.ShapeDtypeStruct(((NODES + 1) * BATCH, LAT), f32),
                jax.ShapeDtypeStruct((NSLOT, LAT), f32),
                jax.ShapeDtypeStruct((NSLOT, LAT), f32),
                jax.ShapeDtypeStruct((NODES, LAT), f32),
                jax.ShapeDtypeStruct((LIST,), i32),
            ],
            in_specs=[smem, smem] + [vmem] * 10,
            out_specs=[any_, vmem, vmem, vmem, vmem, smem],
            scratch_shapes=[
                pltpu.VMEM((ROWS * CELL, LAT), bf16),
                pltpu.VMEM((CELL, BATCH, CELL, LAT), bf16),
                pltpu.VMEM((ROWS, LAT), bf16),
                pltpu.SMEM((LIST,), i32),
                pltpu.SemaphoreType.DMA((CELL,)),
            ],
            compiler_params=pltpu.CompilerParams(vmem_limit_bytes=40 << 20),
            cost_estimate=pl.CostEstimate(flops=20 * 10**9, bytes_accessed=16 << 20, transcendentals=0),
        )(senders, edge_mask, grid_in, mesh_in, edge_in.reshape(NSLOT, 4), w_grid, w_mesh, w_edge, w_msg, w_gupd, w_out, bias_gain)

        mesh_out = pl.pallas_call(
            remote_kernel,
            name='remote',
            out_shape=jax.ShapeDtypeStruct((BATCH, NODES, LAT), bf16),
            in_specs=[smem] + [any_] * 6 + [vmem] * 9,
            out_specs=vmem,
            scratch_shapes=[
                pltpu.VMEM((BLOCKS * BATCH, LANES), bf16),
                pltpu.VMEM((256, LAT), bf16),
                pltpu.VMEM((ROWS, 256), bf16),
                pltpu.VMEM(((NODES + 1) * BATCH, LAT), f32),
                pltpu.SemaphoreType.DMA((6,)),
            ],
            compiler_params=pltpu.CompilerParams(vmem_limit_bytes=24 << 20),
            cost_estimate=pl.CostEstimate(flops=4 * 10**9, bytes_accessed=8 << 20, transcendentals=0),
        )(rlist, got_edge, got_pole, from_north, from_south, got_cn, got_cs, acc, lp, el, vm, w_grid, w_msg, w_node, w_out, bias_gain)
        return mesh_out, grid_out

    grid_spec = P('dp', 'lat', 'lon', None)
    node_spec = P(('lat', 'lon'), None)
    slot_spec = P(('lat', 'lon'), None, None)
    rep = P()
    in_specs = (grid_spec, node_spec, slot_spec, node_spec, node_spec) + (rep,) * 8
    out_specs = (P('dp', ('lat', 'lon'), None), grid_spec)
    return jax.shard_map(cell_step, mesh=mesh, in_specs=in_specs, out_specs=out_specs, check_vma=False)
```

```python
import functools

import jax
import jax.numpy as jnp
from jax import lax
from jax.experimental import pallas as pl
from jax.experimental.pallas import tpu as pltpu
from jax.sharding import PartitionSpec as P

REACH = 3
LN_EPS = 1e-5
CELL = 16
BATCH = 16
CIN = 186
LAT = 512
HALF = 64
LANES = 128
NODES = 8
SLOTS = 48
NSLOT = NODES * SLOTS
GROUP = 16
ROWS = GROUP * BATCH
EDGE_PTS, POLE_PTS, ROW_PTS = 2 * REACH, CELL - 2 * REACH, CELL
EDGE_BLK, POLE_BLK, ROW_BLK = EDGE_PTS * 3 // 2, POLE_PTS * 3 // 2, ROW_PTS * 3 // 2
BASE_EDGE = 0
BASE_POLE = BASE_EDGE + CELL * EDGE_BLK
BASE_NORTH = BASE_POLE + REACH * POLE_BLK
BASE_SOUTH = BASE_NORTH + REACH * ROW_BLK
BASE_CN = BASE_SOUTH + REACH * ROW_BLK
BASE_CS = BASE_CN + REACH * EDGE_BLK
BLOCKS = BASE_CS + REACH * EDGE_BLK
LIST = 512
bf16, f32, i32 = jnp.bfloat16, jnp.float32, jnp.int32
MESH = pl.DeviceIdType.MESH


def dot(a, b):
    return jnp.dot(a, b, preferred_element_type=f32)


def swish(h):
    return (h + h * jnp.tanh(h)).astype(bf16)


def scale(y):
    y = y - jnp.mean(y, axis=-1, keepdims=True)
    var = jnp.mean(y * y, axis=-1, keepdims=True)
    return y * lax.rsqrt(var + LN_EPS)


def norm(y, par):
    return scale(y) * par[2:3] + par[3:4]


def finish(half_pre, w2, par):
    return norm(dot(swish(half_pre), w2) + par[1:2], par)


def pack_hi(y):
    half = y.shape[0] // 2
    hi = y[:, LANES:]
    return y[:, :LANES].astype(bf16), (hi[:half] + pltpu.roll(hi[half:], HALF, 1)).astype(bf16)


def fill_embed(wpad_ref, wg_ref, b1):
    tile = CIN // BATCH * BATCH
    wpad_ref[tile:] = jnp.zeros((256 - tile, LAT), bf16)
    wpad_ref[:CIN] = wg_ref[...]
    b_hi = b1.astype(bf16)
    b_mid = (b1 - b_hi.astype(f32)).astype(bf16)
    b_lo = (b1 - b_hi.astype(f32) - b_mid.astype(f32)).astype(bf16)
    row = lax.broadcasted_iota(i32, (BATCH, LAT), 0) + tile
    edge = wpad_ref[tile:tile + BATCH].astype(f32)
    for k, part in enumerate((b_hi, b_mid, b_lo)):
        edge = jnp.where(row == CIN + k, part.astype(f32), edge)
    wpad_ref[tile:tile + BATCH] = edge.astype(bf16)
    wpad_ref[...] = wpad_ref[...] * bf16(0.5)


def slot_codes(senders, live, lat, lon):
    t = lax.broadcasted_iota(i32, senders.shape, 0) * SLOTS + lax.broadcasted_iota(i32, senders.shape, 1)
    row, col = senders >> 5, senders & 31
    r = row - lat * CELL
    c = col & (CELL - 1)
    own_lon = (col >> 4) == lon
    in_band = (r >= 0) & (r < CELL)
    local = in_band & own_lon
    is_edge = (c < REACH) | (c >= CELL - REACH)
    pole = in_band & jnp.logical_not(is_edge)
    e = jnp.where(c < REACH, c, c - (CELL - EDGE_PTS))
    north = r < 0
    band_base = jnp.where(north, jnp.where(own_lon, BASE_NORTH, BASE_CN), jnp.where(own_lon, BASE_SOUTH, BASE_CS))
    base = jnp.where(in_band, jnp.where(pole, BASE_POLE, BASE_EDGE), band_base)
    pole_line = jnp.where(lat == 0, r, r - (CELL - REACH))
    line = jnp.where(in_band, jnp.where(pole, pole_line, r), jnp.where(north, r + REACH, r - CELL))
    q = jnp.where(pole, c - REACH, jnp.where(own_lon, c, e))
    half = jnp.where(pole, POLE_PTS // 2, jnp.where(own_lon, ROW_PTS // 2, EDGE_PTS // 2))
    start = base + line * (half * 3)
    upper = jnp.where(q >= half, 1, 0)
    lo = start + q
    hi = start + half * 2 + q - upper * half
    near = t | ((r * CELL + c) << 9) | (live << 28)
    far = t | (lo << 9) | (hi << 18) | (upper << 27) | (live << 29)
    return jnp.where(local, near, far)


def flip_matrix(rows, inner):
    a = lax.broadcasted_iota(i32, (rows, rows), 0)
    b = lax.broadcasted_iota(i32, (rows, rows), 1)
    outer = rows // inner
    return jnp.where(a // outer + a % outer * inner == b, 1.0, 0.0).astype(bf16)


def own_kernel(n_lat, n_lon, x_hbm, mesh_ref, edge_ref, send_ref, mask_ref, wg_hbm, wm_hbm, we_hbm, wmsg_hbm, wgu_hbm, wo_hbm, par_hbm,
               vgt_ref, gout_ref, rx_out_ref, lp_ref, el_ref, vm_ref, code_ref,
               x_ref, wg_ref, wm_ref, we_ref, wmsg_ref, wgu_ref, wo_ref, par_ref, xpad_ref, wpad_ref, tx_ref, rx_ref,
               in_sem, send_sem, recv_sem):
    dp = lax.axis_index('dp')
    lon = lax.axis_index('lon')
    lat = lax.axis_index('lat')
    across = (dp, (lon + 1) % n_lon, lat)
    up = (dp, lon, lat - 1)
    down = (dp, lon, lat + 1)
    has_up = lat > 0
    has_down = lat < n_lat - 1
    at_pole = jnp.logical_or(lat == 0, lat == n_lat - 1)

    loads = [(x_hbm, x_ref), (wg_hbm, wg_ref), (par_hbm, par_ref), (wo_hbm, wo_ref), (wgu_hbm, wgu_ref), (wm_hbm, wm_ref),
             (we_hbm, we_ref), (wmsg_hbm, wmsg_ref)]
    loads = [pltpu.make_async_copy(a, b, in_sem.at[k]) for k, (a, b) in enumerate(loads)]
    for load in loads:
        load.start()

    barrier = pltpu.get_barrier_semaphore()
    pl.semaphore_signal(barrier, inc=1, device_id=across, device_id_type=MESH)

    @pl.when(has_up)
    def _():
        pl.semaphore_signal(barrier, inc=1, device_id=up, device_id_type=MESH)

    @pl.when(has_down)
    def _():
        pl.semaphore_signal(barrier, inc=1, device_id=down, device_id_type=MESH)

    def send(k, src_ref, src, dst, count, to):
        return pltpu.make_async_remote_copy(
            src_ref=src_ref.at[pl.ds(src * BATCH, count * BATCH)], dst_ref=rx_ref.at[pl.ds(dst * BATCH, count * BATCH)],
            send_sem=send_sem.at[k], recv_sem=recv_sem.at[k], device_id=to, device_id_type=MESH)

    e_top = send(0, tx_ref, BASE_EDGE, BASE_EDGE, REACH * EDGE_BLK, across)
    e_low = send(1, tx_ref, BASE_EDGE + (CELL - REACH) * EDGE_BLK, BASE_EDGE + (CELL - REACH) * EDGE_BLK, REACH * EDGE_BLK, across)
    e_mid = send(2, tx_ref, BASE_EDGE + REACH * EDGE_BLK, BASE_EDGE + REACH * EDGE_BLK, (CELL - 2 * REACH) * EDGE_BLK, across)
    polar = send(3, tx_ref, BASE_POLE, BASE_POLE, REACH * POLE_BLK, across)
    to_up = send(4, tx_ref, BASE_SOUTH, BASE_SOUTH, REACH * ROW_BLK, up)
    to_down = send(5, tx_ref, BASE_NORTH, BASE_NORTH, REACH * ROW_BLK, down)
    fwd_up = send(6, rx_ref, BASE_EDGE, BASE_CS, REACH * EDGE_BLK, up)
    fwd_down = send(7, rx_ref, BASE_EDGE + (CELL - REACH) * EDGE_BLK, BASE_CN, REACH * EDGE_BLK, down)

    code_ref[...] = slot_codes(send_ref[...], mask_ref[...], lat, lon)
    flip = flip_matrix(ROWS, CELL)
    flip_edge = jnp.concatenate([flip[:REACH * BATCH], flip[(CELL - REACH) * BATCH:]], axis=0)
    lane = lax.broadcasted_iota(i32, (ROWS, LANES), 1) + LANES
    ones = jnp.where((lane >= CIN) & (lane < CIN + 3), 1.0, 0.0).astype(bf16)
    loads[0].wait()

    def put(row, lo, hi):
        n = lo.shape[0]
        at = row * BATCH
        tx_ref[pl.ds(pl.multiple_of(at, BATCH), n), :] = lo
        tx_ref[pl.ds(pl.multiple_of(at + n, BATCH), n // 2), :] = hi

    def pad_row(i):
        at = pl.ds(pl.multiple_of(i * ROWS, ROWS), ROWS)
        xpad_ref[at, LANES:] = ones
        xpad_ref[at, :CIN] = x_ref[:, i].reshape(ROWS, CIN)
        return xpad_ref[at, :]

    def band_row(k, carry):
        for base, first, is_top in ((BASE_SOUTH, 0, True), (BASE_NORTH, CELL - REACH, False)):
            i = first + k
            full = dot(flip, pad_row(i))
            edge = jnp.concatenate([full[:REACH * BATCH], full[(CELL - REACH) * BATCH:]], axis=0)
            put(BASE_EDGE + i * EDGE_BLK, *pack_hi(edge))
            put(base + k * ROW_BLK, *pack_hi(full))
            lo, hi = pack_hi(full[REACH * BATCH:(CELL - REACH) * BATCH])
            if is_top:
                put(BASE_POLE + k * POLE_BLK, lo, hi)
            else:
                @pl.when(lat != 0)
                def _(lo=lo, hi=hi):
                    put(BASE_POLE + k * POLE_BLK, lo, hi)
        return carry

    lax.fori_loop(0, REACH, band_row, 0)
    pl.semaphore_wait(barrier, 1 + has_up.astype(i32) + has_down.astype(i32))
    e_top.start()
    e_low.start()
    pl.when(has_up)(to_up.start)
    pl.when(has_down)(to_down.start)
    pl.when(at_pole)(polar.start)

    def mid_row(i, carry):
        put(BASE_EDGE + i * EDGE_BLK, *pack_hi(dot(flip_edge, pad_row(i))))
        return carry

    lax.fori_loop(REACH, CELL - REACH, mid_row, 0)
    e_mid.start()

    for load in loads[1:]:
        load.wait()
    fill_embed(wpad_ref, wg_ref, par_ref[0][0:1])
    wgu_ref[...] = wgu_ref[...] * bf16(0.5)

    def grid_rows(k, carry):
        vgs = []
        for u in range(2):
            at = pl.ds(pl.multiple_of((k * 2 + u) * ROWS, ROWS), ROWS)
            vgs.append(finish(dot(xpad_ref[at, :], wpad_ref[...]), wo_ref[0], par_ref[0]).astype(bf16))
        for u in range(2):
            i = k * 2 + u
            vgt_ref[pl.ds(pl.multiple_of(i * ROWS, ROWS), ROWS), :] = dot(flip, vgs[u]).astype(bf16)
            upd = finish(dot(vgs[u], wgu_ref[...]) + 0.5 * par_ref[5][0:1], wo_ref[5], par_ref[5])
            gout_ref[i] = (vgs[u].astype(f32) + upd).astype(bf16).reshape(BATCH, CELL, LAT)
        return carry

    lax.fori_loop(0, CELL // 4, grid_rows, 0)
    e_top.wait_recv()
    e_low.wait_recv()
    pl.when(has_up)(fwd_up.start)
    pl.when(has_down)(fwd_down.start)
    lax.fori_loop(CELL // 4, CELL // 2, grid_rows, 0)

    par = par_ref[1]
    vm = finish(0.5 * (dot(mesh_ref[...], wm_ref[...]) + par[0:1]), wo_ref[1], par).astype(bf16)
    vm_ref[...] = vm.astype(f32)
    par = par_ref[2]
    el = finish(0.5 * (dot(edge_ref[...], we_ref[...]) + par[0:1]), wo_ref[2], par).astype(bf16)
    par = par_ref[3]
    el_ref[...] = el.astype(f32) + par[3:4]
    vm_proj = dot(vm, wmsg_ref[2 * LAT:]) + par[0:1]
    lp = dot(el, wmsg_ref[:LAT]).reshape(NODES, SLOTS, LAT) + vm_proj[:, None, :]
    lp_ref[...] = 0.5 * lp.reshape(NSLOT, LAT)

    e_mid.wait_recv()
    pl.when(at_pole)(polar.wait_recv)

    @pl.when(has_down)
    def _():
        to_up.wait_recv()
        fwd_up.wait_recv()

    @pl.when(has_up)
    def _():
        to_down.wait_recv()
        fwd_down.wait_recv()

    rx_out_ref[...] = rx_ref[...]
    e_top.wait_send()
    e_low.wait_send()
    e_mid.wait_send()
    pl.when(at_pole)(polar.wait_send)

    @pl.when(has_up)
    def _():
        to_up.wait_send()
        fwd_up.wait_send()

    @pl.when(has_down)
    def _():
        to_down.wait_send()
        fwd_down.wait_send()


def message(lhs, rows, lp_ref, el_ref, acc_ref, w_msg, w_out3, par):
    pre = dot(lhs, w_msg)
    parts = [pre[u * BATCH:(u + 1) * BATCH] + lp_ref[pl.ds(t, 1), :] for u, (t, _) in enumerate(rows)]
    hid = swish(jnp.concatenate(parts, axis=0))
    upd = scale(dot(hid, w_out3) + par[1:2]) * par[2:3]
    for u, (t, node) in enumerate(rows):
        new = (upd[u * BATCH:(u + 1) * BATCH] + el_ref[pl.ds(t, 1), :]).astype(bf16).astype(f32)
        at = pl.ds(pl.multiple_of(node * BATCH, BATCH), BATCH)
        acc_ref[at, :] = acc_ref[at, :] + new


def slot_kernel(code_ref, vgt_ref, gout_ref, rx_ref, lp_ref, el_ref, vm_ref, wg_ref, wmsg_ref, wnode_ref, wo_ref, par_ref,
                mesh_ref, grid_ref, wpad_ref, wmid_ref, lhs_ref, acc_ref, near_ref, far_ref, sem):
    copies = [pltpu.make_async_copy(gout_ref.at[i], grid_ref.at[:, i], sem.at[i]) for i in range(CELL)]
    for copy in copies:
        copy.start()
    fill_embed(wpad_ref, wg_ref, par_ref[0][0:1])
    wmid_ref[...] = wmsg_ref[LAT:2 * LAT] * bf16(0.5)
    acc_ref[...] = jnp.zeros_like(acc_ref)

    def sort_slots(node, carry):
        n_near, n_far = carry
        for k in range(SLOTS):
            code = code_ref[node, k]
            near_ref[n_near] = code
            far_ref[n_far] = code
            n_near = n_near + ((code >> 28) & 1)
            n_far = n_far + (code >> 29)
        return n_near, n_far

    n_near, n_far = lax.fori_loop(0, NODES, sort_slots, (jnp.int32(0), jnp.int32(0)))

    def block(ref, index):
        return ref[pl.ds(pl.multiple_of(index * BATCH, BATCH), BATCH), :]

    def near_group(g, carry):
        rows = []
        for u in range(GROUP):
            ok = g * GROUP + u < n_near
            code = jnp.where(ok, near_ref[g * GROUP + u], 0)
            t = code & 0x1FF
            rows.append((t, jnp.where(ok, lax.div(t, SLOTS), NODES)))
            lhs_ref[u * BATCH:(u + 1) * BATCH] = block(vgt_ref, (code >> 9) & 0xFF)
        message(lhs_ref[...], rows, lp_ref, el_ref, acc_ref, wmid_ref[...], wo_ref[3], par_ref[3])
        return carry

    lax.fori_loop(0, (n_near + GROUP - 1) // GROUP, near_group, 0)

    def far_group(g, carry):
        rows = []
        for u in range(GROUP):
            ok = g * GROUP + u < n_far
            code = jnp.where(ok, far_ref[g * GROUP + u], 0)
            t = code & 0x1FF
            rows.append((t, jnp.where(ok, lax.div(t, SLOTS), NODES)))
            dst = slice(u * BATCH, (u + 1) * BATCH)
            lhs_ref[dst, :LANES] = block(rx_ref, (code >> 9) & 0x1FF)
            high = block(rx_ref, (code >> 18) & 0x1FF).astype(f32)
            high = jnp.where((code >> 27) & 1 == 1, pltpu.roll(high, HALF, 1), high)
            lhs_ref[dst, LANES:256] = high.astype(bf16)
        vg = finish(dot(lhs_ref[:, :256], wpad_ref[...]), wo_ref[0], par_ref[0]).astype(bf16)
        message(vg, rows, lp_ref, el_ref, acc_ref, wmid_ref[...], wo_ref[3], par_ref[3])
        return carry

    lax.fori_loop(0, (n_far + GROUP - 1) // GROUP, far_group, 0)

    vm = vm_ref[...]
    n_rows = NODES * BATCH
    par = par_ref[4]
    agg = acc_ref[:n_rows].astype(bf16)
    base = dot(vm.astype(bf16), wnode_ref[:LAT]) + par[0:1]
    pre = dot(agg, wnode_ref[LAT:]).reshape(NODES, BATCH, LAT) + base[:, None, :]
    upd = finish(0.5 * pre.reshape(n_rows, LAT), wo_ref[4], par)
    out = (upd.reshape(NODES, BATCH, LAT) + vm[:, None, :]).reshape(n_rows, LAT).astype(bf16)
    mesh_ref[...] = dot(flip_matrix(n_rows, BATCH), out).astype(bf16).reshape(BATCH, NODES, LAT)
    for copy in copies:
        copy.wait()


def solution(mesh):
    n_lat, n_lon = mesh.shape['lat'], mesh.shape['lon']

    def cell_step(grid_in, mesh_in, edge_in, senders, edge_mask, w_grid, w_mesh, w_edge, w_msg, w_node, w_gupd, w_out, bias_gain):
        vmem = pl.BlockSpec(memory_space=pltpu.VMEM)
        smem = pl.BlockSpec(memory_space=pltpu.SMEM)
        hbm = pl.BlockSpec(memory_space=pltpu.HBM)
        heavy = [w_grid, w_mesh, w_edge, w_msg, w_gupd, w_out, bias_gain]
        own = pl.pallas_call(
            functools.partial(own_kernel, n_lat, n_lon),
            name='own',
            out_shape=[
                jax.ShapeDtypeStruct((ROWS * CELL, LAT), bf16),
                jax.ShapeDtypeStruct((CELL, BATCH, CELL, LAT), bf16),
                jax.ShapeDtypeStruct((BLOCKS * BATCH, LANES), bf16),
                jax.ShapeDtypeStruct((NSLOT, LAT), f32),
                jax.ShapeDtypeStruct((NSLOT, LAT), f32),
                jax.ShapeDtypeStruct((NODES, LAT), f32),
                jax.ShapeDtypeStruct((NODES, SLOTS), i32),
            ],
            in_specs=[hbm] + [vmem] * 4 + [hbm] * 7,
            out_specs=[vmem] * 7,
            scratch_shapes=[
                pltpu.VMEM(grid_in.shape, bf16),
                *[pltpu.VMEM(w.shape, w.dtype) for w in heavy],
                pltpu.VMEM((ROWS * CELL, 256), bf16),
                pltpu.VMEM((256, LAT), bf16),
                pltpu.VMEM((BLOCKS * BATCH, LANES), bf16),
                pltpu.VMEM((BLOCKS * BATCH, LANES), bf16),
                pltpu.SemaphoreType.DMA((8,)),
                pltpu.SemaphoreType.DMA((8,)),
                pltpu.SemaphoreType.DMA((8,)),
            ],
            compiler_params=pltpu.CompilerParams(vmem_limit_bytes=36 << 20, collective_id=0, has_side_effects=True),
            cost_estimate=pl.CostEstimate(flops=10 * 10**9, bytes_accessed=16 << 20, transcendentals=0),
        )(grid_in, mesh_in, edge_in.reshape(NSLOT, 4), senders, edge_mask, *heavy)
        vgt, gout, rx, lp, el, vm, code = own

        mesh_out, grid_out = pl.pallas_call(
            slot_kernel,
            name='slots',
            out_shape=[jax.ShapeDtypeStruct((BATCH, NODES, LAT), bf16), jax.ShapeDtypeStruct((BATCH, CELL, CELL, LAT), bf16)],
            in_specs=[smem] + [vmem] * 11,
            out_specs=[vmem, hbm],
            scratch_shapes=[
                pltpu.VMEM((256, LAT), bf16),
                pltpu.VMEM((LAT, LAT), bf16),
                pltpu.VMEM((ROWS, LAT), bf16),
                pltpu.VMEM(((NODES + 1) * BATCH, LAT), f32),
                pltpu.SMEM((LIST,), i32),
                pltpu.SMEM((LIST,), i32),
                pltpu.SemaphoreType.DMA((CELL,)),
            ],
            compiler_params=pltpu.CompilerParams(vmem_limit_bytes=24 << 20),
            cost_estimate=pl.CostEstimate(flops=10 * 10**9, bytes_accessed=16 << 20, transcendentals=0),
        )(code, vgt, gout, rx, lp, el, vm, w_grid, w_msg, w_node, w_out, bias_gain)
        return mesh_out, grid_out

    grid_spec = P('dp', 'lat', 'lon', None)
    node_spec = P(('lat', 'lon'), None)
    slot_spec = P(('lat', 'lon'), None, None)
    rep = P()
    in_specs = (grid_spec, node_spec, slot_spec, node_spec, node_spec) + (rep,) * 8
    out_specs = (P('dp', ('lat', 'lon'), None), grid_spec)
    return jax.shard_map(cell_step, mesh=mesh, in_specs=in_specs, out_specs=out_specs, check_vma=False)
```

```python
import functools

import jax
import jax.numpy as jnp
from jax import lax
from jax.experimental import pallas as pl
from jax.experimental.pallas import tpu as pltpu
from jax.sharding import PartitionSpec as P

REACH = 3
LN_EPS = 1e-5
CELL = 16
BATCH = 16
CIN = 186
LAT = 512
HALF = 64
LANES = 128
NODES = 8
SLOTS = 48
NSLOT = NODES * SLOTS
GROUP = 16
ROWS = GROUP * BATCH
EDGE_PTS, POLE_PTS, ROW_PTS = 2 * REACH, CELL - 2 * REACH, CELL
EDGE_BLK, POLE_BLK, ROW_BLK = EDGE_PTS * 3 // 2, POLE_PTS * 3 // 2, ROW_PTS * 3 // 2
BASE_EDGE = 0
BASE_POLE = BASE_EDGE + CELL * EDGE_BLK
BASE_NORTH = BASE_POLE + REACH * POLE_BLK
BASE_SOUTH = BASE_NORTH + REACH * ROW_BLK
BASE_CN = BASE_SOUTH + REACH * ROW_BLK
BASE_CS = BASE_CN + REACH * EDGE_BLK
BLOCKS = BASE_CS + REACH * EDGE_BLK
LIST = 512
bf16, f32, i32 = jnp.bfloat16, jnp.float32, jnp.int32
MESH = pl.DeviceIdType.MESH


def dot(a, b):
    return jnp.dot(a, b, preferred_element_type=f32)


def dot_t(a, b):
    return lax.dot_general(a, b, (((0,), (0,)), ((), ())), preferred_element_type=f32)


def swish(h):
    return (h + h * jnp.tanh(h)).astype(bf16)


def scale(y):
    y = y - jnp.mean(y, axis=-1, keepdims=True)
    var = jnp.mean(y * y, axis=-1, keepdims=True)
    return y * lax.rsqrt(var + LN_EPS)


def norm(y, par):
    return scale(y) * par[2:3] + par[3:4]


def finish(half_pre, w2, par):
    return norm(dot(swish(half_pre), w2) + par[1:2], par)


def pack_hi(y):
    half = y.shape[0] // 2
    hi = y[:, LANES:]
    return y[:, :LANES].astype(bf16), (hi[:half] + pltpu.roll(hi[half:], HALF, 1)).astype(bf16)


def fill_embed(wpad_ref, wg_ref, b1):
    tile = CIN // BATCH * BATCH
    wpad_ref[tile:] = jnp.zeros((256 - tile, LAT), bf16)
    wpad_ref[:CIN] = wg_ref[...]
    b_hi = b1.astype(bf16)
    b_mid = (b1 - b_hi.astype(f32)).astype(bf16)
    b_lo = (b1 - b_hi.astype(f32) - b_mid.astype(f32)).astype(bf16)
    row = lax.broadcasted_iota(i32, (BATCH, LAT), 0) + tile
    edge = wpad_ref[tile:tile + BATCH].astype(f32)
    for k, part in enumerate((b_hi, b_mid, b_lo)):
        edge = jnp.where(row == CIN + k, part.astype(f32), edge)
    wpad_ref[tile:tile + BATCH] = edge.astype(bf16)
    wpad_ref[...] = wpad_ref[...] * bf16(0.5)


def slot_codes(senders, live, lat, lon):
    t = lax.broadcasted_iota(i32, senders.shape, 0) * SLOTS + lax.broadcasted_iota(i32, senders.shape, 1)
    row, col = senders >> 5, senders & 31
    r = row - lat * CELL
    c = col & (CELL - 1)
    own_lon = (col >> 4) == lon
    in_band = (r >= 0) & (r < CELL)
    local = in_band & own_lon
    is_edge = (c < REACH) | (c >= CELL - REACH)
    pole = in_band & jnp.logical_not(is_edge)
    e = jnp.where(c < REACH, c, c - (CELL - EDGE_PTS))
    north = r < 0
    band_base = jnp.where(north, jnp.where(own_lon, BASE_NORTH, BASE_CN), jnp.where(own_lon, BASE_SOUTH, BASE_CS))
    base = jnp.where(in_band, jnp.where(pole, BASE_POLE, BASE_EDGE), band_base)
    pole_line = jnp.where(lat == 0, r, r - (CELL - REACH))
    line = jnp.where(in_band, jnp.where(pole, pole_line, r), jnp.where(north, r + REACH, r - CELL))
    q = jnp.where(pole, c - REACH, jnp.where(own_lon, c, e))
    half = jnp.where(pole, POLE_PTS // 2, jnp.where(own_lon, ROW_PTS // 2, EDGE_PTS // 2))
    start = base + line * (half * 3)
    upper = jnp.where(q >= half, 1, 0)
    lo = start + q
    hi = start + half * 2 + q - upper * half
    near = t | ((r * CELL + c) << 9) | (live << 28)
    far = t | (lo << 9) | (hi << 18) | (upper << 27) | (live << 29)
    return jnp.where(local, near, far)


def flip_matrix(rows, inner):
    a = lax.broadcasted_iota(i32, (rows, rows), 0)
    b = lax.broadcasted_iota(i32, (rows, rows), 1)
    outer = rows // inner
    return jnp.where(a // outer + a % outer * inner == b, 1.0, 0.0).astype(bf16)


def own_kernel(n_lat, n_lon, x_hbm, mesh_hbm, edge_hbm, send_hbm, mask_hbm, wg_hbm, wm_hbm, we_hbm, wmsg_hbm, wgu_hbm, wo_hbm, par_hbm,
               vgt_ref, gout_ref, rx_out_ref, lp_ref, el_ref, vm_ref, code_ref,
               x_ref, mesh_ref, edge_ref, send_ref, mask_ref, wg_ref, wm_ref, we_ref, wmsg_ref, wgu_ref, wo_ref, par_ref, xpad_ref, wpad_ref, tx_ref, rx_ref,
               in_sem, send_sem, recv_sem):
    dp = lax.axis_index('dp')
    lon = lax.axis_index('lon')
    lat = lax.axis_index('lat')
    across = (dp, (lon + 1) % n_lon, lat)
    up = (dp, lon, lat - 1)
    down = (dp, lon, lat + 1)
    has_up = lat > 0
    has_down = lat < n_lat - 1
    at_pole = jnp.logical_or(lat == 0, lat == n_lat - 1)

    loads = [(x_hbm, x_ref), (wg_hbm, wg_ref), (par_hbm, par_ref), (wo_hbm, wo_ref), (wgu_hbm, wgu_ref), (wm_hbm, wm_ref),
             (we_hbm, we_ref), (wmsg_hbm, wmsg_ref), (mesh_hbm, mesh_ref), (edge_hbm, edge_ref), (send_hbm, send_ref), (mask_hbm, mask_ref)]
    loads = [pltpu.make_async_copy(a, b, in_sem.at[k]) for k, (a, b) in enumerate(loads)]
    for load in loads:
        load.start()

    barrier = pltpu.get_barrier_semaphore()
    pl.semaphore_signal(barrier, inc=1, device_id=across, device_id_type=MESH)

    @pl.when(has_up)
    def _():
        pl.semaphore_signal(barrier, inc=1, device_id=up, device_id_type=MESH)

    @pl.when(has_down)
    def _():
        pl.semaphore_signal(barrier, inc=1, device_id=down, device_id_type=MESH)

    def send(k, src_ref, src, dst, count, to):
        return pltpu.make_async_remote_copy(
            src_ref=src_ref.at[pl.ds(src * BATCH, count * BATCH)], dst_ref=rx_ref.at[pl.ds(dst * BATCH, count * BATCH)],
            send_sem=send_sem.at[k], recv_sem=recv_sem.at[k], device_id=to, device_id_type=MESH)

    e_top = send(0, tx_ref, BASE_EDGE, BASE_EDGE, REACH * EDGE_BLK, across)
    e_low = send(1, tx_ref, BASE_EDGE + (CELL - REACH) * EDGE_BLK, BASE_EDGE + (CELL - REACH) * EDGE_BLK, REACH * EDGE_BLK, across)
    e_mid = send(2, tx_ref, BASE_EDGE + REACH * EDGE_BLK, BASE_EDGE + REACH * EDGE_BLK, (CELL - 2 * REACH) * EDGE_BLK, across)
    polar = send(3, tx_ref, BASE_POLE, BASE_POLE, REACH * POLE_BLK, across)
    to_up = send(4, tx_ref, BASE_SOUTH, BASE_SOUTH, REACH * ROW_BLK, up)
    to_down = send(5, tx_ref, BASE_NORTH, BASE_NORTH, REACH * ROW_BLK, down)
    fwd_up = send(6, rx_ref, BASE_EDGE, BASE_CS, REACH * EDGE_BLK, up)
    fwd_down = send(7, rx_ref, BASE_EDGE + (CELL - REACH) * EDGE_BLK, BASE_CN, REACH * EDGE_BLK, down)

    flip = flip_matrix(ROWS, CELL)
    flip_edge = jnp.concatenate([flip[:REACH * BATCH], flip[(CELL - REACH) * BATCH:]], axis=0)
    lane = lax.broadcasted_iota(i32, (ROWS, LANES), 1) + LANES
    ones = jnp.where((lane >= CIN) & (lane < CIN + 3), 1.0, 0.0).astype(bf16)
    loads[0].wait()

    def put(row, lo, hi):
        n = lo.shape[0]
        at = row * BATCH
        tx_ref[pl.ds(pl.multiple_of(at, BATCH), n), :] = lo
        tx_ref[pl.ds(pl.multiple_of(at + n, BATCH), n // 2), :] = hi

    def pad_row(i):
        at = pl.ds(pl.multiple_of(i * ROWS, ROWS), ROWS)
        xpad_ref[at, LANES:] = ones
        xpad_ref[at, :CIN] = x_ref[:, i].reshape(ROWS, CIN)
        return xpad_ref[at, :]

    def band_row(k, carry):
        for base, first, is_top in ((BASE_SOUTH, 0, True), (BASE_NORTH, CELL - REACH, False)):
            i = first + k
            full = dot(flip, pad_row(i))
            edge = jnp.concatenate([full[:REACH * BATCH], full[(CELL - REACH) * BATCH:]], axis=0)
            put(BASE_EDGE + i * EDGE_BLK, *pack_hi(edge))
            put(base + k * ROW_BLK, *pack_hi(full))
            lo, hi = pack_hi(full[REACH * BATCH:(CELL - REACH) * BATCH])
            if is_top:
                put(BASE_POLE + k * POLE_BLK, lo, hi)
            else:
                @pl.when(lat != 0)
                def _(lo=lo, hi=hi):
                    put(BASE_POLE + k * POLE_BLK, lo, hi)
        return carry

    lax.fori_loop(0, REACH, band_row, 0)
    pl.semaphore_wait(barrier, 1 + has_up.astype(i32) + has_down.astype(i32))
    e_top.start()
    e_low.start()
    pl.when(has_up)(to_up.start)
    pl.when(has_down)(to_down.start)
    pl.when(at_pole)(polar.start)

    def mid_row(i, carry):
        put(BASE_EDGE + i * EDGE_BLK, *pack_hi(dot(flip_edge, pad_row(i))))
        return carry

    lax.fori_loop(REACH, CELL - REACH, mid_row, 0)
    e_mid.start()

    for load in loads[1:]:
        load.wait()
    code_ref[...] = slot_codes(send_ref[...], mask_ref[...], lat, lon)
    fill_embed(wpad_ref, wg_ref, par_ref[0][0:1])
    wgu_ref[...] = wgu_ref[...] * bf16(0.5)

    def grid_rows(k, carry):
        vgs = []
        for u in range(2):
            at = pl.ds(pl.multiple_of((k * 2 + u) * ROWS, ROWS), ROWS)
            vgs.append(finish(dot(xpad_ref[at, :], wpad_ref[...]), wo_ref[0], par_ref[0]).astype(bf16))
        for u in range(2):
            i = k * 2 + u
            vgt_ref[pl.ds(pl.multiple_of(i * ROWS, ROWS), ROWS), :] = dot(flip, vgs[u]).astype(bf16)
            upd = finish(dot(vgs[u], wgu_ref[...]) + 0.5 * par_ref[5][0:1], wo_ref[5], par_ref[5])
            gout_ref[i] = (vgs[u].astype(f32) + upd).astype(bf16).reshape(BATCH, CELL, LAT)
        return carry

    lax.fori_loop(0, CELL // 4, grid_rows, 0)
    e_top.wait_recv()
    e_low.wait_recv()
    pl.when(has_up)(fwd_up.start)
    pl.when(has_down)(fwd_down.start)
    lax.fori_loop(CELL // 4, CELL // 2, grid_rows, 0)

    par = par_ref[1]
    vm = finish(0.5 * (dot_t(mesh_ref[...], wm_ref[...]) + par[0:1]), wo_ref[1], par).astype(bf16)
    vm_ref[...] = vm.astype(f32)
    par = par_ref[2]
    el = finish(0.5 * (jnp.concatenate([dot_t(edge_ref[n], we_ref[...]) for n in range(NODES)], axis=0) + par[0:1]), wo_ref[2], par).astype(bf16)
    par = par_ref[3]
    el_ref[...] = el.astype(f32) + par[3:4]
    vm_proj = dot(vm, wmsg_ref[2 * LAT:]) + par[0:1]
    lp = dot(el, wmsg_ref[:LAT]).reshape(NODES, SLOTS, LAT) + vm_proj[:, None, :]
    lp_ref[...] = 0.5 * lp.reshape(NSLOT, LAT)

    e_mid.wait_recv()
    pl.when(at_pole)(polar.wait_recv)

    @pl.when(has_down)
    def _():
        to_up.wait_recv()
        fwd_up.wait_recv()

    @pl.when(has_up)
    def _():
        to_down.wait_recv()
        fwd_down.wait_recv()

    rx_out_ref[...] = rx_ref[...]
    e_top.wait_send()
    e_low.wait_send()
    e_mid.wait_send()
    pl.when(at_pole)(polar.wait_send)

    @pl.when(has_up)
    def _():
        to_up.wait_send()
        fwd_up.wait_send()

    @pl.when(has_down)
    def _():
        to_down.wait_send()
        fwd_down.wait_send()


def message(lhs, rows, lp_ref, el_ref, acc_ref, w_msg, w_out3, par):
    pre = dot(lhs, w_msg)
    parts = [pre[u * BATCH:(u + 1) * BATCH] + lp_ref[pl.ds(t, 1), :] for u, (t, _) in enumerate(rows)]
    hid = swish(jnp.concatenate(parts, axis=0))
    upd = scale(dot(hid, w_out3) + par[1:2]) * par[2:3]
    for u, (t, node) in enumerate(rows):
        new = (upd[u * BATCH:(u + 1) * BATCH] + el_ref[pl.ds(t, 1), :]).astype(bf16).astype(f32)
        at = pl.ds(pl.multiple_of(node * BATCH, BATCH), BATCH)
        acc_ref[at, :] = acc_ref[at, :] + new


def slot_kernel(code_ref, vgt_ref, gout_ref, rx_ref, lp_ref, el_ref, vm_ref, wg_ref, wmsg_ref, wnode_ref, wo_ref, par_ref,
                mesh_ref, grid_ref, wpad_ref, wmid_ref, lhs_ref, acc_ref, near_ref, far_ref, sem):
    copies = [pltpu.make_async_copy(gout_ref.at[i], grid_ref.at[:, i], sem.at[i]) for i in range(CELL)]
    for copy in copies:
        copy.start()
    fill_embed(wpad_ref, wg_ref, par_ref[0][0:1])
    wmid_ref[...] = wmsg_ref[LAT:2 * LAT] * bf16(0.5)
    acc_ref[...] = jnp.zeros_like(acc_ref)

    def sort_slots(node, carry):
        n_near, n_far = carry
        for k in range(SLOTS):
            code = code_ref[node, k]
            near_ref[n_near] = code
            far_ref[n_far] = code
            n_near = n_near + ((code >> 28) & 1)
            n_far = n_far + (code >> 29)
        return n_near, n_far

    n_near, n_far = lax.fori_loop(0, NODES, sort_slots, (jnp.int32(0), jnp.int32(0)))

    def block(ref, index):
        return ref[pl.ds(pl.multiple_of(index * BATCH, BATCH), BATCH), :]

    def near_group(g, carry):
        rows = []
        for u in range(GROUP):
            ok = g * GROUP + u < n_near
            code = jnp.where(ok, near_ref[g * GROUP + u], 0)
            t = code & 0x1FF
            rows.append((t, jnp.where(ok, lax.div(t, SLOTS), NODES)))
            lhs_ref[u * BATCH:(u + 1) * BATCH] = block(vgt_ref, (code >> 9) & 0xFF)
        message(lhs_ref[...], rows, lp_ref, el_ref, acc_ref, wmid_ref[...], wo_ref[3], par_ref[3])
        return carry

    lax.fori_loop(0, (n_near + GROUP - 1) // GROUP, near_group, 0)

    def far_group(g, carry):
        rows = []
        for u in range(GROUP):
            ok = g * GROUP + u < n_far
            code = jnp.where(ok, far_ref[g * GROUP + u], 0)
            t = code & 0x1FF
            rows.append((t, jnp.where(ok, lax.div(t, SLOTS), NODES)))
            dst = slice(u * BATCH, (u + 1) * BATCH)
            lhs_ref[dst, :LANES] = block(rx_ref, (code >> 9) & 0x1FF)
            high = block(rx_ref, (code >> 18) & 0x1FF).astype(f32)
            high = jnp.where((code >> 27) & 1 == 1, pltpu.roll(high, HALF, 1), high)
            lhs_ref[dst, LANES:256] = high.astype(bf16)
        vg = finish(dot(lhs_ref[:, :256], wpad_ref[...]), wo_ref[0], par_ref[0]).astype(bf16)
        message(vg, rows, lp_ref, el_ref, acc_ref, wmid_ref[...], wo_ref[3], par_ref[3])
        return carry

    lax.fori_loop(0, (n_far + GROUP - 1) // GROUP, far_group, 0)

    vm = vm_ref[...]
    n_rows = NODES * BATCH
    par = par_ref[4]
    agg = acc_ref[:n_rows].astype(bf16)
    base = dot(vm.astype(bf16), wnode_ref[:LAT]) + par[0:1]
    pre = dot(agg, wnode_ref[LAT:]).reshape(NODES, BATCH, LAT) + base[:, None, :]
    upd = finish(0.5 * pre.reshape(n_rows, LAT), wo_ref[4], par)
    out = (upd.reshape(NODES, BATCH, LAT) + vm[:, None, :]).reshape(n_rows, LAT).astype(bf16)
    mesh_ref[...] = dot(flip_matrix(n_rows, BATCH), out).astype(bf16).reshape(BATCH, NODES, LAT)
    for copy in copies:
        copy.wait()


def solution(mesh):
    n_lat, n_lon = mesh.shape['lat'], mesh.shape['lon']

    def cell_step(grid_in, mesh_in, edge_in, senders, edge_mask, w_grid, w_mesh, w_edge, w_msg, w_node, w_gupd, w_out, bias_gain):
        vmem = pl.BlockSpec(memory_space=pltpu.VMEM)
        smem = pl.BlockSpec(memory_space=pltpu.SMEM)
        hbm = pl.BlockSpec(memory_space=pltpu.HBM)
        loaded = [grid_in, mesh_in.T, edge_in.transpose(0, 2, 1), senders, edge_mask, w_grid, w_mesh, w_edge, w_msg, w_gupd, w_out, bias_gain]
        pin = lambda x: pltpu.with_memory_space_constraint(x, pltpu.HBM)
        own = pl.pallas_call(
            functools.partial(own_kernel, n_lat, n_lon),
            name='own',
            out_shape=[
                pltpu.VMEM((ROWS * CELL, LAT), bf16),
                pltpu.VMEM((CELL, BATCH, CELL, LAT), bf16),
                pltpu.VMEM((BLOCKS * BATCH, LANES), bf16),
                pltpu.VMEM((NSLOT, LAT), f32),
                pltpu.VMEM((NSLOT, LAT), f32),
                pltpu.VMEM((NODES, LAT), f32),
                pltpu.VMEM((NODES, SLOTS), i32),
            ],
            in_specs=[hbm] * 12,
            out_specs=[vmem] * 7,
            scratch_shapes=[
                *[pltpu.VMEM(a.shape, a.dtype) for a in loaded],
                pltpu.VMEM((ROWS * CELL, 256), bf16),
                pltpu.VMEM((256, LAT), bf16),
                pltpu.VMEM((BLOCKS * BATCH, LANES), bf16),
                pltpu.VMEM((BLOCKS * BATCH, LANES), bf16),
                pltpu.SemaphoreType.DMA((12,)),
                pltpu.SemaphoreType.DMA((8,)),
                pltpu.SemaphoreType.DMA((8,)),
            ],
            compiler_params=pltpu.CompilerParams(vmem_limit_bytes=20 << 20, collective_id=0, has_side_effects=True),
            cost_estimate=pl.CostEstimate(flops=10 * 10**9, bytes_accessed=16 << 20, transcendentals=0),
        )(*map(pin, loaded))
        vgt, gout, rx, lp, el, vm, code = own

        mesh_out, grid_out = pl.pallas_call(
            slot_kernel,
            name='slots',
            out_shape=[jax.ShapeDtypeStruct((BATCH, NODES, LAT), bf16), jax.ShapeDtypeStruct((BATCH, CELL, CELL, LAT), bf16)],
            in_specs=[smem] + [vmem] * 11,
            out_specs=[vmem, hbm],
            scratch_shapes=[
                pltpu.VMEM((256, LAT), bf16),
                pltpu.VMEM((LAT, LAT), bf16),
                pltpu.VMEM((ROWS, LAT), bf16),
                pltpu.VMEM(((NODES + 1) * BATCH, LAT), f32),
                pltpu.SMEM((LIST,), i32),
                pltpu.SMEM((LIST,), i32),
                pltpu.SemaphoreType.DMA((CELL,)),
            ],
            compiler_params=pltpu.CompilerParams(vmem_limit_bytes=24 << 20),
            cost_estimate=pl.CostEstimate(flops=10 * 10**9, bytes_accessed=16 << 20, transcendentals=0),
        )(code, vgt, gout, rx, lp, el, vm, w_grid, w_msg, w_node, w_out, bias_gain)
        return mesh_out, grid_out

    grid_spec = P('dp', 'lat', 'lon', None)
    node_spec = P(('lat', 'lon'), None)
    slot_spec = P(('lat', 'lon'), None, None)
    rep = P()
    in_specs = (grid_spec, node_spec, slot_spec, node_spec, node_spec) + (rep,) * 8
    out_specs = (P('dp', ('lat', 'lon'), None), grid_spec)
    return jax.shard_map(cell_step, mesh=mesh, in_specs=in_specs, out_specs=out_specs, check_vma=False)
```

```python
import functools

import jax
import jax.numpy as jnp
from jax import lax
from jax.experimental import pallas as pl
from jax.experimental.pallas import tpu as pltpu
from jax.sharding import PartitionSpec as P

REACH = 3
LN_EPS = 1e-5
CELL = 16
BATCH = 16
CIN = 186
LAT = 512
HALF = 64
LANES = 128
NODES = 8
SLOTS = 48
NSLOT = NODES * SLOTS
GROUP = 16
ROWS = GROUP * BATCH
EDGE_PTS, POLE_PTS, ROW_PTS = 2 * REACH, CELL - 2 * REACH, CELL
EDGE_BLK, POLE_BLK, ROW_BLK = EDGE_PTS * 3 // 2, POLE_PTS * 3 // 2, ROW_PTS * 3 // 2
BASE_EDGE = 0
BASE_POLE = BASE_EDGE + CELL * EDGE_BLK
BASE_NORTH = BASE_POLE + REACH * POLE_BLK
BASE_SOUTH = BASE_NORTH + REACH * ROW_BLK
BASE_CN = BASE_SOUTH + REACH * ROW_BLK
BASE_CS = BASE_CN + REACH * EDGE_BLK
BLOCKS = BASE_CS + REACH * EDGE_BLK
LIST = 512
FRONT = 3 * GROUP
UNROLL = 2
CHUNK = 256
bf16, f32, i32 = jnp.bfloat16, jnp.float32, jnp.int32
MESH = pl.DeviceIdType.MESH


def dot(a, b):
    return jnp.dot(a, b, preferred_element_type=f32)


def dot_t(a, b):
    return lax.dot_general(a, b, (((0,), (0,)), ((), ())), preferred_element_type=f32)


def swish(h):
    return (h + h * jnp.tanh(h)).astype(bf16)


def scale(y):
    y = y - jnp.mean(y, axis=-1, keepdims=True)
    var = jnp.mean(y * y, axis=-1, keepdims=True)
    return y * lax.rsqrt(var + LN_EPS)


def norm(y, par):
    return scale(y) * par[2:3] + par[3:4]


def finish(half_pre, w2, par):
    return norm(dot(swish(half_pre), w2) + par[1:2], par)


def pack_hi(y):
    half = y.shape[0] // 2
    hi = y[:, LANES:]
    return y[:, :LANES].astype(bf16), (hi[:half] + pltpu.roll(hi[half:], HALF, 1)).astype(bf16)


def fill_embed(wpad_ref, wg_ref, b1):
    tile = CIN // BATCH * BATCH
    wpad_ref[tile:] = jnp.zeros((256 - tile, LAT), bf16)
    wpad_ref[:CIN] = wg_ref[...]
    b_hi = b1.astype(bf16)
    b_mid = (b1 - b_hi.astype(f32)).astype(bf16)
    b_lo = (b1 - b_hi.astype(f32) - b_mid.astype(f32)).astype(bf16)
    row = lax.broadcasted_iota(i32, (BATCH, LAT), 0) + tile
    edge = wpad_ref[tile:tile + BATCH].astype(f32)
    for k, part in enumerate((b_hi, b_mid, b_lo)):
        edge = jnp.where(row == CIN + k, part.astype(f32), edge)
    wpad_ref[tile:tile + BATCH] = edge.astype(bf16)
    wpad_ref[...] = wpad_ref[...] * bf16(0.5)


def slot_codes(senders, live, lat, lon):
    t = lax.broadcasted_iota(i32, senders.shape, 0) * SLOTS + lax.broadcasted_iota(i32, senders.shape, 1)
    row, col = senders >> 5, senders & 31
    r = row - lat * CELL
    c = col & (CELL - 1)
    own_lon = (col >> 4) == lon
    in_band = (r >= 0) & (r < CELL)
    local = in_band & own_lon
    is_edge = (c < REACH) | (c >= CELL - REACH)
    pole = in_band & jnp.logical_not(is_edge)
    e = jnp.where(c < REACH, c, c - (CELL - EDGE_PTS))
    north = r < 0
    band_base = jnp.where(north, jnp.where(own_lon, BASE_NORTH, BASE_CN), jnp.where(own_lon, BASE_SOUTH, BASE_CS))
    base = jnp.where(in_band, jnp.where(pole, BASE_POLE, BASE_EDGE), band_base)
    pole_line = jnp.where(lat == 0, r, r - (CELL - REACH))
    line = jnp.where(in_band, jnp.where(pole, pole_line, r), jnp.where(north, r + REACH, r - CELL))
    q = jnp.where(pole, c - REACH, jnp.where(own_lon, c, e))
    half = jnp.where(pole, POLE_PTS // 2, jnp.where(own_lon, ROW_PTS // 2, EDGE_PTS // 2))
    start = base + line * (half * 3)
    upper = jnp.where(q >= half, 1, 0)
    lo = start + q
    hi = start + half * 2 + q - upper * half
    n_slots = senders.shape[1]

    def ahead(flag):
        value = flag.astype(f32)
        earlier = lax.broadcasted_iota(i32, (n_slots, n_slots), 0) < lax.broadcasted_iota(i32, (n_slots, n_slots), 1)
        inside = dot(value.astype(bf16), jnp.where(earlier, 1.0, 0.0).astype(bf16))
        total = jnp.broadcast_to(jnp.sum(value, axis=1, keepdims=True), (senders.shape[0], LANES)).astype(bf16)
        earlier = lax.broadcasted_iota(i32, (NODES, NODES), 1) < lax.broadcasted_iota(i32, (NODES, NODES), 0)
        return (inside + dot(jnp.where(earlier, 1.0, 0.0).astype(bf16), total)[:, :n_slots]).astype(i32)

    active = live == 1
    far = active & jnp.logical_not(local)
    far_at = ahead(far)
    node = lax.broadcasted_iota(i32, senders.shape, 0)
    source = jnp.where(local, r * CELL + c, far_at + (1 << 9))
    word = t | (node << 9) | (source << 13)
    halo = lo | (hi << 9) | (upper << 18)
    place = jnp.where(active, ahead(active) + FRONT, LIST - 1) | (jnp.where(far, far_at, LIST - 1) << 16)
    count = jnp.sum(active.astype(f32)).astype(i32), jnp.sum(far.astype(f32)).astype(i32)
    return word, halo, place, count


def flip_matrix(rows, inner):
    a = lax.broadcasted_iota(i32, (rows, rows), 0)
    b = lax.broadcasted_iota(i32, (rows, rows), 1)
    outer = rows // inner
    return jnp.where(a // outer + a % outer * inner == b, 1.0, 0.0).astype(bf16)


def own_kernel(n_lat, n_lon, x_hbm, mesh_hbm, edge_hbm, send_hbm, mask_hbm, wg_hbm, wm_hbm, we_hbm, wmsg_hbm, wgu_hbm, wo_hbm, par_hbm,
               vgt_ref, gout_ref, rx_out_ref, lp_ref, el_ref, vm_ref, code_ref,
               x_ref, mesh_ref, edge_ref, send_ref, mask_ref, wg_ref, wm_ref, we_ref, wmsg_ref, wgu_ref, wo_ref, par_ref, xpad_ref, wpad_ref, vg_ref, tx_ref, rx_ref,
               in_sem, send_sem, recv_sem):
    dp = lax.axis_index('dp')
    lon = lax.axis_index('lon')
    lat = lax.axis_index('lat')
    across = (dp, (lon + 1) % n_lon, lat)
    up = (dp, lon, lat - 1)
    down = (dp, lon, lat + 1)
    has_up = lat > 0
    has_down = lat < n_lat - 1
    at_pole = jnp.logical_or(lat == 0, lat == n_lat - 1)

    loads = [(x_hbm, x_ref), (wg_hbm, wg_ref), (par_hbm, par_ref), (wo_hbm, wo_ref), (wgu_hbm, wgu_ref), (wm_hbm, wm_ref),
             (we_hbm, we_ref), (wmsg_hbm, wmsg_ref), (mesh_hbm, mesh_ref), (edge_hbm, edge_ref), (send_hbm, send_ref), (mask_hbm, mask_ref)]
    loads = [pltpu.make_async_copy(a, b, in_sem.at[k]) for k, (a, b) in enumerate(loads)]
    for load in loads:
        load.start()

    barrier = pltpu.get_barrier_semaphore()
    pl.semaphore_signal(barrier, inc=1, device_id=across, device_id_type=MESH)

    @pl.when(has_up)
    def _():
        pl.semaphore_signal(barrier, inc=1, device_id=up, device_id_type=MESH)

    @pl.when(has_down)
    def _():
        pl.semaphore_signal(barrier, inc=1, device_id=down, device_id_type=MESH)

    def send(k, src_ref, src, dst, count, to):
        return pltpu.make_async_remote_copy(
            src_ref=src_ref.at[pl.ds(src * BATCH, count * BATCH)], dst_ref=rx_ref.at[pl.ds(dst * BATCH, count * BATCH)],
            send_sem=send_sem.at[k], recv_sem=recv_sem.at[k], device_id=to, device_id_type=MESH)

    e_top = send(0, tx_ref, BASE_EDGE, BASE_EDGE, REACH * EDGE_BLK, across)
    e_low = send(1, tx_ref, BASE_EDGE + (CELL - REACH) * EDGE_BLK, BASE_EDGE + (CELL - REACH) * EDGE_BLK, REACH * EDGE_BLK, across)
    e_mid = send(2, tx_ref, BASE_EDGE + REACH * EDGE_BLK, BASE_EDGE + REACH * EDGE_BLK, (CELL - 2 * REACH) * EDGE_BLK, across)
    polar = send(3, tx_ref, BASE_POLE, BASE_POLE, REACH * POLE_BLK, across)
    to_up = send(4, tx_ref, BASE_SOUTH, BASE_SOUTH, REACH * ROW_BLK, up)
    to_down = send(5, tx_ref, BASE_NORTH, BASE_NORTH, REACH * ROW_BLK, down)
    fwd_up = send(6, rx_ref, BASE_EDGE, BASE_CS, REACH * EDGE_BLK, up)
    fwd_down = send(7, rx_ref, BASE_EDGE + (CELL - REACH) * EDGE_BLK, BASE_CN, REACH * EDGE_BLK, down)

    flip = flip_matrix(ROWS, CELL)
    flip_edge = jnp.concatenate([flip[:REACH * BATCH], flip[(CELL - REACH) * BATCH:]], axis=0)
    lane = lax.broadcasted_iota(i32, (ROWS, LANES), 1) + LANES
    ones = jnp.where((lane >= CIN) & (lane < CIN + 3), 1.0, 0.0).astype(bf16)
    loads[0].wait()

    def put(row, lo, hi):
        n = lo.shape[0]
        at = row * BATCH
        tx_ref[pl.ds(pl.multiple_of(at, BATCH), n), :] = lo
        tx_ref[pl.ds(pl.multiple_of(at + n, BATCH), n // 2), :] = hi

    def pad_row(i):
        at = pl.ds(pl.multiple_of(i * ROWS, ROWS), ROWS)
        xpad_ref[at, LANES:] = ones
        xpad_ref[at, :CIN] = x_ref[:, i].reshape(ROWS, CIN)
        return xpad_ref[at, :]

    def band_row(k, carry):
        for base, first, is_top in ((BASE_SOUTH, 0, True), (BASE_NORTH, CELL - REACH, False)):
            i = first + k
            full = dot(flip, pad_row(i))
            edge = jnp.concatenate([full[:REACH * BATCH], full[(CELL - REACH) * BATCH:]], axis=0)
            put(BASE_EDGE + i * EDGE_BLK, *pack_hi(edge))
            put(base + k * ROW_BLK, *pack_hi(full))
            lo, hi = pack_hi(full[REACH * BATCH:(CELL - REACH) * BATCH])
            if is_top:
                put(BASE_POLE + k * POLE_BLK, lo, hi)
            else:
                @pl.when(lat != 0)
                def _(lo=lo, hi=hi):
                    put(BASE_POLE + k * POLE_BLK, lo, hi)
        return carry

    lax.fori_loop(0, REACH, band_row, 0)
    pl.semaphore_wait(barrier, 1 + has_up.astype(i32) + has_down.astype(i32))
    e_top.start()
    e_low.start()
    pl.when(has_up)(to_up.start)
    pl.when(has_down)(to_down.start)
    pl.when(at_pole)(polar.start)

    def mid_row(i, carry):
        put(BASE_EDGE + i * EDGE_BLK, *pack_hi(dot(flip_edge, pad_row(i))))
        return carry

    lax.fori_loop(REACH, CELL - REACH, mid_row, 0)
    e_mid.start()

    for load in loads[1:]:
        load.wait()
    fill_embed(wpad_ref, wg_ref, par_ref[0][0:1])
    wgu_ref[...] = wgu_ref[...] * bf16(0.5)

    def embed_rows(k):
        for u in range(UNROLL * ROWS // CHUNK):
            at = pl.ds(pl.multiple_of(k * (UNROLL * ROWS) + u * CHUNK, CHUNK), CHUNK)
            vg_ref[u * CHUNK:(u + 1) * CHUNK] = finish(dot(xpad_ref[at, :], wpad_ref[...]), wo_ref[0], par_ref[0]).astype(bf16)

    def update_rows(k):
        for u in range(UNROLL):
            i = k * UNROLL + u
            vg = vg_ref[u * ROWS:(u + 1) * ROWS]
            vgt_ref[pl.ds(pl.multiple_of(i * ROWS, ROWS), ROWS), :] = dot(flip, vg).astype(bf16)
            for v in range(ROWS // CHUNK):
                vg = vg_ref[u * ROWS + v * CHUNK:u * ROWS + (v + 1) * CHUNK]
                upd = finish(dot(vg, wgu_ref[...]) + 0.5 * par_ref[5][0:1], wo_ref[5], par_ref[5])
                states = CHUNK // CELL
                gout_ref[i, v * states:(v + 1) * states] = (vg.astype(f32) + upd).astype(bf16).reshape(states, CELL, LAT)

    def grid_rows(k, carry):
        update_rows(k - 1)
        embed_rows(k)
        return carry

    trips = CELL // UNROLL
    embed_rows(0)
    lax.fori_loop(1, trips // 2, grid_rows, 0)
    e_top.wait_recv()
    e_low.wait_recv()
    pl.when(has_up)(fwd_up.start)
    pl.when(has_down)(fwd_down.start)
    lax.fori_loop(trips // 2, trips, grid_rows, 0)
    update_rows(trips - 1)

    word, halo, place, counts = slot_codes(send_ref[...], mask_ref[...], lat, lon)
    code_ref[0:NODES] = word
    code_ref[NODES:2 * NODES] = halo
    code_ref[2 * NODES:3 * NODES] = place
    code_ref[3 * NODES:] = jnp.where(lax.broadcasted_iota(i32, (NODES, SLOTS), 1) == 0, counts[0], counts[1])
    par = par_ref[1]
    vm = finish(0.5 * (dot_t(mesh_ref[...], wm_ref[...]) + par[0:1]), wo_ref[1], par).astype(bf16)
    vm_ref[...] = vm.astype(f32)
    par = par_ref[2]
    el = finish(0.5 * (jnp.concatenate([dot_t(edge_ref[n], we_ref[...]) for n in range(NODES)], axis=0) + par[0:1]), wo_ref[2], par).astype(bf16)
    par = par_ref[3]
    el_ref[...] = el.astype(f32) + par[3:4]
    vm_proj = dot(vm, wmsg_ref[2 * LAT:]) + par[0:1]
    lp = dot(el, wmsg_ref[:LAT]).reshape(NODES, SLOTS, LAT) + vm_proj[:, None, :]
    lp_ref[...] = 0.5 * lp.reshape(NSLOT, LAT)

    e_mid.wait_recv()
    pl.when(at_pole)(polar.wait_recv)

    @pl.when(has_down)
    def _():
        to_up.wait_recv()
        fwd_up.wait_recv()

    @pl.when(has_up)
    def _():
        to_down.wait_recv()
        fwd_down.wait_recv()

    rx_out_ref[...] = rx_ref[...]
    e_top.wait_send()
    e_low.wait_send()
    e_mid.wait_send()
    pl.when(at_pole)(polar.wait_send)

    @pl.when(has_up)
    def _():
        to_up.wait_send()
        fwd_up.wait_send()

    @pl.when(has_down)
    def _():
        to_down.wait_send()
        fwd_down.wait_send()


def slot_kernel(code_ref, vgt_ref, gout_ref, rx_ref, lp_ref, el_ref, vm_ref, wg_ref, wmsg_ref, wnode_ref, wo_ref, par_ref,
                mesh_ref, grid_ref, wpad_ref, wmid_ref, lhs_ref, pre_ref, hid_ref, y_ref, far_vg_ref, acc_ref, all_ref, far_ref, sem):
    copies = [pltpu.make_async_copy(gout_ref.at[i], grid_ref.at[:, i], sem.at[i]) for i in range(CELL)]
    for copy in copies:
        copy.start()
    fill_embed(wpad_ref, wg_ref, par_ref[0][0:1])
    wmid_ref[...] = wmsg_ref[LAT:2 * LAT] * bf16(0.5)
    acc_ref[...] = jnp.zeros_like(acc_ref)

    n_all, n_far = code_ref[3 * NODES, 0], code_ref[3 * NODES, 1]

    def fill_lists(node, carry):
        for k in range(SLOTS):
            place = code_ref[2 * NODES + node, k]
            all_ref[place & 0xFFFF] = code_ref[node, k]
            far_ref[place >> 16] = code_ref[NODES + node, k]
        return carry

    lax.fori_loop(0, NODES, fill_lists, 0)
    for k in range(FRONT):
        all_ref[k] = NODES << 9
    for k in range(4 * GROUP):
        all_ref[FRONT + n_all + k] = NODES << 9
    for k in range(4 * GROUP):
        far_ref[n_far + k] = 0

    def block(ref, index):
        return ref[pl.ds(pl.multiple_of(index * BATCH, BATCH), BATCH), :]

    par = par_ref[3]

    n_groups = NSLOT // GROUP

    def slot(at):
        word = all_ref[FRONT + at]
        return word & 0x1FF, (word >> 9) & 0xF, word >> 13

    def embed_step(j, p):
        q = 1 - p
        y_ref[p] = dot(hid_ref[p], wo_ref[0])
        for u in range(GROUP):
            halo = far_ref[j * GROUP + u]
            lo, hi, upper = halo & 0x1FF, (halo >> 9) & 0x1FF, halo >> 18
            dst = slice(u * BATCH, (u + 1) * BATCH)
            lhs_ref[p, dst, :LANES] = block(rx_ref, lo)
            high = block(rx_ref, hi).astype(f32)
            high = jnp.where(upper == 1, pltpu.roll(high, HALF, 1), high)
            lhs_ref[p, dst, LANES:256] = high.astype(bf16)
        pre_ref[p] = dot(lhs_ref[p, :, :256], wpad_ref[...])
        hid_ref[q] = swish(pre_ref[q])
        to = jnp.where(j < 3, n_groups, j - 3)
        vg = norm(y_ref[q] + par_ref[0][1:2], par_ref[0])
        far_vg_ref[pl.ds(pl.multiple_of(to * ROWS, ROWS), ROWS), :] = vg.astype(bf16)

    def message_step(j, p):
        q = 1 - p
        y_ref[p] = dot(hid_ref[p], wo_ref[3])
        for u in range(GROUP):
            source = slot(j * GROUP + u)[2]
            sender = jnp.where(source >= 1 << 9, block(far_vg_ref, source & 0x1FF), block(vgt_ref, source & 0xFF))
            lhs_ref[p, u * BATCH:(u + 1) * BATCH] = sender
        pre_ref[p] = dot(lhs_ref[p], wmid_ref[...])
        for u in range(GROUP):
            t = slot((j - 1) * GROUP + u)[0]
            at = slice(u * BATCH, (u + 1) * BATCH)
            hid_ref[q, at] = swish(pre_ref[q, at] + lp_ref[pl.ds(t, 1), :])
        for u in range(GROUP):
            t, node = slot((j - 3) * GROUP + u)[:2]
            upd = scale(y_ref[q, u * BATCH:(u + 1) * BATCH] + par[1:2]) * par[2:3]
            new = (upd + el_ref[pl.ds(t, 1), :]).astype(bf16).astype(f32)
            at = pl.ds(pl.multiple_of(node * BATCH, BATCH), BATCH)
            acc_ref[at, :] = acc_ref[at, :] + new

    def run(step, n):
        def two(k, carry):
            step(2 * k, 0)
            step(2 * k + 1, 1)
            return carry

        groups = (n + GROUP - 1) // GROUP
        lax.fori_loop(0, jnp.where(groups > 0, (groups + 4) // 2, 0), two, 0)

    run(embed_step, n_far)
    run(message_step, n_all)

    vm = vm_ref[...]
    n_rows = NODES * BATCH
    par = par_ref[4]
    agg = acc_ref[:n_rows].astype(bf16)
    base = dot(vm.astype(bf16), wnode_ref[:LAT]) + par[0:1]
    pre = dot(agg, wnode_ref[LAT:]).reshape(NODES, BATCH, LAT) + base[:, None, :]
    upd = finish(0.5 * pre.reshape(n_rows, LAT), wo_ref[4], par)
    out = (upd.reshape(NODES, BATCH, LAT) + vm[:, None, :]).reshape(n_rows, LAT).astype(bf16)
    mesh_ref[...] = dot(flip_matrix(n_rows, BATCH), out).astype(bf16).reshape(BATCH, NODES, LAT)
    for copy in copies:
        copy.wait()


def solution(mesh):
    n_lat, n_lon = mesh.shape['lat'], mesh.shape['lon']

    def cell_step(grid_in, mesh_in, edge_in, senders, edge_mask, w_grid, w_mesh, w_edge, w_msg, w_node, w_gupd, w_out, bias_gain):
        vmem = pl.BlockSpec(memory_space=pltpu.VMEM)
        smem = pl.BlockSpec(memory_space=pltpu.SMEM)
        hbm = pl.BlockSpec(memory_space=pltpu.HBM)
        loaded = [grid_in, mesh_in.T, edge_in.transpose(0, 2, 1), senders, edge_mask, w_grid, w_mesh, w_edge, w_msg, w_gupd, w_out, bias_gain]
        pin = lambda x: pltpu.with_memory_space_constraint(x, pltpu.HBM)
        own = pl.pallas_call(
            functools.partial(own_kernel, n_lat, n_lon),
            name='own',
            out_shape=[
                pltpu.VMEM((ROWS * CELL, LAT), bf16),
                pltpu.VMEM((CELL, BATCH, CELL, LAT), bf16),
                pltpu.VMEM((BLOCKS * BATCH, LANES), bf16),
                pltpu.VMEM((NSLOT, LAT), f32),
                pltpu.VMEM((NSLOT, LAT), f32),
                pltpu.VMEM((NODES, LAT), f32),
                pltpu.VMEM((4 * NODES, SLOTS), i32),
            ],
            in_specs=[hbm] * 12,
            out_specs=[vmem] * 7,
            scratch_shapes=[
                *[pltpu.VMEM(a.shape, a.dtype) for a in loaded],
                pltpu.VMEM((ROWS * CELL, 256), bf16),
                pltpu.VMEM((256, LAT), bf16),
                pltpu.VMEM((UNROLL * ROWS, LAT), bf16),
                pltpu.VMEM((BLOCKS * BATCH, LANES), bf16),
                pltpu.VMEM((BLOCKS * BATCH, LANES), bf16),
                pltpu.SemaphoreType.DMA((12,)),
                pltpu.SemaphoreType.DMA((8,)),
                pltpu.SemaphoreType.DMA((8,)),
            ],
            compiler_params=pltpu.CompilerParams(vmem_limit_bytes=20 << 20, collective_id=0, has_side_effects=True),
            cost_estimate=pl.CostEstimate(flops=10 * 10**9, bytes_accessed=16 << 20, transcendentals=0),
        )(*map(pin, loaded))
        vgt, gout, rx, lp, el, vm, code = own

        mesh_out, grid_out = pl.pallas_call(
            slot_kernel,
            name='slots',
            out_shape=[jax.ShapeDtypeStruct((BATCH, NODES, LAT), bf16), jax.ShapeDtypeStruct((BATCH, CELL, CELL, LAT), bf16)],
            in_specs=[smem] + [vmem] * 11,
            out_specs=[vmem, hbm],
            scratch_shapes=[
                pltpu.VMEM((256, LAT), bf16),
                pltpu.VMEM((LAT, LAT), bf16),
                pltpu.VMEM((2, ROWS, LAT), bf16),
                pltpu.VMEM((2, ROWS, LAT), f32),
                pltpu.VMEM((2, ROWS, LAT), bf16),
                pltpu.VMEM((2, ROWS, LAT), f32),
                pltpu.VMEM((NSLOT * BATCH + 3 * ROWS, LAT), bf16),
                pltpu.VMEM(((NODES + 1) * BATCH, LAT), f32),
                pltpu.SMEM((LIST + 2 * FRONT,), i32),
                pltpu.SMEM((LIST,), i32),
                pltpu.SemaphoreType.DMA((CELL,)),
            ],
            compiler_params=pltpu.CompilerParams(vmem_limit_bytes=24 << 20),
            cost_estimate=pl.CostEstimate(flops=10 * 10**9, bytes_accessed=16 << 20, transcendentals=0),
        )(code, vgt, gout, rx, lp, el, vm, w_grid, w_msg, w_node, w_out, bias_gain)
        return mesh_out, grid_out

    grid_spec = P('dp', 'lat', 'lon', None)
    node_spec = P(('lat', 'lon'), None)
    slot_spec = P(('lat', 'lon'), None, None)
    rep = P()
    in_specs = (grid_spec, node_spec, slot_spec, node_spec, node_spec) + (rep,) * 8
    out_specs = (P('dp', ('lat', 'lon'), None), grid_spec)
    return jax.shard_map(cell_step, mesh=mesh, in_specs=in_specs, out_specs=out_specs, check_vma=False)
```

```python
import functools

import jax
import jax.numpy as jnp
from jax import lax
from jax.experimental import pallas as pl
from jax.experimental.pallas import tpu as pltpu
from jax.sharding import PartitionSpec as P

REACH = 3
LN_EPS = 1e-5
CELL = 16
BATCH = 16
CIN = 186
LAT = 512
HALF = 64
LANES = 128
NODES = 8
SLOTS = 48
NSLOT = NODES * SLOTS
GROUP = 16
ROWS = GROUP * BATCH
EDGE_PTS, POLE_PTS, ROW_PTS = 2 * REACH, CELL - 2 * REACH, CELL
EDGE_BLK, POLE_BLK, ROW_BLK = EDGE_PTS * 3 // 2, POLE_PTS * 3 // 2, ROW_PTS * 3 // 2
BASE_EDGE = 0
BASE_POLE = BASE_EDGE + CELL * EDGE_BLK
BASE_NORTH = BASE_POLE + REACH * POLE_BLK
BASE_SOUTH = BASE_NORTH + REACH * ROW_BLK
BASE_CN = BASE_SOUTH + REACH * ROW_BLK
BASE_CS = BASE_CN + REACH * EDGE_BLK
BLOCKS = BASE_CS + REACH * EDGE_BLK
LIST = 512
FRONT = 3 * GROUP
UNROLL = 4
bf16, f32, i32 = jnp.bfloat16, jnp.float32, jnp.int32
MESH = pl.DeviceIdType.MESH


def dot(a, b):
    return jnp.dot(a, b, preferred_element_type=f32)


def dot_t(a, b):
    return lax.dot_general(a, b, (((0,), (0,)), ((), ())), preferred_element_type=f32)


def swish(h):
    return (h + h * jnp.tanh(h)).astype(bf16)


def scale(y):
    y = y - jnp.mean(y, axis=-1, keepdims=True)
    var = jnp.mean(y * y, axis=-1, keepdims=True)
    return y * lax.rsqrt(var + LN_EPS)


def norm(y, par):
    return scale(y) * par[2:3] + par[3:4]


def finish(half_pre, w2, par):
    return norm(dot(swish(half_pre), w2) + par[1:2], par)


def pack_hi(y):
    half = y.shape[0] // 2
    hi = y[:, LANES:]
    return y[:, :LANES].astype(bf16), (hi[:half] + pltpu.roll(hi[half:], HALF, 1)).astype(bf16)


def fill_embed(wpad_ref, wg_ref, b1):
    tile = CIN // BATCH * BATCH
    wpad_ref[tile:] = jnp.zeros((256 - tile, LAT), bf16)
    wpad_ref[:CIN] = wg_ref[...]
    b_hi = b1.astype(bf16)
    b_mid = (b1 - b_hi.astype(f32)).astype(bf16)
    b_lo = (b1 - b_hi.astype(f32) - b_mid.astype(f32)).astype(bf16)
    row = lax.broadcasted_iota(i32, (BATCH, LAT), 0) + tile
    edge = wpad_ref[tile:tile + BATCH].astype(f32)
    for k, part in enumerate((b_hi, b_mid, b_lo)):
        edge = jnp.where(row == CIN + k, part.astype(f32), edge)
    wpad_ref[tile:tile + BATCH] = edge.astype(bf16)
    wpad_ref[...] = wpad_ref[...] * bf16(0.5)


def slot_codes(senders, live, lat, lon):
    t = lax.broadcasted_iota(i32, senders.shape, 0) * SLOTS + lax.broadcasted_iota(i32, senders.shape, 1)
    row, col = senders >> 5, senders & 31
    r = row - lat * CELL
    c = col & (CELL - 1)
    own_lon = (col >> 4) == lon
    in_band = (r >= 0) & (r < CELL)
    local = in_band & own_lon
    is_edge = (c < REACH) | (c >= CELL - REACH)
    pole = in_band & jnp.logical_not(is_edge)
    e = jnp.where(c < REACH, c, c - (CELL - EDGE_PTS))
    north = r < 0
    band_base = jnp.where(north, jnp.where(own_lon, BASE_NORTH, BASE_CN), jnp.where(own_lon, BASE_SOUTH, BASE_CS))
    base = jnp.where(in_band, jnp.where(pole, BASE_POLE, BASE_EDGE), band_base)
    pole_line = jnp.where(lat == 0, r, r - (CELL - REACH))
    line = jnp.where(in_band, jnp.where(pole, pole_line, r), jnp.where(north, r + REACH, r - CELL))
    q = jnp.where(pole, c - REACH, jnp.where(own_lon, c, e))
    half = jnp.where(pole, POLE_PTS // 2, jnp.where(own_lon, ROW_PTS // 2, EDGE_PTS // 2))
    start = base + line * (half * 3)
    upper = jnp.where(q >= half, 1, 0)
    lo = start + q
    hi = start + half * 2 + q - upper * half
    n_slots = senders.shape[1]

    def ahead(flag):
        value = flag.astype(f32)
        earlier = lax.broadcasted_iota(i32, (n_slots, n_slots), 0) < lax.broadcasted_iota(i32, (n_slots, n_slots), 1)
        inside = dot(value.astype(bf16), jnp.where(earlier, 1.0, 0.0).astype(bf16))
        total = jnp.broadcast_to(jnp.sum(value, axis=1, keepdims=True), (senders.shape[0], LANES)).astype(bf16)
        earlier = lax.broadcasted_iota(i32, (NODES, NODES), 1) < lax.broadcasted_iota(i32, (NODES, NODES), 0)
        return (inside + dot(jnp.where(earlier, 1.0, 0.0).astype(bf16), total)[:, :n_slots]).astype(i32)

    active = live == 1
    far = active & jnp.logical_not(local)
    eye = lax.broadcasted_iota(i32, (n_slots, n_slots), 0) == lax.broadcasted_iota(i32, (n_slots, n_slots), 1)
    point = lax.broadcasted_iota(i32, (n_slots, LIST), 1).astype(f32)
    wanted = jnp.where(far, lo, LIST - 1).astype(f32)
    hits = []
    for n in range(NODES):
        column = jnp.sum(jnp.where(eye, wanted[n:n + 1], 0.0), axis=1, keepdims=True)
        hits.append(jnp.where(point == column, 1.0, 0.0))
    used = jnp.sum(functools.reduce(jnp.maximum, hits), axis=0, keepdims=True)
    lanes = lax.broadcasted_iota(i32, (NODES, LIST), 1)
    used = jnp.where((jnp.broadcast_to(used, (NODES, LIST)) > 0) & (lanes < LIST - 1), 1.0, 0.0)
    earlier = lax.broadcasted_iota(i32, (LIST, LIST), 0) < lax.broadcasted_iota(i32, (LIST, LIST), 1)
    rank = dot(used.astype(bf16), jnp.where(earlier, 1.0, 0.0).astype(bf16))[0:1]
    far_at = []
    for hit in hits:
        column = jnp.sum(hit * rank, axis=1, keepdims=True)
        far_at.append(jnp.sum(jnp.where(eye, column, 0.0), axis=0, keepdims=True))
    far_at = jnp.concatenate(far_at, axis=0).astype(i32)
    node = lax.broadcasted_iota(i32, senders.shape, 0)
    source = jnp.where(local, r * CELL + c, far_at + (1 << 9))
    word = t | (node << 9) | (source << 13)
    halo = lo | (hi << 9) | (upper << 18)
    place = jnp.where(active, ahead(active) + FRONT, LIST - 1) | (jnp.where(far, far_at, LIST - 1) << 16)
    count = jnp.sum(active.astype(f32)).astype(i32), jnp.sum(used[0:1]).astype(i32)
    return word, halo, place, count


def flip_matrix(rows, inner):
    a = lax.broadcasted_iota(i32, (rows, rows), 0)
    b = lax.broadcasted_iota(i32, (rows, rows), 1)
    outer = rows // inner
    return jnp.where(a // outer + a % outer * inner == b, 1.0, 0.0).astype(bf16)


def own_kernel(n_lat, n_lon, x_hbm, mesh_hbm, edge_hbm, send_hbm, mask_hbm, wg_hbm, wm_hbm, we_hbm, wmsg_hbm, wgu_hbm, wo_hbm, par_hbm,
               vgt_ref, gout_ref, rx_out_ref, lp_ref, el_ref, vm_ref, code_ref,
               x_ref, mesh_ref, edge_ref, send_ref, mask_ref, wg_ref, wm_ref, we_ref, wmsg_ref, wgu_ref, wo_ref, par_ref, xpad_ref, wpad_ref, pre_ref, hid_ref, y_ref, vg_ref, tx_ref, rx_ref,
               in_sem, send_sem, recv_sem):
    dp = lax.axis_index('dp')
    lon = lax.axis_index('lon')
    lat = lax.axis_index('lat')
    across = (dp, (lon + 1) % n_lon, lat)
    up = (dp, lon, lat - 1)
    down = (dp, lon, lat + 1)
    has_up = lat > 0
    has_down = lat < n_lat - 1
    at_pole = jnp.logical_or(lat == 0, lat == n_lat - 1)

    loads = [(x_hbm, x_ref), (wg_hbm, wg_ref), (par_hbm, par_ref), (wo_hbm, wo_ref), (wgu_hbm, wgu_ref), (wm_hbm, wm_ref),
             (we_hbm, we_ref), (wmsg_hbm, wmsg_ref), (mesh_hbm, mesh_ref), (edge_hbm, edge_ref), (send_hbm, send_ref), (mask_hbm, mask_ref)]
    loads = [pltpu.make_async_copy(a, b, in_sem.at[k]) for k, (a, b) in enumerate(loads)]
    for load in loads:
        load.start()

    barrier = pltpu.get_barrier_semaphore()
    pl.semaphore_signal(barrier, inc=1, device_id=across, device_id_type=MESH)

    @pl.when(has_up)
    def _():
        pl.semaphore_signal(barrier, inc=1, device_id=up, device_id_type=MESH)

    @pl.when(has_down)
    def _():
        pl.semaphore_signal(barrier, inc=1, device_id=down, device_id_type=MESH)

    def send(k, src_ref, src, dst, count, to):
        return pltpu.make_async_remote_copy(
            src_ref=src_ref.at[pl.ds(src * BATCH, count * BATCH)], dst_ref=rx_ref.at[pl.ds(dst * BATCH, count * BATCH)],
            send_sem=send_sem.at[k], recv_sem=recv_sem.at[k], device_id=to, device_id_type=MESH)

    e_top = send(0, tx_ref, BASE_EDGE, BASE_EDGE, REACH * EDGE_BLK, across)
    e_low = send(1, tx_ref, BASE_EDGE + (CELL - REACH) * EDGE_BLK, BASE_EDGE + (CELL - REACH) * EDGE_BLK, REACH * EDGE_BLK, across)
    e_mid = send(2, tx_ref, BASE_EDGE + REACH * EDGE_BLK, BASE_EDGE + REACH * EDGE_BLK, (CELL - 2 * REACH) * EDGE_BLK, across)
    polar = send(3, tx_ref, BASE_POLE, BASE_POLE, REACH * POLE_BLK, across)
    to_up = send(4, tx_ref, BASE_SOUTH, BASE_SOUTH, REACH * ROW_BLK, up)
    to_down = send(5, tx_ref, BASE_NORTH, BASE_NORTH, REACH * ROW_BLK, down)
    fwd_up = send(6, rx_ref, BASE_EDGE, BASE_CS, REACH * EDGE_BLK, up)
    fwd_down = send(7, rx_ref, BASE_EDGE + (CELL - REACH) * EDGE_BLK, BASE_CN, REACH * EDGE_BLK, down)

    flip = flip_matrix(ROWS, CELL)
    flip_edge = jnp.concatenate([flip[:REACH * BATCH], flip[(CELL - REACH) * BATCH:]], axis=0)
    lane = lax.broadcasted_iota(i32, (ROWS, LANES), 1) + LANES
    ones = jnp.where((lane >= CIN) & (lane < CIN + 3), 1.0, 0.0).astype(bf16)
    loads[0].wait()

    def put(row, lo, hi):
        n = lo.shape[0]
        tx_ref[row * BATCH:row * BATCH + n] = lo
        tx_ref[row * BATCH + n:row * BATCH + n * 3 // 2] = hi

    def pad_row(i):
        at = slice(i * ROWS, (i + 1) * ROWS)
        xpad_ref[at, LANES:] = ones
        xpad_ref[at, :CIN] = x_ref[:, i].reshape(ROWS, CIN)
        return xpad_ref[at, :]

    for k in range(REACH):
        inner = []
        for base, first in ((BASE_SOUTH, 0), (BASE_NORTH, CELL - REACH)):
            full = dot(flip, pad_row(first + k))
            edge = jnp.concatenate([full[:REACH * BATCH], full[(CELL - REACH) * BATCH:]], axis=0)
            put(BASE_EDGE + (first + k) * EDGE_BLK, *pack_hi(edge))
            put(base + k * ROW_BLK, *pack_hi(full))
            inner.append(full[REACH * BATCH:(CELL - REACH) * BATCH])
        put(BASE_POLE + k * POLE_BLK, *pack_hi(jnp.where(lat == 0, *inner)))
    pl.semaphore_wait(barrier, 1 + has_up.astype(i32) + has_down.astype(i32))
    e_top.start()
    e_low.start()
    pl.when(has_up)(to_up.start)
    pl.when(has_down)(to_down.start)
    pl.when(at_pole)(polar.start)

    for i in range(REACH, CELL - REACH):
        put(BASE_EDGE + i * EDGE_BLK, *pack_hi(dot(flip_edge, pad_row(i))))
    e_mid.start()

    for load in loads[1:]:
        load.wait()
    fill_embed(wpad_ref, wg_ref, par_ref[0][0:1])
    wgu_ref[...] = wgu_ref[...] * bf16(0.5)

    def rows_at(j):
        return pl.ds(j * ROWS if isinstance(j, int) else pl.multiple_of(j * ROWS, ROWS), ROWS)

    def embed_step(j, p, entering=True, leaving=(True, True, True)):
        q = 1 - p
        if leaving[1]:
            y_ref[p] = dot(hid_ref[p], wo_ref[0])
        if entering:
            pre_ref[p] = dot(xpad_ref[rows_at(j), :], wpad_ref[...])
        if leaving[0]:
            hid_ref[q] = swish(pre_ref[q])
        if leaving[2]:
            vg_ref[rows_at(j - 3), :] = norm(y_ref[q] + par_ref[0][1:2], par_ref[0]).astype(bf16)

    def update_step(j, p, entering=True, leaving=(True, True, True)):
        q = 1 - p
        if leaving[1]:
            y_ref[2 + p] = dot(hid_ref[2 + p], wo_ref[5])
        if entering:
            vg = vg_ref[rows_at(j), :]
            pre_ref[2 + p] = dot(vg, wgu_ref[...])
            vgt_ref[rows_at(j), :] = dot(flip, vg).astype(bf16)
        if leaving[0]:
            hid_ref[2 + q] = swish(pre_ref[2 + q] + 0.5 * par_ref[5][0:1])
        if leaving[2]:
            upd = norm(y_ref[2 + q] + par_ref[5][1:2], par_ref[5])
            gout_ref[j - 3] = (vg_ref[rows_at(j - 3), :].astype(f32) + upd).astype(bf16).reshape(BATCH, CELL, LAT)

    def fill(step):
        step(0, 0, True, (False, False, False))
        step(1, 1, True, (True, False, False))
        step(2, 0, True, (True, True, False))

    def drain(step):
        step(CELL, 0, False, (True, True, True))
        step(CELL + 1, 1, False, (False, True, True))
        step(CELL + 2, 0, False, (False, False, True))

    def run(step, first, trips):
        def some(k, carry):
            for u in range(UNROLL):
                step(first + k * UNROLL + u, (first + u) % 2)
            return carry

        lax.fori_loop(0, trips, some, 0)

    fill(embed_step)
    run(embed_step, 3, 12 // UNROLL)
    embed_step(CELL - 1, 1)
    drain(embed_step)
    fill(update_step)
    run(update_step, 3, 4 // UNROLL)
    e_top.wait_recv()
    e_low.wait_recv()
    pl.when(has_up)(fwd_up.start)
    pl.when(has_down)(fwd_down.start)
    run(update_step, 7, 8 // UNROLL)
    update_step(CELL - 1, 1)
    drain(update_step)

    word, halo, place, counts = slot_codes(send_ref[...], mask_ref[...], lat, lon)
    code_ref[0:NODES] = word
    code_ref[NODES:2 * NODES] = halo
    code_ref[2 * NODES:3 * NODES] = place
    code_ref[3 * NODES:] = jnp.where(lax.broadcasted_iota(i32, (NODES, SLOTS), 1) == 0, counts[0], counts[1])
    par = par_ref[1]
    vm = finish(0.5 * (dot_t(mesh_ref[...], wm_ref[...]) + par[0:1]), wo_ref[1], par).astype(bf16)
    vm_ref[...] = vm.astype(f32)
    par = par_ref[2]
    el = finish(0.5 * (jnp.concatenate([dot_t(edge_ref[n], we_ref[...]) for n in range(NODES)], axis=0) + par[0:1]), wo_ref[2], par).astype(bf16)
    par = par_ref[3]
    el_ref[...] = el.astype(f32) + par[3:4]
    vm_proj = dot(vm, wmsg_ref[2 * LAT:]) + par[0:1]
    lp = dot(el, wmsg_ref[:LAT]).reshape(NODES, SLOTS, LAT) + vm_proj[:, None, :]
    lp_ref[...] = 0.5 * lp.reshape(NSLOT, LAT)

    e_mid.wait_recv()
    pl.when(at_pole)(polar.wait_recv)

    @pl.when(has_down)
    def _():
        to_up.wait_recv()
        fwd_up.wait_recv()

    @pl.when(has_up)
    def _():
        to_down.wait_recv()
        fwd_down.wait_recv()

    rx_out_ref[...] = rx_ref[...]
    e_top.wait_send()
    e_low.wait_send()
    e_mid.wait_send()
    pl.when(at_pole)(polar.wait_send)

    @pl.when(has_up)
    def _():
        to_up.wait_send()
        fwd_up.wait_send()

    @pl.when(has_down)
    def _():
        to_down.wait_send()
        fwd_down.wait_send()


def slot_kernel(code_ref, vgt_ref, gout_ref, rx_ref, lp_ref, el_ref, vm_ref, wg_ref, wmsg_ref, wnode_ref, wo_ref, par_ref,
                mesh_ref, grid_ref, wpad_ref, wmid_ref, lhs_ref, pre_ref, hid_ref, y_ref, far_vg_ref, acc_ref, all_ref, far_ref, sem):
    copies = [pltpu.make_async_copy(gout_ref.at[i], grid_ref.at[:, i], sem.at[i]) for i in range(CELL)]
    for copy in copies:
        copy.start()
    fill_embed(wpad_ref, wg_ref, par_ref[0][0:1])
    wmid_ref[...] = wmsg_ref[LAT:2 * LAT] * bf16(0.5)
    acc_ref[...] = jnp.zeros_like(acc_ref)

    n_all, n_far = code_ref[3 * NODES, 0], code_ref[3 * NODES, 1]

    def fill_lists(node, carry):
        for k in range(SLOTS):
            place = code_ref[2 * NODES + node, k]
            all_ref[place & 0xFFFF] = code_ref[node, k]
            far_ref[place >> 16] = code_ref[NODES + node, k]
        return carry

    lax.fori_loop(0, NODES, fill_lists, 0)
    for k in range(FRONT):
        all_ref[k] = NODES << 9
    for k in range(4 * GROUP):
        all_ref[FRONT + n_all + k] = NODES << 9
    for k in range(4 * GROUP):
        far_ref[n_far + k] = 0

    def block(ref, index):
        return ref[pl.ds(pl.multiple_of(index * BATCH, BATCH), BATCH), :]

    par = par_ref[3]

    n_groups = NSLOT // GROUP

    def slot(at):
        word = all_ref[FRONT + at]
        return word & 0x1FF, (word >> 9) & 0xF, word >> 13

    def embed_step(j, p):
        q = 1 - p
        y_ref[p] = dot(hid_ref[p], wo_ref[0])
        for u in range(GROUP):
            halo = far_ref[j * GROUP + u]
            lo, hi, upper = halo & 0x1FF, (halo >> 9) & 0x1FF, halo >> 18
            dst = slice(u * BATCH, (u + 1) * BATCH)
            lhs_ref[p, dst, :LANES] = block(rx_ref, lo)
            high = block(rx_ref, hi).astype(f32)
            high = jnp.where(upper == 1, pltpu.roll(high, HALF, 1), high)
            lhs_ref[p, dst, LANES:256] = high.astype(bf16)
        pre_ref[p] = dot(lhs_ref[p, :, :256], wpad_ref[...])
        hid_ref[q] = swish(pre_ref[q])
        to = jnp.where(j < 3, n_groups, j - 3)
        vg = norm(y_ref[q] + par_ref[0][1:2], par_ref[0])
        far_vg_ref[pl.ds(pl.multiple_of(to * ROWS, ROWS), ROWS), :] = vg.astype(bf16)

    def message_step(j, p):
        q = 1 - p
        y_ref[p] = dot(hid_ref[p], wo_ref[3])
        for u in range(GROUP):
            source = slot(j * GROUP + u)[2]
            sender = jnp.where(source >= 1 << 9, block(far_vg_ref, source & 0x1FF), block(vgt_ref, source & 0xFF))
            lhs_ref[p, u * BATCH:(u + 1) * BATCH] = sender
        pre_ref[p] = dot(lhs_ref[p], wmid_ref[...])
        for u in range(GROUP):
            t = slot((j - 1) * GROUP + u)[0]
            at = slice(u * BATCH, (u + 1) * BATCH)
            hid_ref[q, at] = swish(pre_ref[q, at] + lp_ref[pl.ds(t, 1), :])
        for u in range(GROUP):
            t, node = slot((j - 3) * GROUP + u)[:2]
            upd = scale(y_ref[q, u * BATCH:(u + 1) * BATCH] + par[1:2]) * par[2:3]
            new = (upd + el_ref[pl.ds(t, 1), :]).astype(bf16).astype(f32)
            at = pl.ds(pl.multiple_of(node * BATCH, BATCH), BATCH)
            acc_ref[u % 4, at, :] = acc_ref[u % 4, at, :] + new

    def run(step, n):
        steps = jnp.where(n > 0, (n + GROUP - 1) // GROUP + 3, 0)
        fours = steps // 4

        def four(k, carry):
            for u in range(4):
                step(4 * k + u, u % 2)
            return carry

        def two(k, carry):
            step(2 * k, 0)
            step(2 * k + 1, 1)
            return carry

        lax.fori_loop(0, fours, four, 0)
        lax.fori_loop(2 * fours, (steps + 1) // 2, two, 0)

    run(embed_step, n_far)
    run(message_step, n_all)

    vm = vm_ref[...]
    n_rows = NODES * BATCH
    par = par_ref[4]
    agg = ((acc_ref[0, :n_rows] + acc_ref[1, :n_rows]) + (acc_ref[2, :n_rows] + acc_ref[3, :n_rows])).astype(bf16)
    base = dot(vm.astype(bf16), wnode_ref[:LAT]) + par[0:1]
    pre = dot(agg, wnode_ref[LAT:]).reshape(NODES, BATCH, LAT) + base[:, None, :]
    upd = finish(0.5 * pre.reshape(n_rows, LAT), wo_ref[4], par)
    out = (upd.reshape(NODES, BATCH, LAT) + vm[:, None, :]).reshape(n_rows, LAT).astype(bf16)
    mesh_ref[...] = dot(flip_matrix(n_rows, BATCH), out).astype(bf16).reshape(BATCH, NODES, LAT)
    for copy in copies:
        copy.wait()


def solution(mesh):
    n_lat, n_lon = mesh.shape['lat'], mesh.shape['lon']

    def cell_step(grid_in, mesh_in, edge_in, senders, edge_mask, w_grid, w_mesh, w_edge, w_msg, w_node, w_gupd, w_out, bias_gain):
        vmem = pl.BlockSpec(memory_space=pltpu.VMEM)
        smem = pl.BlockSpec(memory_space=pltpu.SMEM)
        hbm = pl.BlockSpec(memory_space=pltpu.HBM)
        loaded = [grid_in, mesh_in.T, edge_in.transpose(0, 2, 1), senders, edge_mask, w_grid, w_mesh, w_edge, w_msg, w_gupd, w_out, bias_gain]
        pin = lambda x: pltpu.with_memory_space_constraint(x, pltpu.HBM)
        own = pl.pallas_call(
            functools.partial(own_kernel, n_lat, n_lon),
            name='own',
            out_shape=[
                pltpu.VMEM((ROWS * CELL, LAT), bf16),
                pltpu.VMEM((CELL, BATCH, CELL, LAT), bf16),
                pltpu.VMEM((BLOCKS * BATCH, LANES), bf16),
                pltpu.VMEM((NSLOT, LAT), f32),
                pltpu.VMEM((NSLOT, LAT), f32),
                pltpu.VMEM((NODES, LAT), f32),
                pltpu.VMEM((4 * NODES, SLOTS), i32),
            ],
            in_specs=[hbm] * 12,
            out_specs=[vmem] * 7,
            scratch_shapes=[
                *[pltpu.VMEM(a.shape, a.dtype) for a in loaded],
                pltpu.VMEM((ROWS * CELL, 256), bf16),
                pltpu.VMEM((256, LAT), bf16),
                pltpu.VMEM((4, ROWS, LAT), f32),
                pltpu.VMEM((4, ROWS, LAT), bf16),
                pltpu.VMEM((4, ROWS, LAT), f32),
                pltpu.VMEM((CELL * ROWS, LAT), bf16),
                pltpu.VMEM((BLOCKS * BATCH, LANES), bf16),
                pltpu.VMEM((BLOCKS * BATCH, LANES), bf16),
                pltpu.SemaphoreType.DMA((12,)),
                pltpu.SemaphoreType.DMA((8,)),
                pltpu.SemaphoreType.DMA((8,)),
            ],
            compiler_params=pltpu.CompilerParams(vmem_limit_bytes=28 << 20, collective_id=0, has_side_effects=True),
            cost_estimate=pl.CostEstimate(flops=10 * 10**9, bytes_accessed=16 << 20, transcendentals=0),
        )(*map(pin, loaded))
        vgt, gout, rx, lp, el, vm, code = own

        mesh_out, grid_out = pl.pallas_call(
            slot_kernel,
            name='slots',
            out_shape=[jax.ShapeDtypeStruct((BATCH, NODES, LAT), bf16), jax.ShapeDtypeStruct((BATCH, CELL, CELL, LAT), bf16)],
            in_specs=[smem] + [vmem] * 11,
            out_specs=[vmem, hbm],
            scratch_shapes=[
                pltpu.VMEM((256, LAT), bf16),
                pltpu.VMEM((LAT, LAT), bf16),
                pltpu.VMEM((2, ROWS, LAT), bf16),
                pltpu.VMEM((2, ROWS, LAT), f32),
                pltpu.VMEM((2, ROWS, LAT), bf16),
                pltpu.VMEM((2, ROWS, LAT), f32),
                pltpu.VMEM((NSLOT * BATCH + 3 * ROWS, LAT), bf16),
                pltpu.VMEM((4, (NODES + 1) * BATCH, LAT), f32),
                pltpu.SMEM((LIST + 2 * FRONT,), i32),
                pltpu.SMEM((LIST,), i32),
                pltpu.SemaphoreType.DMA((CELL,)),
            ],
            compiler_params=pltpu.CompilerParams(vmem_limit_bytes=24 << 20),
            cost_estimate=pl.CostEstimate(flops=10 * 10**9, bytes_accessed=16 << 20, transcendentals=0),
        )(code, vgt, gout, rx, lp, el, vm, w_grid, w_msg, w_node, w_out, bias_gain)
        return mesh_out, grid_out

    grid_spec = P('dp', 'lat', 'lon', None)
    node_spec = P(('lat', 'lon'), None)
    slot_spec = P(('lat', 'lon'), None, None)
    rep = P()
    in_specs = (grid_spec, node_spec, slot_spec, node_spec, node_spec) + (rep,) * 8
    out_specs = (P('dp', ('lat', 'lon'), None), grid_spec)
    return jax.shard_map(cell_step, mesh=mesh, in_specs=in_specs, out_specs=out_specs, check_vma=False)
```

```python
import functools

import jax
import jax.numpy as jnp
from jax import lax
from jax.experimental import pallas as pl
from jax.experimental.pallas import tpu as pltpu
from jax.sharding import PartitionSpec as P

REACH = 3
LN_EPS = 1e-5
CELL = 16
BATCH = 16
CIN = 186
LAT = 512
HALF = 64
LANES = 128
NODES = 8
SLOTS = 48
NSLOT = NODES * SLOTS
GROUP = 16
ROWS = GROUP * BATCH
EDGE_PTS, POLE_PTS, ROW_PTS = 2 * REACH, CELL - 2 * REACH, CELL
EDGE_BLK, POLE_BLK, ROW_BLK = EDGE_PTS * 3 // 2, POLE_PTS * 3 // 2, ROW_PTS * 3 // 2
BASE_EDGE = 0
BASE_POLE = BASE_EDGE + CELL * EDGE_BLK
BASE_NORTH = BASE_POLE + REACH * POLE_BLK
BASE_SOUTH = BASE_NORTH + REACH * ROW_BLK
BASE_CN = BASE_SOUTH + REACH * ROW_BLK
BASE_CS = BASE_CN + REACH * EDGE_BLK
BLOCKS = BASE_CS + REACH * EDGE_BLK
LIST = 512
FRONT = 3 * GROUP
UNROLL = 4
bf16, f32, i32 = jnp.bfloat16, jnp.float32, jnp.int32
MESH = pl.DeviceIdType.MESH


def dot(a, b):
    return jnp.dot(a, b, preferred_element_type=f32)


def dot_t(a, b):
    return lax.dot_general(a, b, (((0,), (0,)), ((), ())), preferred_element_type=f32)


def swish(h):
    return (h + h * jnp.tanh(h)).astype(bf16)


def scale(y):
    y = y - jnp.mean(y, axis=-1, keepdims=True)
    var = jnp.mean(y * y, axis=-1, keepdims=True)
    return y * lax.rsqrt(var + LN_EPS)


def norm(y, par):
    return scale(y) * par[2:3] + par[3:4]


def finish(half_pre, w2, par):
    return norm(dot(swish(half_pre), w2) + par[1:2], par)


def pack_hi(y):
    half = y.shape[0] // 2
    hi = y[:, LANES:]
    return y[:, :LANES].astype(bf16), (hi[:half] + pltpu.roll(hi[half:], HALF, 1)).astype(bf16)


def fill_embed(wpad_ref, wg_ref, b1):
    tile = CIN // BATCH * BATCH
    wpad_ref[tile:] = jnp.zeros((256 - tile, LAT), bf16)
    wpad_ref[:CIN] = wg_ref[...]
    b_hi = b1.astype(bf16)
    b_mid = (b1 - b_hi.astype(f32)).astype(bf16)
    b_lo = (b1 - b_hi.astype(f32) - b_mid.astype(f32)).astype(bf16)
    row = lax.broadcasted_iota(i32, (BATCH, LAT), 0) + tile
    edge = wpad_ref[tile:tile + BATCH].astype(f32)
    for k, part in enumerate((b_hi, b_mid, b_lo)):
        edge = jnp.where(row == CIN + k, part.astype(f32), edge)
    wpad_ref[tile:tile + BATCH] = edge.astype(bf16)
    wpad_ref[...] = wpad_ref[...] * bf16(0.5)


def slot_lists(senders, live, lat, lon):
    row, col = senders >> 5, senders & 31
    r = row - lat * CELL
    c = col & (CELL - 1)
    own_lon = (col >> 4) == lon
    in_band = (r >= 0) & (r < CELL)
    local = in_band & own_lon
    is_edge = (c < REACH) | (c >= CELL - REACH)
    pole = in_band & jnp.logical_not(is_edge)
    e = jnp.where(c < REACH, c, c - (CELL - EDGE_PTS))
    north = r < 0
    band_base = jnp.where(north, jnp.where(own_lon, BASE_NORTH, BASE_CN), jnp.where(own_lon, BASE_SOUTH, BASE_CS))
    base = jnp.where(in_band, jnp.where(pole, BASE_POLE, BASE_EDGE), band_base)
    pole_line = jnp.where(lat == 0, r, r - (CELL - REACH))
    line = jnp.where(in_band, jnp.where(pole, pole_line, r), jnp.where(north, r + REACH, r - CELL))
    q = jnp.where(pole, c - REACH, jnp.where(own_lon, c, e))
    half = jnp.where(pole, POLE_PTS // 2, jnp.where(own_lon, ROW_PTS // 2, EDGE_PTS // 2))
    start = base + line * (half * 3)
    upper = jnp.where(q >= half, 1, 0)
    lo = start + q
    hi = start + half * 2 + q - upper * half
    n_slots = senders.shape[1]

    def ahead(flag):
        value = flag.astype(f32)
        earlier = lax.broadcasted_iota(i32, (n_slots, n_slots), 0) < lax.broadcasted_iota(i32, (n_slots, n_slots), 1)
        inside = dot(value.astype(bf16), jnp.where(earlier, 1.0, 0.0).astype(bf16))
        total = jnp.broadcast_to(jnp.sum(value, axis=1, keepdims=True), (senders.shape[0], LANES)).astype(bf16)
        earlier = lax.broadcasted_iota(i32, (NODES, NODES), 1) < lax.broadcasted_iota(i32, (NODES, NODES), 0)
        return inside + dot(jnp.where(earlier, 1.0, 0.0).astype(bf16), total)[:, :n_slots]

    active = live == 1
    far = active & jnp.logical_not(local)
    eye = lax.broadcasted_iota(i32, (n_slots, n_slots), 0) == lax.broadcasted_iota(i32, (n_slots, n_slots), 1)
    point = lax.broadcasted_iota(i32, (n_slots, LIST), 1).astype(f32)
    wanted = jnp.where(far, lo, LIST - 1).astype(f32)
    hits = []
    for n in range(NODES):
        column = jnp.sum(jnp.where(eye, wanted[n:n + 1], 0.0), axis=1, keepdims=True)
        hits.append(jnp.where(point == column, 1.0, 0.0))
    used = jnp.sum(functools.reduce(jnp.maximum, hits), axis=0, keepdims=True)
    lanes = lax.broadcasted_iota(i32, (NODES, LIST), 1)
    used = jnp.where((jnp.broadcast_to(used, (NODES, LIST)) > 0) & (lanes < LIST - 1), 1.0, 0.0)
    earlier = lax.broadcasted_iota(i32, (LIST, LIST), 0) < lax.broadcasted_iota(i32, (LIST, LIST), 1)
    rank = dot(used.astype(bf16), jnp.where(earlier, 1.0, 0.0).astype(bf16))[0:1]
    far_at = []
    for hit in hits:
        column = jnp.sum(hit * rank, axis=1, keepdims=True)
        far_at.append(jnp.sum(jnp.where(eye, column, 0.0), axis=0, keepdims=True))
    far_at = jnp.concatenate(far_at, axis=0)
    all_at = jnp.where(active, ahead(active) + FRONT, LIST - 1).astype(f32)
    to_far = jnp.where(far, far_at, LIST - 1.0)
    slot_id = lax.broadcasted_iota(i32, senders.shape, 1)

    def gather(places, fields):
        total = jnp.zeros((8, LIST), f32)
        for n in range(NODES):
            column = jnp.sum(jnp.where(eye, places[n:n + 1], 0.0), axis=1, keepdims=True)
            rows = [f[n:n + 1].astype(f32) for f in fields]
            rows = jnp.concatenate(rows + [jnp.zeros((8 - len(rows), n_slots), f32)], axis=0).astype(bf16)
            total = total + dot(rows, jnp.where(point == column, 1.0, 0.0).astype(bf16))
        return total

    one = jnp.ones(senders.shape, f32)
    node = lax.broadcasted_iota(i32, senders.shape, 0)
    near_row = jnp.where(local, r * CELL + c, 0)
    got = gather(all_at, [slot_id, node, near_row, jnp.where(far, far_at, 0.0), far.astype(f32), one]).astype(i32)
    lane = lax.broadcasted_iota(i32, (1, LIST), 1)
    valid = (got[5:6] == 1) & (lane < LIST - 1)
    n_all = jnp.sum(active.astype(f32)).astype(i32)
    n_far = jnp.sum(used[0:1]).astype(i32)
    main = [jnp.where(valid, got[1:2] * SLOTS + got[0:1], 0), jnp.where(valid, got[1:2], NODES) * BATCH,
            got[2:3] * BATCH, got[3:4] * BATCH, got[4:5]]
    main = [jnp.where(valid, m, 0) if k != 1 else m for k, m in enumerate(main)]
    counts = jnp.where(lane == 0, n_all, n_far)
    got = gather(to_far, [lo >> 4, lo & 15, hi >> 4, hi & 15, upper, one])
    got = (got / jnp.maximum(got[5:6], 1.0) + 0.5).astype(i32)
    valid = lane < n_far
    halo = [jnp.where(valid, v, 0) for v in ((got[0:1] * 16 + got[1:2]) * BATCH, (got[2:3] * 16 + got[3:4]) * BATCH, got[4:5])]
    zero = jnp.zeros((1, LIST), i32)
    return jnp.concatenate(main + [zero, zero, counts] + halo + [zero] * 5, axis=0)


def flip_matrix(rows, inner):
    a = lax.broadcasted_iota(i32, (rows, rows), 0)
    b = lax.broadcasted_iota(i32, (rows, rows), 1)
    outer = rows // inner
    return jnp.where(a // outer + a % outer * inner == b, 1.0, 0.0).astype(bf16)


def own_kernel(n_lat, n_lon, x_hbm, mesh_hbm, edge_hbm, send_hbm, mask_hbm, wg_hbm, wm_hbm, we_hbm, wmsg_hbm, wgu_hbm, wo_hbm, par_hbm,
               vgt_ref, gout_ref, rx_out_ref, lp_ref, el_ref, vm_ref, code_ref,
               x_ref, mesh_ref, edge_ref, send_ref, mask_ref, wg_ref, wm_ref, we_ref, wmsg_ref, wgu_ref, wo_ref, par_ref, xpad_ref, wpad_ref, pre_ref, hid_ref, y_ref, vg_ref, tx_ref, rx_ref,
               in_sem, send_sem, recv_sem):
    dp = lax.axis_index('dp')
    lon = lax.axis_index('lon')
    lat = lax.axis_index('lat')
    across = (dp, (lon + 1) % n_lon, lat)
    up = (dp, lon, lat - 1)
    down = (dp, lon, lat + 1)
    has_up = lat > 0
    has_down = lat < n_lat - 1
    at_pole = jnp.logical_or(lat == 0, lat == n_lat - 1)

    loads = [(x_hbm.at[:, :REACH], x_ref.at[:, :REACH]), (x_hbm.at[:, CELL - REACH:], x_ref.at[:, CELL - REACH:]),
             (x_hbm.at[:, REACH:CELL - REACH], x_ref.at[:, REACH:CELL - REACH]), (wg_hbm, wg_ref), (par_hbm, par_ref), (wo_hbm, wo_ref), (wgu_hbm, wgu_ref), (wm_hbm, wm_ref),
             (we_hbm, we_ref), (wmsg_hbm, wmsg_ref), (mesh_hbm, mesh_ref), (edge_hbm, edge_ref), (send_hbm, send_ref), (mask_hbm, mask_ref)]
    loads = [pltpu.make_async_copy(a, b, in_sem.at[k]) for k, (a, b) in enumerate(loads)]
    for load in loads:
        load.start()

    barrier = pltpu.get_barrier_semaphore()
    pl.semaphore_signal(barrier, inc=1, device_id=across, device_id_type=MESH)

    @pl.when(has_up)
    def _():
        pl.semaphore_signal(barrier, inc=1, device_id=up, device_id_type=MESH)

    @pl.when(has_down)
    def _():
        pl.semaphore_signal(barrier, inc=1, device_id=down, device_id_type=MESH)

    def send(k, src_ref, src, dst, count, to):
        return pltpu.make_async_remote_copy(
            src_ref=src_ref.at[pl.ds(src * BATCH, count * BATCH)], dst_ref=rx_ref.at[pl.ds(dst * BATCH, count * BATCH)],
            send_sem=send_sem.at[k], recv_sem=recv_sem.at[k], device_id=to, device_id_type=MESH)

    e_top = send(0, tx_ref, BASE_EDGE, BASE_EDGE, REACH * EDGE_BLK, across)
    e_low = send(1, tx_ref, BASE_EDGE + (CELL - REACH) * EDGE_BLK, BASE_EDGE + (CELL - REACH) * EDGE_BLK, REACH * EDGE_BLK, across)
    e_mid = send(2, tx_ref, BASE_EDGE + REACH * EDGE_BLK, BASE_EDGE + REACH * EDGE_BLK, (CELL - 2 * REACH) * EDGE_BLK, across)
    polar = send(3, tx_ref, BASE_POLE, BASE_POLE, REACH * POLE_BLK, across)
    to_up = send(4, tx_ref, BASE_SOUTH, BASE_SOUTH, REACH * ROW_BLK, up)
    to_down = send(5, tx_ref, BASE_NORTH, BASE_NORTH, REACH * ROW_BLK, down)
    fwd_up = send(6, rx_ref, BASE_EDGE, BASE_CS, REACH * EDGE_BLK, up)
    fwd_down = send(7, rx_ref, BASE_EDGE + (CELL - REACH) * EDGE_BLK, BASE_CN, REACH * EDGE_BLK, down)

    flip = flip_matrix(ROWS, CELL)
    flip_edge = jnp.concatenate([flip[:REACH * BATCH], flip[(CELL - REACH) * BATCH:]], axis=0)
    lane = lax.broadcasted_iota(i32, (ROWS, LANES), 1) + LANES
    ones = jnp.where((lane >= CIN) & (lane < CIN + 3), 1.0, 0.0).astype(bf16)
    loads[0].wait()
    loads[1].wait()

    def put(row, lo, hi):
        n = lo.shape[0]
        tx_ref[row * BATCH:row * BATCH + n] = lo
        tx_ref[row * BATCH + n:row * BATCH + n * 3 // 2] = hi

    def pad_row(i):
        at = slice(i * ROWS, (i + 1) * ROWS)
        xpad_ref[at, LANES:] = ones
        xpad_ref[at, :CIN] = x_ref[:, i].reshape(ROWS, CIN)
        return xpad_ref[at, :]

    for k in range(REACH):
        inner = []
        for base, first in ((BASE_SOUTH, 0), (BASE_NORTH, CELL - REACH)):
            full = dot(flip, pad_row(first + k))
            edge = jnp.concatenate([full[:REACH * BATCH], full[(CELL - REACH) * BATCH:]], axis=0)
            put(BASE_EDGE + (first + k) * EDGE_BLK, *pack_hi(edge))
            put(base + k * ROW_BLK, *pack_hi(full))
            inner.append(full[REACH * BATCH:(CELL - REACH) * BATCH])
        put(BASE_POLE + k * POLE_BLK, *pack_hi(jnp.where(lat == 0, *inner)))
    pl.semaphore_wait(barrier, 1 + has_up.astype(i32) + has_down.astype(i32))
    e_top.start()
    e_low.start()
    pl.when(has_up)(to_up.start)
    pl.when(has_down)(to_down.start)
    pl.when(at_pole)(polar.start)

    loads[2].wait()
    for i in range(REACH, CELL - REACH):
        put(BASE_EDGE + i * EDGE_BLK, *pack_hi(dot(flip_edge, pad_row(i))))
    e_mid.start()

    for load in loads[3:]:
        load.wait()
    fill_embed(wpad_ref, wg_ref, par_ref[0][0:1])
    wgu_ref[...] = wgu_ref[...] * bf16(0.5)

    def rows_at(j):
        return pl.ds(j * ROWS if isinstance(j, int) else pl.multiple_of(j * ROWS, ROWS), ROWS)

    def embed_step(j, p, entering=True, leaving=(True, True, True)):
        q = 1 - p
        if leaving[1]:
            y_ref[p] = dot(hid_ref[p], wo_ref[0])
        if entering:
            pre_ref[p] = dot(xpad_ref[rows_at(j), :], wpad_ref[...])
        if leaving[0]:
            hid_ref[q] = swish(pre_ref[q])
        if leaving[2]:
            vg_ref[rows_at(j - 3), :] = norm(y_ref[q] + par_ref[0][1:2], par_ref[0]).astype(bf16)

    def update_step(j, p, entering=True, leaving=(True, True, True)):
        q = 1 - p
        if leaving[1]:
            y_ref[2 + p] = dot(hid_ref[2 + p], wo_ref[5])
        if entering:
            vg = vg_ref[rows_at(j), :]
            pre_ref[2 + p] = dot(vg, wgu_ref[...])
            vgt_ref[rows_at(j), :] = dot(flip, vg).astype(bf16)
        if leaving[0]:
            hid_ref[2 + q] = swish(pre_ref[2 + q] + 0.5 * par_ref[5][0:1])
        if leaving[2]:
            upd = norm(y_ref[2 + q] + par_ref[5][1:2], par_ref[5])
            gout_ref[j - 3] = (vg_ref[rows_at(j - 3), :].astype(f32) + upd).astype(bf16).reshape(BATCH, CELL, LAT)

    def fill(step):
        step(0, 0, True, (False, False, False))
        step(1, 1, True, (True, False, False))
        step(2, 0, True, (True, True, False))

    def drain(step):
        step(CELL, 0, False, (True, True, True))
        step(CELL + 1, 1, False, (False, True, True))
        step(CELL + 2, 0, False, (False, False, True))

    def run(step, first, trips):
        def some(k, carry):
            for u in range(UNROLL):
                step(first + k * UNROLL + u, (first + u) % 2)
            return carry

        lax.fori_loop(0, trips, some, 0)

    fill(embed_step)
    run(embed_step, 3, 12 // UNROLL)
    embed_step(CELL - 1, 1)
    drain(embed_step)
    fill(update_step)
    run(update_step, 3, 4 // UNROLL)
    e_top.wait_recv()
    e_low.wait_recv()
    pl.when(has_up)(fwd_up.start)
    pl.when(has_down)(fwd_down.start)
    run(update_step, 7, 8 // UNROLL)
    update_step(CELL - 1, 1)
    drain(update_step)

    code_ref[...] = slot_lists(send_ref[...], mask_ref[...], lat, lon)
    par = par_ref[1]
    vm = finish(0.5 * (dot_t(mesh_ref[...], wm_ref[...]) + par[0:1]), wo_ref[1], par).astype(bf16)
    vm_ref[...] = vm.astype(f32)
    par = par_ref[2]
    el = finish(0.5 * (jnp.concatenate([dot_t(edge_ref[n], we_ref[...]) for n in range(NODES)], axis=0) + par[0:1]), wo_ref[2], par).astype(bf16)
    par = par_ref[3]
    el_ref[...] = el.astype(f32) + par[3:4]
    vm_proj = dot(vm, wmsg_ref[2 * LAT:]) + par[0:1]
    lp = dot(el, wmsg_ref[:LAT]).reshape(NODES, SLOTS, LAT) + vm_proj[:, None, :]
    lp_ref[...] = 0.5 * lp.reshape(NSLOT, LAT)

    e_mid.wait_recv()
    pl.when(at_pole)(polar.wait_recv)

    @pl.when(has_down)
    def _():
        to_up.wait_recv()
        fwd_up.wait_recv()

    @pl.when(has_up)
    def _():
        to_down.wait_recv()
        fwd_down.wait_recv()

    rx_out_ref[...] = rx_ref[...]
    e_top.wait_send()
    e_low.wait_send()
    e_mid.wait_send()
    pl.when(at_pole)(polar.wait_send)

    @pl.when(has_up)
    def _():
        to_up.wait_send()
        fwd_up.wait_send()

    @pl.when(has_down)
    def _():
        to_down.wait_send()
        fwd_down.wait_send()


def slot_kernel(code_ref, vgt_ref, gout_ref, rx_ref, lp_ref, el_ref, vm_ref, wg_ref, wmsg_ref, wnode_ref, wo_ref, par_ref,
                mesh_ref, grid_ref, wpad_ref, wmid_ref, lhs_ref, pre_ref, hid_ref, y_ref, far_vg_ref, acc_ref, base_ref, sem):
    copies = [pltpu.make_async_copy(gout_ref.at[i], grid_ref.at[:, i], sem.at[i]) for i in range(CELL)]
    for copy in copies:
        copy.start()
    fill_embed(wpad_ref, wg_ref, par_ref[0][0:1])
    wmid_ref[...] = wmsg_ref[LAT:2 * LAT] * bf16(0.5)
    acc_ref[...] = jnp.zeros_like(acc_ref)

    n_all, n_far = code_ref[7, 0], code_ref[7, 1]
    vm = vm_ref[...]
    base_ref[...] = dot(vm.astype(bf16), wnode_ref[:LAT]) + par_ref[4][0:1]

    def block(ref, index):
        return ref[pl.ds(pl.multiple_of(index, BATCH), BATCH), :]

    par = par_ref[3]

    n_groups = NSLOT // GROUP

    def embed_step(j, p):
        q = 1 - p
        y_ref[p] = dot(hid_ref[p], wo_ref[0])
        for u in range(GROUP):
            lo, hi, upper = [code_ref[k, j * GROUP + u] for k in (8, 9, 10)]
            dst = slice(u * BATCH, (u + 1) * BATCH)
            lhs_ref[p, dst, :LANES] = block(rx_ref, lo)
            high = block(rx_ref, hi).astype(f32)
            high = jnp.where(upper == 1, pltpu.roll(high, HALF, 1), high)
            lhs_ref[p, dst, LANES:256] = high.astype(bf16)
        pre_ref[p] = dot(lhs_ref[p, :, :256], wpad_ref[...])
        hid_ref[q] = swish(pre_ref[q])
        to = jnp.where(j < 3, n_groups, j - 3)
        vg = norm(y_ref[q] + par_ref[0][1:2], par_ref[0])
        far_vg_ref[pl.ds(pl.multiple_of(to * ROWS, ROWS), ROWS), :] = vg.astype(bf16)

    def message_step(j, p):
        q = 1 - p
        y_ref[p] = dot(hid_ref[p], wo_ref[3])
        for u in range(GROUP):
            near, far, is_far = [code_ref[k, FRONT + j * GROUP + u] for k in (2, 3, 4)]
            sender = jnp.where(is_far == 1, block(far_vg_ref, far), block(vgt_ref, near))
            lhs_ref[p, u * BATCH:(u + 1) * BATCH] = sender
        pre_ref[p] = dot(lhs_ref[p], wmid_ref[...])
        for u in range(GROUP):
            t = code_ref[0, FRONT + (j - 1) * GROUP + u]
            at = slice(u * BATCH, (u + 1) * BATCH)
            hid_ref[q, at] = swish(pre_ref[q, at] + lp_ref[pl.ds(t, 1), :])
        for u in range(GROUP):
            t, node = [code_ref[k, FRONT + (j - 3) * GROUP + u] for k in (0, 1)]
            upd = scale(y_ref[q, u * BATCH:(u + 1) * BATCH] + par[1:2]) * par[2:3]
            new = (upd + el_ref[pl.ds(t, 1), :]).astype(bf16).astype(f32)
            at = pl.ds(pl.multiple_of(node, BATCH), BATCH)
            acc_ref[u % 4, at, :] = acc_ref[u % 4, at, :] + new

    def run(step, n):
        steps = jnp.where(n > 0, (n + GROUP - 1) // GROUP + 3, 0)
        fours = steps // 4

        def four(k, carry):
            for u in range(4):
                step(4 * k + u, u % 2)
            return carry

        def two(k, carry):
            step(2 * k, 0)
            step(2 * k + 1, 1)
            return carry

        lax.fori_loop(0, fours, four, 0)
        lax.fori_loop(2 * fours, (steps + 1) // 2, two, 0)

    run(embed_step, n_far)
    run(message_step, n_all)

    n_rows = NODES * BATCH
    par = par_ref[4]
    agg = ((acc_ref[0, :n_rows] + acc_ref[1, :n_rows]) + (acc_ref[2, :n_rows] + acc_ref[3, :n_rows])).astype(bf16)
    base = base_ref[...]
    pre = dot(agg, wnode_ref[LAT:]).reshape(NODES, BATCH, LAT) + base[:, None, :]
    upd = finish(0.5 * pre.reshape(n_rows, LAT), wo_ref[4], par)
    out = (upd.reshape(NODES, BATCH, LAT) + vm[:, None, :]).reshape(n_rows, LAT).astype(bf16)
    mesh_ref[...] = dot(flip_matrix(n_rows, BATCH), out).astype(bf16).reshape(BATCH, NODES, LAT)
    for copy in copies:
        copy.wait()


def solution(mesh):
    n_lat, n_lon = mesh.shape['lat'], mesh.shape['lon']

    def cell_step(grid_in, mesh_in, edge_in, senders, edge_mask, w_grid, w_mesh, w_edge, w_msg, w_node, w_gupd, w_out, bias_gain):
        vmem = pl.BlockSpec(memory_space=pltpu.VMEM)
        smem = pl.BlockSpec(memory_space=pltpu.SMEM)
        hbm = pl.BlockSpec(memory_space=pltpu.HBM)
        loaded = [grid_in, mesh_in.T, edge_in.transpose(0, 2, 1), senders, edge_mask, w_grid, w_mesh, w_edge, w_msg, w_gupd, w_out, bias_gain]
        pin = lambda x: pltpu.with_memory_space_constraint(x, pltpu.HBM)
        own = pl.pallas_call(
            functools.partial(own_kernel, n_lat, n_lon),
            name='own',
            out_shape=[
                pltpu.VMEM((ROWS * CELL, LAT), bf16),
                pltpu.VMEM((CELL, BATCH, CELL, LAT), bf16),
                pltpu.VMEM((BLOCKS * BATCH, LANES), bf16),
                pltpu.VMEM((NSLOT, LAT), f32),
                pltpu.VMEM((NSLOT, LAT), f32),
                pltpu.VMEM((NODES, LAT), f32),
                pltpu.VMEM((16, LIST), i32),
            ],
            in_specs=[hbm] * 12,
            out_specs=[vmem] * 7,
            scratch_shapes=[
                *[pltpu.VMEM(a.shape, a.dtype) for a in loaded],
                pltpu.VMEM((ROWS * CELL, 256), bf16),
                pltpu.VMEM((256, LAT), bf16),
                pltpu.VMEM((4, ROWS, LAT), f32),
                pltpu.VMEM((4, ROWS, LAT), bf16),
                pltpu.VMEM((4, ROWS, LAT), f32),
                pltpu.VMEM((CELL * ROWS, LAT), bf16),
                pltpu.VMEM((BLOCKS * BATCH, LANES), bf16),
                pltpu.VMEM((BLOCKS * BATCH, LANES), bf16),
                pltpu.SemaphoreType.DMA((14,)),
                pltpu.SemaphoreType.DMA((8,)),
                pltpu.SemaphoreType.DMA((8,)),
            ],
            compiler_params=pltpu.CompilerParams(vmem_limit_bytes=28 << 20, collective_id=0, has_side_effects=True),
            cost_estimate=pl.CostEstimate(flops=10 * 10**9, bytes_accessed=16 << 20, transcendentals=0),
        )(*map(pin, loaded))
        vgt, gout, rx, lp, el, vm, code = own

        mesh_out, grid_out = pl.pallas_call(
            slot_kernel,
            name='slots',
            out_shape=[jax.ShapeDtypeStruct((BATCH, NODES, LAT), bf16), jax.ShapeDtypeStruct((BATCH, CELL, CELL, LAT), bf16)],
            in_specs=[smem] + [vmem] * 11,
            out_specs=[vmem, hbm],
            scratch_shapes=[
                pltpu.VMEM((256, LAT), bf16),
                pltpu.VMEM((LAT, LAT), bf16),
                pltpu.VMEM((2, ROWS, LAT), bf16),
                pltpu.VMEM((2, ROWS, LAT), f32),
                pltpu.VMEM((2, ROWS, LAT), bf16),
                pltpu.VMEM((2, ROWS, LAT), f32),
                pltpu.VMEM((NSLOT * BATCH + 3 * ROWS, LAT), bf16),
                pltpu.VMEM((4, (NODES + 1) * BATCH, LAT), f32),
                pltpu.VMEM((NODES, LAT), f32),
                pltpu.SemaphoreType.DMA((CELL,)),
            ],
            compiler_params=pltpu.CompilerParams(vmem_limit_bytes=24 << 20),
            cost_estimate=pl.CostEstimate(flops=10 * 10**9, bytes_accessed=16 << 20, transcendentals=0),
        )(code, vgt, gout, rx, lp, el, vm, w_grid, w_msg, w_node, w_out, bias_gain)
        return mesh_out, grid_out

    grid_spec = P('dp', 'lat', 'lon', None)
    node_spec = P(('lat', 'lon'), None)
    slot_spec = P(('lat', 'lon'), None, None)
    rep = P()
    in_specs = (grid_spec, node_spec, slot_spec, node_spec, node_spec) + (rep,) * 8
    out_specs = (P('dp', ('lat', 'lon'), None), grid_spec)
    return jax.shard_map(cell_step, mesh=mesh, in_specs=in_specs, out_specs=out_specs, check_vma=False)
```

```python
import functools

import jax
import jax.numpy as jnp
from jax import lax
from jax.experimental import pallas as pl
from jax.experimental.pallas import tpu as pltpu
from jax.sharding import PartitionSpec as P

REACH = 3
LN_EPS = 1e-5
CELL = 16
BATCH = 16
CIN = 186
LAT = 512
HALF = 64
LANES = 128
NODES = 8
SLOTS = 48
NSLOT = NODES * SLOTS
GROUP = 16
ROWS = GROUP * BATCH
EDGE_PTS, POLE_PTS, ROW_PTS = 2 * REACH, CELL - 2 * REACH, CELL
EDGE_BLK, POLE_BLK, ROW_BLK = EDGE_PTS * 3 // 2, POLE_PTS * 3 // 2, ROW_PTS * 3 // 2
BASE_EDGE = 0
BASE_POLE = BASE_EDGE + CELL * EDGE_BLK
BASE_NORTH = BASE_POLE + REACH * POLE_BLK
BASE_SOUTH = BASE_NORTH + REACH * ROW_BLK
BASE_CN = BASE_SOUTH + REACH * ROW_BLK
BASE_CS = BASE_CN + REACH * EDGE_BLK
BLOCKS = BASE_CS + REACH * EDGE_BLK
LIST = 512
FRONT = 3 * GROUP
UNROLL = 4
bf16, f32, i32 = jnp.bfloat16, jnp.float32, jnp.int32
MESH = pl.DeviceIdType.MESH


def dot(a, b):
    return jnp.dot(a, b, preferred_element_type=f32)


def dot_t(a, b):
    return lax.dot_general(a, b, (((0,), (0,)), ((), ())), preferred_element_type=f32)


def swish(h):
    return (h + h * jnp.tanh(h)).astype(bf16)


def scale(y):
    y = y - jnp.mean(y, axis=-1, keepdims=True)
    var = jnp.mean(y * y, axis=-1, keepdims=True)
    return y * lax.rsqrt(var + LN_EPS)


def norm(y, par):
    return scale(y) * par[2:3] + par[3:4]


def finish(half_pre, w2, par):
    return norm(dot(swish(half_pre), w2) + par[1:2], par)


def pack_hi(y):
    half = y.shape[0] // 2
    hi = y[:, LANES:]
    return y[:, :LANES].astype(bf16), (hi[:half] + pltpu.roll(hi[half:], HALF, 1)).astype(bf16)


def fill_embed(wpad_ref, wg_ref, b1):
    tile = CIN // BATCH * BATCH
    wpad_ref[tile:] = jnp.zeros((256 - tile, LAT), bf16)
    wpad_ref[:CIN] = wg_ref[...]
    b_hi = b1.astype(bf16)
    b_mid = (b1 - b_hi.astype(f32)).astype(bf16)
    b_lo = (b1 - b_hi.astype(f32) - b_mid.astype(f32)).astype(bf16)
    row = lax.broadcasted_iota(i32, (BATCH, LAT), 0) + tile
    edge = wpad_ref[tile:tile + BATCH].astype(f32)
    for k, part in enumerate((b_hi, b_mid, b_lo)):
        edge = jnp.where(row == CIN + k, part.astype(f32), edge)
    wpad_ref[tile:tile + BATCH] = edge.astype(bf16)
    wpad_ref[...] = wpad_ref[...] * bf16(0.5)


def slot_lists(senders, live, lat, lon):
    row, col = senders >> 5, senders & 31
    r = row - lat * CELL
    c = col & (CELL - 1)
    own_lon = (col >> 4) == lon
    in_band = (r >= 0) & (r < CELL)
    local = in_band & own_lon
    is_edge = (c < REACH) | (c >= CELL - REACH)
    pole = in_band & jnp.logical_not(is_edge)
    e = jnp.where(c < REACH, c, c - (CELL - EDGE_PTS))
    north = r < 0
    band_base = jnp.where(north, jnp.where(own_lon, BASE_NORTH, BASE_CN), jnp.where(own_lon, BASE_SOUTH, BASE_CS))
    base = jnp.where(in_band, jnp.where(pole, BASE_POLE, BASE_EDGE), band_base)
    pole_line = jnp.where(lat == 0, r, r - (CELL - REACH))
    line = jnp.where(in_band, jnp.where(pole, pole_line, r), jnp.where(north, r + REACH, r - CELL))
    q = jnp.where(pole, c - REACH, jnp.where(own_lon, c, e))
    half = jnp.where(pole, POLE_PTS // 2, jnp.where(own_lon, ROW_PTS // 2, EDGE_PTS // 2))
    start = base + line * (half * 3)
    upper = jnp.where(q >= half, 1, 0)
    lo = start + q
    hi = start + half * 2 + q - upper * half
    n_slots = senders.shape[1]

    def ahead(flag):
        value = flag.astype(f32)
        earlier = lax.broadcasted_iota(i32, (n_slots, n_slots), 0) < lax.broadcasted_iota(i32, (n_slots, n_slots), 1)
        inside = dot(value.astype(bf16), jnp.where(earlier, 1.0, 0.0).astype(bf16))
        total = jnp.broadcast_to(jnp.sum(value, axis=1, keepdims=True), (senders.shape[0], LANES)).astype(bf16)
        earlier = lax.broadcasted_iota(i32, (NODES, NODES), 1) < lax.broadcasted_iota(i32, (NODES, NODES), 0)
        return inside + dot(jnp.where(earlier, 1.0, 0.0).astype(bf16), total)[:, :n_slots]

    active = live == 1
    far = active & jnp.logical_not(local)
    eye = lax.broadcasted_iota(i32, (n_slots, n_slots), 0) == lax.broadcasted_iota(i32, (n_slots, n_slots), 1)
    point = lax.broadcasted_iota(i32, (n_slots, LIST), 1).astype(f32)
    wanted = jnp.where(far, lo, LIST - 1).astype(f32)
    hits = []
    for n in range(NODES):
        column = jnp.sum(jnp.where(eye, wanted[n:n + 1], 0.0), axis=1, keepdims=True)
        hits.append(jnp.where(point == column, 1.0, 0.0))
    used = jnp.sum(functools.reduce(jnp.maximum, hits), axis=0, keepdims=True)
    lanes = lax.broadcasted_iota(i32, (NODES, LIST), 1)
    used = jnp.where((jnp.broadcast_to(used, (NODES, LIST)) > 0) & (lanes < LIST - 1), 1.0, 0.0)
    earlier = lax.broadcasted_iota(i32, (LIST, LIST), 0) < lax.broadcasted_iota(i32, (LIST, LIST), 1)
    rank = dot(used.astype(bf16), jnp.where(earlier, 1.0, 0.0).astype(bf16))[0:1]
    far_at = []
    for hit in hits:
        column = jnp.sum(hit * rank, axis=1, keepdims=True)
        far_at.append(jnp.sum(jnp.where(eye, column, 0.0), axis=0, keepdims=True))
    far_at = jnp.concatenate(far_at, axis=0)
    near = active & local
    n_near = jnp.sum(near.astype(f32))
    all_at = jnp.where(active, jnp.where(local, ahead(near), ahead(far) + n_near) + FRONT, LIST - 1.0)
    to_far = jnp.where(far, far_at, LIST - 1.0)
    slot_id = lax.broadcasted_iota(i32, senders.shape, 1)

    def gather(places, fields):
        total = jnp.zeros((8, LIST), f32)
        for n in range(NODES):
            column = jnp.sum(jnp.where(eye, places[n:n + 1], 0.0), axis=1, keepdims=True)
            rows = [f[n:n + 1].astype(f32) for f in fields]
            rows = jnp.concatenate(rows + [jnp.zeros((8 - len(rows), n_slots), f32)], axis=0).astype(bf16)
            total = total + dot(rows, jnp.where(point == column, 1.0, 0.0).astype(bf16))
        return total

    one = jnp.ones(senders.shape, f32)
    node = lax.broadcasted_iota(i32, senders.shape, 0)
    near_row = jnp.where(local, r * CELL + c, 0)
    got = gather(all_at, [slot_id, node, near_row, jnp.where(far, far_at, 0.0), far.astype(f32), one]).astype(i32)
    lane = lax.broadcasted_iota(i32, (1, LIST), 1)
    valid = (got[5:6] == 1) & (lane < LIST - 1)
    n_all = jnp.sum(active.astype(f32)).astype(i32)
    n_far = jnp.sum(used[0:1]).astype(i32)
    main = [jnp.where(valid, got[1:2] * SLOTS + got[0:1], 0), jnp.where(valid, got[1:2], NODES) * BATCH,
            got[2:3] * BATCH, got[3:4] * BATCH, got[4:5]]
    main = [jnp.where(valid, m, 0) if k != 1 else m for k, m in enumerate(main)]
    counts = jnp.where(lane == 0, n_all, jnp.where(lane == 1, n_far, n_near.astype(i32)))
    got = gather(to_far, [lo >> 4, lo & 15, hi >> 4, hi & 15, upper, one])
    got = (got / jnp.maximum(got[5:6], 1.0) + 0.5).astype(i32)
    valid = lane < n_far
    halo = [jnp.where(valid, v, 0) for v in ((got[0:1] * 16 + got[1:2]) * BATCH, (got[2:3] * 16 + got[3:4]) * BATCH, got[4:5])]
    zero = jnp.zeros((1, LIST), i32)
    return jnp.concatenate(main + [zero, zero, counts] + halo + [zero] * 5, axis=0)


def flip_matrix(rows, inner):
    a = lax.broadcasted_iota(i32, (rows, rows), 0)
    b = lax.broadcasted_iota(i32, (rows, rows), 1)
    outer = rows // inner
    return jnp.where(a // outer + a % outer * inner == b, 1.0, 0.0).astype(bf16)


def own_kernel(n_lat, n_lon, x_hbm, mesh_hbm, edge_hbm, send_hbm, mask_hbm, wg_hbm, wm_hbm, we_hbm, wmsg_hbm, wgu_hbm, wo_hbm, par_hbm,
               vgt_ref, gout_ref, rx_out_ref, lp_ref, el_ref, vm_ref, code_ref,
               x_ref, mesh_ref, edge_ref, send_ref, mask_ref, wg_ref, wm_ref, we_ref, wmsg_ref, wgu_ref, wo_ref, par_ref, xpad_ref, wpad_ref, pre_ref, hid_ref, y_ref, vg_ref, tx_ref, rx_ref,
               in_sem, send_sem, recv_sem):
    dp = lax.axis_index('dp')
    lon = lax.axis_index('lon')
    lat = lax.axis_index('lat')
    across = (dp, (lon + 1) % n_lon, lat)
    up = (dp, lon, lat - 1)
    down = (dp, lon, lat + 1)
    has_up = lat > 0
    has_down = lat < n_lat - 1
    at_pole = jnp.logical_or(lat == 0, lat == n_lat - 1)

    loads = [(x_hbm.at[:, :REACH], x_ref.at[:, :REACH]), (x_hbm.at[:, CELL - REACH:], x_ref.at[:, CELL - REACH:]),
             (x_hbm.at[:, REACH:CELL - REACH], x_ref.at[:, REACH:CELL - REACH]), (wg_hbm, wg_ref), (par_hbm, par_ref), (wo_hbm, wo_ref), (wgu_hbm, wgu_ref), (wm_hbm, wm_ref),
             (we_hbm, we_ref), (wmsg_hbm, wmsg_ref), (mesh_hbm, mesh_ref), (edge_hbm, edge_ref), (send_hbm, send_ref), (mask_hbm, mask_ref)]
    loads = [pltpu.make_async_copy(a, b, in_sem.at[k]) for k, (a, b) in enumerate(loads)]
    for load in loads:
        load.start()

    barrier = pltpu.get_barrier_semaphore()
    pl.semaphore_signal(barrier, inc=1, device_id=across, device_id_type=MESH)

    @pl.when(has_up)
    def _():
        pl.semaphore_signal(barrier, inc=1, device_id=up, device_id_type=MESH)

    @pl.when(has_down)
    def _():
        pl.semaphore_signal(barrier, inc=1, device_id=down, device_id_type=MESH)

    def send(k, src_ref, src, dst, count, to):
        return pltpu.make_async_remote_copy(
            src_ref=src_ref.at[pl.ds(src * BATCH, count * BATCH)], dst_ref=rx_ref.at[pl.ds(dst * BATCH, count * BATCH)],
            send_sem=send_sem.at[k], recv_sem=recv_sem.at[k], device_id=to, device_id_type=MESH)

    e_top = send(0, tx_ref, BASE_EDGE, BASE_EDGE, REACH * EDGE_BLK, across)
    e_low = send(1, tx_ref, BASE_EDGE + (CELL - REACH) * EDGE_BLK, BASE_EDGE + (CELL - REACH) * EDGE_BLK, REACH * EDGE_BLK, across)
    e_mid = send(2, tx_ref, BASE_EDGE + REACH * EDGE_BLK, BASE_EDGE + REACH * EDGE_BLK, (CELL - 2 * REACH) * EDGE_BLK, across)
    polar = send(3, tx_ref, BASE_POLE, BASE_POLE, REACH * POLE_BLK, across)
    to_up = send(4, tx_ref, BASE_SOUTH, BASE_SOUTH, REACH * ROW_BLK, up)
    to_down = send(5, tx_ref, BASE_NORTH, BASE_NORTH, REACH * ROW_BLK, down)
    fwd_up = send(6, rx_ref, BASE_EDGE, BASE_CS, REACH * EDGE_BLK, up)
    fwd_down = send(7, rx_ref, BASE_EDGE + (CELL - REACH) * EDGE_BLK, BASE_CN, REACH * EDGE_BLK, down)

    flip = flip_matrix(ROWS, CELL)
    flip_edge = jnp.concatenate([flip[:REACH * BATCH], flip[(CELL - REACH) * BATCH:]], axis=0)
    lane = lax.broadcasted_iota(i32, (ROWS, LANES), 1) + LANES
    ones = jnp.where((lane >= CIN) & (lane < CIN + 3), 1.0, 0.0).astype(bf16)
    loads[0].wait()
    loads[1].wait()

    def put(row, lo, hi):
        n = lo.shape[0]
        tx_ref[row * BATCH:row * BATCH + n] = lo
        tx_ref[row * BATCH + n:row * BATCH + n * 3 // 2] = hi

    def pad_row(i):
        at = slice(i * ROWS, (i + 1) * ROWS)
        xpad_ref[at, LANES:] = ones
        xpad_ref[at, :CIN] = x_ref[:, i].reshape(ROWS, CIN)
        return xpad_ref[at, :]

    outer = [*range(REACH), *range(CELL - REACH, CELL)]
    rows = {i: pad_row(i) for i in outer}
    for i in outer:
        put(BASE_EDGE + i * EDGE_BLK, *pack_hi(dot(flip_edge, rows[i])))
    pl.semaphore_wait(barrier, 1 + has_up.astype(i32) + has_down.astype(i32))
    e_top.start()
    e_low.start()
    for k in range(REACH):
        inner = []
        for base, first in ((BASE_SOUTH, 0), (BASE_NORTH, CELL - REACH)):
            full = dot(flip, rows[first + k])
            put(base + k * ROW_BLK, *pack_hi(full))
            inner.append(full[REACH * BATCH:(CELL - REACH) * BATCH])
        put(BASE_POLE + k * POLE_BLK, *pack_hi(jnp.where(lat == 0, *inner)))
    pl.when(has_up)(to_up.start)
    pl.when(has_down)(to_down.start)
    pl.when(at_pole)(polar.start)

    loads[2].wait()
    for i in range(REACH, CELL - REACH):
        put(BASE_EDGE + i * EDGE_BLK, *pack_hi(dot(flip_edge, pad_row(i))))
    e_mid.start()

    for load in loads[3:]:
        load.wait()
    fill_embed(wpad_ref, wg_ref, par_ref[0][0:1])
    wgu_ref[...] = wgu_ref[...] * bf16(0.5)

    def rows_at(j):
        return pl.ds(j * ROWS if isinstance(j, int) else pl.multiple_of(j * ROWS, ROWS), ROWS)

    def embed_step(j, p, entering=True, leaving=(True, True, True)):
        q = 1 - p
        if leaving[1]:
            y_ref[p] = dot(hid_ref[p], wo_ref[0])
        if entering:
            pre_ref[p] = dot(xpad_ref[rows_at(j), :], wpad_ref[...])
        if leaving[0]:
            hid_ref[q] = swish(pre_ref[q])
        if leaving[2]:
            vg_ref[rows_at(j - 3), :] = norm(y_ref[q] + par_ref[0][1:2], par_ref[0]).astype(bf16)

    def update_step(j, p, entering=True, leaving=(True, True, True)):
        q = 1 - p
        if leaving[1]:
            y_ref[2 + p] = dot(hid_ref[2 + p], wo_ref[5])
        if entering:
            vg = vg_ref[rows_at(j), :]
            pre_ref[2 + p] = dot(vg, wgu_ref[...])
            vgt_ref[rows_at(j), :] = dot(flip, vg).astype(bf16)
        if leaving[0]:
            hid_ref[2 + q] = swish(pre_ref[2 + q] + 0.5 * par_ref[5][0:1])
        if leaving[2]:
            upd = norm(y_ref[2 + q] + par_ref[5][1:2], par_ref[5])
            gout_ref[j - 3] = (vg_ref[rows_at(j - 3), :].astype(f32) + upd).astype(bf16).reshape(BATCH, CELL, LAT)

    def fill(step):
        step(0, 0, True, (False, False, False))
        step(1, 1, True, (True, False, False))
        step(2, 0, True, (True, True, False))

    def drain(step):
        step(CELL, 0, False, (True, True, True))
        step(CELL + 1, 1, False, (False, True, True))
        step(CELL + 2, 0, False, (False, False, True))

    def run(step, first, trips):
        def some(k, carry):
            for u in range(UNROLL):
                step(first + k * UNROLL + u, (first + u) % 2)
            return carry

        lax.fori_loop(0, trips, some, 0)

    fill(embed_step)
    run(embed_step, 3, 12 // UNROLL)
    embed_step(CELL - 1, 1)
    drain(embed_step)
    fill(update_step)
    run(update_step, 3, 4 // UNROLL)
    e_top.wait_recv()
    e_low.wait_recv()
    pl.when(has_up)(fwd_up.start)
    pl.when(has_down)(fwd_down.start)
    run(update_step, 7, 8 // UNROLL)
    update_step(CELL - 1, 1)
    drain(update_step)

    code_ref[...] = slot_lists(send_ref[...], mask_ref[...], lat, lon)
    par = par_ref[1]
    vm = finish(0.5 * (dot_t(mesh_ref[...], wm_ref[...]) + par[0:1]), wo_ref[1], par).astype(bf16)
    vm_ref[...] = vm.astype(f32)
    par = par_ref[2]
    el = finish(0.5 * (jnp.concatenate([dot_t(edge_ref[n], we_ref[...]) for n in range(NODES)], axis=0) + par[0:1]), wo_ref[2], par).astype(bf16)
    par = par_ref[3]
    el_ref[...] = el.astype(f32) + par[3:4]
    vm_proj = dot(vm, wmsg_ref[2 * LAT:]) + par[0:1]
    lp = dot(el, wmsg_ref[:LAT]).reshape(NODES, SLOTS, LAT) + vm_proj[:, None, :]
    lp_ref[...] = 0.5 * lp.reshape(NSLOT, LAT)

    pl.when(at_pole)(polar.wait_recv)

    @pl.when(has_down)
    def _():
        to_up.wait_recv()
        fwd_up.wait_recv()

    @pl.when(has_up)
    def _():
        to_down.wait_recv()
        fwd_down.wait_recv()

    for first, last in ((0, BASE_EDGE + REACH * EDGE_BLK), (BASE_EDGE + (CELL - REACH) * EDGE_BLK, BLOCKS)):
        rx_out_ref[first * BATCH:last * BATCH] = rx_ref[first * BATCH:last * BATCH]
    e_mid.wait_recv()
    at = slice((BASE_EDGE + REACH * EDGE_BLK) * BATCH, (BASE_EDGE + (CELL - REACH) * EDGE_BLK) * BATCH)
    rx_out_ref[at] = rx_ref[at]
    e_top.wait_send()
    e_low.wait_send()
    e_mid.wait_send()
    pl.when(at_pole)(polar.wait_send)

    @pl.when(has_up)
    def _():
        to_up.wait_send()
        fwd_up.wait_send()

    @pl.when(has_down)
    def _():
        to_down.wait_send()
        fwd_down.wait_send()


def slot_kernel(code_ref, vgt_ref, gout_ref, rx_ref, lp_ref, el_ref, vm_ref, wg_ref, wmsg_ref, wnode_ref, wo_ref, par_ref,
                mesh_ref, grid_ref, wpad_ref, wmid_ref, raw_ref, lhs_ref, pre_ref, hid_ref, y_ref, far_vg_ref, acc_ref, base_ref, sem):
    copies = [pltpu.make_async_copy(gout_ref.at[i], grid_ref.at[:, i], sem.at[i]) for i in range(CELL)]
    for copy in copies:
        copy.start()
    fill_embed(wpad_ref, wg_ref, par_ref[0][0:1])
    wmid_ref[...] = wmsg_ref[LAT:2 * LAT] * bf16(0.5)
    acc_ref[...] = jnp.zeros_like(acc_ref)

    n_all, n_far, n_near = [code_ref[7, k] for k in range(3)]
    vm = vm_ref[...]
    base_ref[...] = dot(vm.astype(bf16), wnode_ref[:LAT]) + par_ref[4][0:1]

    def block(ref, index):
        return ref[pl.ds(pl.multiple_of(index, BATCH), BATCH), :]

    par = par_ref[3]

    def embed_step(j, p, entering=True, leaving=(True, True, True)):
        q = 1 - p
        if leaving[1]:
            y_ref[2 + p] = dot(hid_ref[2 + p], wo_ref[0])
        if entering:
            for u in range(GROUP):
                lo, hi, upper = [code_ref[k, j * GROUP + u] for k in (8, 9, 10)]
                dst = slice(u * BATCH, (u + 1) * BATCH)
                raw_ref[p, dst, :LANES] = block(rx_ref, lo)
                high = block(rx_ref, hi).astype(f32)
                high = jnp.where(upper == 1, pltpu.roll(high, HALF, 1), high)
                raw_ref[p, dst, LANES:] = high.astype(bf16)
            pre_ref[2 + p] = dot(raw_ref[p], wpad_ref[...])
        if leaving[0]:
            hid_ref[2 + q] = swish(pre_ref[2 + q])
        if leaving[2]:
            vg = norm(y_ref[2 + q] + par_ref[0][1:2], par_ref[0])
            far_vg_ref[pl.ds(pl.multiple_of((j - 3) * ROWS, ROWS), ROWS), :] = vg.astype(bf16)

    def message_step(j, p, near_only=False, entering=True, leaving=(True, True, True)):
        q = 1 - p
        now, old, oldest = [jnp.maximum(FRONT + (j - k) * GROUP, 0) for k in (0, 1, 3)]
        if leaving[1]:
            y_ref[p] = dot(hid_ref[p], wo_ref[3])
        if entering:
            for u in range(GROUP):
                sender = block(vgt_ref, code_ref[2, now + u])
                if not near_only:
                    sender = jnp.where(code_ref[4, now + u] == 1, block(far_vg_ref, code_ref[3, now + u]), sender)
                lhs_ref[p, u * BATCH:(u + 1) * BATCH] = sender
            pre_ref[p] = dot(lhs_ref[p], wmid_ref[...])
        if leaving[0]:
            for u in range(GROUP):
                at = slice(u * BATCH, (u + 1) * BATCH)
                hid_ref[q, at] = swish(pre_ref[q, at] + lp_ref[pl.ds(code_ref[0, old + u], 1), :])
        if leaving[2]:
            for u in range(GROUP):
                t, node = code_ref[0, oldest + u], code_ref[1, oldest + u]
                upd = scale(y_ref[q, u * BATCH:(u + 1) * BATCH] + par[1:2]) * par[2:3]
                new = (upd + el_ref[pl.ds(t, 1), :]).astype(bf16).astype(f32)
                at = pl.ds(pl.multiple_of(node, BATCH), BATCH)
                acc_ref[u % 4, at, :] = acc_ref[u % 4, at, :] + new

    embed_steps = jnp.maximum((n_far + 2 * GROUP - 1) // (2 * GROUP) * 2, 4)
    beside = embed_steps + 4
    late = jnp.where(n_far > 0, jnp.maximum(beside - n_near // GROUP, 0), 0)
    groups = (n_all + GROUP - 1) // GROUP + late
    steps = jnp.maximum((groups + 1) // 2 * 2, beside)

    stages = [(False, False, False), (True, False, False), (True, True, False), (True, True, True)]
    for j in range(4):
        message_step(j - late, j % 2, True, True, stages[j])
        embed_step(j, j % 2, True, stages[j])

    def both(k, carry):
        for p in range(2):
            message_step(2 * k + p - late, p, True)
            embed_step(2 * k + p, p)
        return carry

    lax.fori_loop(2, embed_steps // 2, both, 0)
    ends = [(True, True, True), (False, True, True), (False, False, True)]
    for j in range(4):
        message_step(embed_steps + j - late, j % 2, True)
        if j < 3:
            embed_step(embed_steps + j, j % 2, False, ends[j])

    def many(count, start):
        def body(k, carry):
            for u in range(count):
                message_step(start + count * k + u - late, u % 2)
            return carry
        return body

    rest = steps - beside
    fours = rest // 4
    lax.fori_loop(0, fours, many(4, beside), 0)
    lax.fori_loop(0, rest // 2 - 2 * fours, many(2, beside + 4 * fours), 0)
    for j in range(3):
        message_step(steps + j - late, j % 2, False, False, ends[j])

    n_rows = NODES * BATCH
    par = par_ref[4]
    agg = ((acc_ref[0, :n_rows] + acc_ref[1, :n_rows]) + (acc_ref[2, :n_rows] + acc_ref[3, :n_rows])).astype(bf16)
    base = base_ref[...]
    pre = dot(agg, wnode_ref[LAT:]).reshape(NODES, BATCH, LAT) + base[:, None, :]
    upd = finish(0.5 * pre.reshape(n_rows, LAT), wo_ref[4], par)
    out = (upd.reshape(NODES, BATCH, LAT) + vm[:, None, :]).reshape(n_rows, LAT).astype(bf16)
    mesh_ref[...] = dot(flip_matrix(n_rows, BATCH), out).astype(bf16).reshape(BATCH, NODES, LAT)
    for copy in copies:
        copy.wait()


def solution(mesh):
    n_lat, n_lon = mesh.shape['lat'], mesh.shape['lon']

    def cell_step(grid_in, mesh_in, edge_in, senders, edge_mask, w_grid, w_mesh, w_edge, w_msg, w_node, w_gupd, w_out, bias_gain):
        vmem = pl.BlockSpec(memory_space=pltpu.VMEM)
        smem = pl.BlockSpec(memory_space=pltpu.SMEM)
        hbm = pl.BlockSpec(memory_space=pltpu.HBM)
        loaded = [grid_in, mesh_in.T, edge_in.transpose(0, 2, 1), senders, edge_mask, w_grid, w_mesh, w_edge, w_msg, w_gupd, w_out, bias_gain]
        pin = lambda x: pltpu.with_memory_space_constraint(x, pltpu.HBM)
        own = pl.pallas_call(
            functools.partial(own_kernel, n_lat, n_lon),
            name='own',
            out_shape=[
                pltpu.VMEM((ROWS * CELL, LAT), bf16),
                pltpu.VMEM((CELL, BATCH, CELL, LAT), bf16),
                pltpu.VMEM((BLOCKS * BATCH, LANES), bf16),
                pltpu.VMEM((NSLOT, LAT), f32),
                pltpu.VMEM((NSLOT, LAT), f32),
                pltpu.VMEM((NODES, LAT), f32),
                pltpu.VMEM((16, LIST), i32),
            ],
            in_specs=[hbm] * 12,
            out_specs=[vmem] * 7,
            scratch_shapes=[
                *[pltpu.VMEM(a.shape, a.dtype) for a in loaded],
                pltpu.VMEM((ROWS * CELL, 256), bf16),
                pltpu.VMEM((256, LAT), bf16),
                pltpu.VMEM((4, ROWS, LAT), f32),
                pltpu.VMEM((4, ROWS, LAT), bf16),
                pltpu.VMEM((4, ROWS, LAT), f32),
                pltpu.VMEM((CELL * ROWS, LAT), bf16),
                pltpu.VMEM((BLOCKS * BATCH, LANES), bf16),
                pltpu.VMEM((BLOCKS * BATCH, LANES), bf16),
                pltpu.SemaphoreType.DMA((14,)),
                pltpu.SemaphoreType.DMA((8,)),
                pltpu.SemaphoreType.DMA((8,)),
            ],
            compiler_params=pltpu.CompilerParams(vmem_limit_bytes=28 << 20, collective_id=0, has_side_effects=True),
            cost_estimate=pl.CostEstimate(flops=10 * 10**9, bytes_accessed=16 << 20, transcendentals=0),
        )(*map(pin, loaded))
        vgt, gout, rx, lp, el, vm, code = own

        mesh_out, grid_out = pl.pallas_call(
            slot_kernel,
            name='slots',
            out_shape=[jax.ShapeDtypeStruct((BATCH, NODES, LAT), bf16), jax.ShapeDtypeStruct((BATCH, CELL, CELL, LAT), bf16)],
            in_specs=[smem] + [vmem] * 11,
            out_specs=[vmem, hbm],
            scratch_shapes=[
                pltpu.VMEM((256, LAT), bf16),
                pltpu.VMEM((LAT, LAT), bf16),
                pltpu.VMEM((2, ROWS, 256), bf16),
                pltpu.VMEM((2, ROWS, LAT), bf16),
                pltpu.VMEM((4, ROWS, LAT), f32),
                pltpu.VMEM((4, ROWS, LAT), bf16),
                pltpu.VMEM((4, ROWS, LAT), f32),
                pltpu.VMEM((NSLOT * BATCH + 3 * ROWS, LAT), bf16),
                pltpu.VMEM((4, (NODES + 1) * BATCH, LAT), f32),
                pltpu.VMEM((NODES, LAT), f32),
                pltpu.SemaphoreType.DMA((CELL,)),
            ],
            compiler_params=pltpu.CompilerParams(vmem_limit_bytes=24 << 20),
            cost_estimate=pl.CostEstimate(flops=10 * 10**9, bytes_accessed=16 << 20, transcendentals=0),
        )(code, vgt, gout, rx, lp, el, vm, w_grid, w_msg, w_node, w_out, bias_gain)
        return mesh_out, grid_out

    grid_spec = P('dp', 'lat', 'lon', None)
    node_spec = P(('lat', 'lon'), None)
    slot_spec = P(('lat', 'lon'), None, None)
    rep = P()
    in_specs = (grid_spec, node_spec, slot_spec, node_spec, node_spec) + (rep,) * 8
    out_specs = (P('dp', ('lat', 'lon'), None), grid_spec)
    return jax.shard_map(cell_step, mesh=mesh, in_specs=in_specs, out_specs=out_specs, check_vma=False)
```

```python
import functools

import jax
import jax.numpy as jnp
from jax import lax
from jax.experimental import pallas as pl
from jax.experimental.pallas import tpu as pltpu
from jax.sharding import PartitionSpec as P

REACH = 3
LN_EPS = 1e-5
CELL = 16
BATCH = 16
CIN = 186
LAT = 512
HALF = 64
LANES = 128
NODES = 8
SLOTS = 48
NSLOT = NODES * SLOTS
GROUP = 16
ROWS = GROUP * BATCH
EDGE_PTS, POLE_PTS, ROW_PTS = 2 * REACH, CELL - 2 * REACH, CELL
EDGE_BLK, POLE_BLK, ROW_BLK = EDGE_PTS * 3 // 2, POLE_PTS * 3 // 2, ROW_PTS * 3 // 2
BASE_EDGE = 0
BASE_POLE = BASE_EDGE + CELL * EDGE_BLK
BASE_NORTH = BASE_POLE + REACH * POLE_BLK
BASE_SOUTH = BASE_NORTH + REACH * ROW_BLK
BASE_CN = BASE_SOUTH + REACH * ROW_BLK
BASE_CS = BASE_CN + REACH * EDGE_BLK
BLOCKS = BASE_CS + REACH * EDGE_BLK
LIST = 512
FRONT = 3 * GROUP
UNROLL = 4
bf16, f32, i32 = jnp.bfloat16, jnp.float32, jnp.int32
MESH = pl.DeviceIdType.MESH


def dot(a, b):
    return jnp.dot(a, b, preferred_element_type=f32)


def dot_t(a, b):
    return lax.dot_general(a, b, (((0,), (0,)), ((), ())), preferred_element_type=f32)


def swish(h):
    return (h + h * jnp.tanh(h)).astype(bf16)


def scale(y):
    y = y - jnp.mean(y, axis=-1, keepdims=True)
    var = jnp.mean(y * y, axis=-1, keepdims=True)
    return y * lax.rsqrt(var + LN_EPS)


def norm(y, par):
    return scale(y) * par[2:3] + par[3:4]


def finish(half_pre, w2, par):
    return norm(dot(swish(half_pre), w2) + par[1:2], par)


def pack_hi(y):
    half = y.shape[0] // 2
    hi = y[:, LANES:]
    return y[:, :LANES].astype(bf16), (hi[:half] + pltpu.roll(hi[half:], HALF, 1)).astype(bf16)


def fill_embed(wpad_ref, wg_ref, b1):
    tile = CIN // BATCH * BATCH
    wpad_ref[tile:] = jnp.zeros((256 - tile, LAT), bf16)
    wpad_ref[:CIN] = wg_ref[...]
    b_hi = b1.astype(bf16)
    b_mid = (b1 - b_hi.astype(f32)).astype(bf16)
    b_lo = (b1 - b_hi.astype(f32) - b_mid.astype(f32)).astype(bf16)
    row = lax.broadcasted_iota(i32, (BATCH, LAT), 0) + tile
    edge = wpad_ref[tile:tile + BATCH].astype(f32)
    for k, part in enumerate((b_hi, b_mid, b_lo)):
        edge = jnp.where(row == CIN + k, part.astype(f32), edge)
    wpad_ref[tile:tile + BATCH] = edge.astype(bf16)
    wpad_ref[...] = wpad_ref[...] * bf16(0.5)


def slot_lists(senders, live, lat, lon):
    row, col = senders >> 5, senders & 31
    r = row - lat * CELL
    c = col & (CELL - 1)
    own_lon = (col >> 4) == lon
    in_band = (r >= 0) & (r < CELL)
    local = in_band & own_lon
    is_edge = (c < REACH) | (c >= CELL - REACH)
    pole = in_band & jnp.logical_not(is_edge)
    e = jnp.where(c < REACH, c, c - (CELL - EDGE_PTS))
    north = r < 0
    band_base = jnp.where(north, jnp.where(own_lon, BASE_NORTH, BASE_CN), jnp.where(own_lon, BASE_SOUTH, BASE_CS))
    base = jnp.where(in_band, jnp.where(pole, BASE_POLE, BASE_EDGE), band_base)
    pole_line = jnp.where(lat == 0, r, r - (CELL - REACH))
    line = jnp.where(in_band, jnp.where(pole, pole_line, r), jnp.where(north, r + REACH, r - CELL))
    q = jnp.where(pole, c - REACH, jnp.where(own_lon, c, e))
    half = jnp.where(pole, POLE_PTS // 2, jnp.where(own_lon, ROW_PTS // 2, EDGE_PTS // 2))
    start = base + line * (half * 3)
    upper = jnp.where(q >= half, 1, 0)
    lo = start + q
    hi = start + half * 2 + q - upper * half
    n_slots = senders.shape[1]

    def ahead(flag):
        value = flag.astype(f32)
        earlier = lax.broadcasted_iota(i32, (n_slots, n_slots), 0) < lax.broadcasted_iota(i32, (n_slots, n_slots), 1)
        inside = dot(value.astype(bf16), jnp.where(earlier, 1.0, 0.0).astype(bf16))
        total = jnp.broadcast_to(jnp.sum(value, axis=1, keepdims=True), (senders.shape[0], LANES)).astype(bf16)
        earlier = lax.broadcasted_iota(i32, (NODES, NODES), 1) < lax.broadcasted_iota(i32, (NODES, NODES), 0)
        return inside + dot(jnp.where(earlier, 1.0, 0.0).astype(bf16), total)[:, :n_slots]

    active = live == 1
    far = active & jnp.logical_not(local)
    eye = lax.broadcasted_iota(i32, (n_slots, n_slots), 0) == lax.broadcasted_iota(i32, (n_slots, n_slots), 1)
    point = lax.broadcasted_iota(i32, (n_slots, LIST), 1).astype(f32)
    wanted = jnp.where(far, lo, LIST - 1).astype(f32)
    hits = []
    for n in range(NODES):
        column = jnp.sum(jnp.where(eye, wanted[n:n + 1], 0.0), axis=1, keepdims=True)
        hits.append(jnp.where(point == column, 1.0, 0.0))
    used = jnp.sum(functools.reduce(jnp.maximum, hits), axis=0, keepdims=True)
    lanes = lax.broadcasted_iota(i32, (NODES, LIST), 1)
    used = jnp.where((jnp.broadcast_to(used, (NODES, LIST)) > 0) & (lanes < LIST - 1), 1.0, 0.0)
    earlier = lax.broadcasted_iota(i32, (LIST, LIST), 0) < lax.broadcasted_iota(i32, (LIST, LIST), 1)
    rank = dot(used.astype(bf16), jnp.where(earlier, 1.0, 0.0).astype(bf16))[0:1]
    far_at = []
    for hit in hits:
        column = jnp.sum(hit * rank, axis=1, keepdims=True)
        far_at.append(jnp.sum(jnp.where(eye, column, 0.0), axis=0, keepdims=True))
    far_at = jnp.concatenate(far_at, axis=0)
    near = active & local
    n_near = jnp.sum(near.astype(f32))
    all_at = jnp.where(active, jnp.where(local, ahead(near), ahead(far) + n_near) + FRONT, LIST - 1.0)
    to_far = jnp.where(far, far_at, LIST - 1.0)
    slot_id = lax.broadcasted_iota(i32, senders.shape, 1)

    def gather(places, fields):
        total = jnp.zeros((8, LIST), f32)
        for n in range(NODES):
            column = jnp.sum(jnp.where(eye, places[n:n + 1], 0.0), axis=1, keepdims=True)
            rows = [f[n:n + 1].astype(f32) for f in fields]
            rows = jnp.concatenate(rows + [jnp.zeros((8 - len(rows), n_slots), f32)], axis=0).astype(bf16)
            total = total + dot(rows, jnp.where(point == column, 1.0, 0.0).astype(bf16))
        return total

    one = jnp.ones(senders.shape, f32)
    node = lax.broadcasted_iota(i32, senders.shape, 0)
    near_row = jnp.where(local, r * CELL + c, 0)
    got = gather(all_at, [slot_id, node, near_row, jnp.where(far, far_at, 0.0), far.astype(f32), one]).astype(i32)
    lane = lax.broadcasted_iota(i32, (1, LIST), 1)
    valid = (got[5:6] == 1) & (lane < LIST - 1)
    n_all = jnp.sum(active.astype(f32)).astype(i32)
    n_far = jnp.sum(used[0:1]).astype(i32)
    edge_row = jnp.where(valid, got[1:2] * SLOTS + got[0:1], 0) | (jnp.where(valid, got[1:2], NODES) << 16)
    near_block = jnp.where(valid, got[2:3], 0)
    far_block = jnp.where(valid, got[3:4] + (got[4:5] << 9), 0)
    got = gather(to_far, [lo >> 4, lo & 15, hi >> 4, hi & 15, upper, one])
    got = (got / jnp.maximum(got[5:6], 1.0) + 0.5).astype(i32)
    valid = lane < n_far
    halo = jnp.where(valid, (got[0:1] * 16 + got[1:2]) | ((got[2:3] * 16 + got[3:4] + (got[4:5] << 9)) << 16), 0)
    for k, count in enumerate((n_all, n_far, n_near.astype(i32))):
        halo = jnp.where(lane == LIST - 3 + k, count, halo)
    return jnp.concatenate([edge_row, near_block, far_block, halo], axis=0)


def flip_matrix(rows, inner):
    a = lax.broadcasted_iota(i32, (rows, rows), 0)
    b = lax.broadcasted_iota(i32, (rows, rows), 1)
    outer = rows // inner
    return jnp.where(a // outer + a % outer * inner == b, 1.0, 0.0).astype(bf16)


def own_kernel(n_lat, n_lon, x_hbm, mesh_hbm, edge_hbm, send_hbm, mask_hbm, wg_hbm, wm_hbm, we_hbm, wmsg_hbm, wgu_hbm, wo_hbm, par_hbm,
               vgt_ref, gout_ref, rx_out_ref, lp_ref, el_ref, vm_ref, code_ref,
               x_ref, mesh_ref, edge_ref, send_ref, mask_ref, wg_ref, wm_ref, we_ref, wmsg_ref, wgu_ref, wo_ref, par_ref, xpad_ref, wpad_ref, pre_ref, hid_ref, y_ref, vg_ref, tx_ref, rx_ref,
               in_sem, send_sem, recv_sem):
    dp = lax.axis_index('dp')
    lon = lax.axis_index('lon')
    lat = lax.axis_index('lat')
    across = (dp, (lon + 1) % n_lon, lat)
    up = (dp, lon, lat - 1)
    down = (dp, lon, lat + 1)
    has_up = lat > 0
    has_down = lat < n_lat - 1
    at_pole = jnp.logical_or(lat == 0, lat == n_lat - 1)

    loads = [(x_hbm.at[:, :REACH], x_ref.at[:, :REACH]), (x_hbm.at[:, CELL - REACH:], x_ref.at[:, CELL - REACH:]),
             (x_hbm.at[:, REACH:CELL - REACH], x_ref.at[:, REACH:CELL - REACH]), (wg_hbm, wg_ref), (par_hbm, par_ref), (wo_hbm, wo_ref), (wgu_hbm, wgu_ref), (wm_hbm, wm_ref),
             (we_hbm, we_ref), (wmsg_hbm, wmsg_ref), (mesh_hbm, mesh_ref), (edge_hbm, edge_ref), (send_hbm, send_ref), (mask_hbm, mask_ref)]
    loads = [pltpu.make_async_copy(a, b, in_sem.at[k]) for k, (a, b) in enumerate(loads)]
    for load in loads:
        load.start()

    barrier = pltpu.get_barrier_semaphore()
    pl.semaphore_signal(barrier, inc=1, device_id=across, device_id_type=MESH)

    @pl.when(has_up)
    def _():
        pl.semaphore_signal(barrier, inc=1, device_id=up, device_id_type=MESH)

    @pl.when(has_down)
    def _():
        pl.semaphore_signal(barrier, inc=1, device_id=down, device_id_type=MESH)

    def send(k, src_ref, src, dst, count, to):
        return pltpu.make_async_remote_copy(
            src_ref=src_ref.at[pl.ds(src * BATCH, count * BATCH)], dst_ref=rx_ref.at[pl.ds(dst * BATCH, count * BATCH)],
            send_sem=send_sem.at[k], recv_sem=recv_sem.at[k], device_id=to, device_id_type=MESH)

    e_top = send(0, tx_ref, BASE_EDGE, BASE_EDGE, REACH * EDGE_BLK, across)
    e_low = send(1, tx_ref, BASE_EDGE + (CELL - REACH) * EDGE_BLK, BASE_EDGE + (CELL - REACH) * EDGE_BLK, REACH * EDGE_BLK, across)
    e_mid = send(2, tx_ref, BASE_EDGE + REACH * EDGE_BLK, BASE_EDGE + REACH * EDGE_BLK, (CELL - 2 * REACH) * EDGE_BLK, across)
    polar = send(3, tx_ref, BASE_POLE, BASE_POLE, REACH * POLE_BLK, across)
    to_up = send(4, tx_ref, BASE_SOUTH, BASE_SOUTH, REACH * ROW_BLK, up)
    to_down = send(5, tx_ref, BASE_NORTH, BASE_NORTH, REACH * ROW_BLK, down)
    fwd_up = send(6, rx_ref, BASE_EDGE, BASE_CS, REACH * EDGE_BLK, up)
    fwd_down = send(7, rx_ref, BASE_EDGE + (CELL - REACH) * EDGE_BLK, BASE_CN, REACH * EDGE_BLK, down)

    flip = flip_matrix(ROWS, CELL)
    flip_edge = jnp.concatenate([flip[:REACH * BATCH], flip[(CELL - REACH) * BATCH:]], axis=0)
    lane = lax.broadcasted_iota(i32, (ROWS, LANES), 1) + LANES
    ones = jnp.where((lane >= CIN) & (lane < CIN + 3), 1.0, 0.0).astype(bf16)
    loads[0].wait()

    def put(row, lo, hi):
        n = lo.shape[0]
        tx_ref[row * BATCH:row * BATCH + n] = lo
        tx_ref[row * BATCH + n:row * BATCH + n * 3 // 2] = hi

    def pad_row(i):
        at = slice(i * ROWS, (i + 1) * ROWS)
        xpad_ref[at, LANES:] = ones
        xpad_ref[at, :CIN] = x_ref[:, i].reshape(ROWS, CIN)
        return xpad_ref[at, :]

    rows = {i: pad_row(i) for i in range(REACH)}
    for i in range(REACH):
        put(BASE_EDGE + i * EDGE_BLK, *pack_hi(dot(flip_edge, rows[i])))
    pl.semaphore_wait(barrier, 1 + has_up.astype(i32) + has_down.astype(i32))
    e_top.start()
    loads[1].wait()
    for i in range(CELL - REACH, CELL):
        rows[i] = pad_row(i)
        put(BASE_EDGE + i * EDGE_BLK, *pack_hi(dot(flip_edge, rows[i])))
    e_low.start()
    for k in range(REACH):
        inner = []
        for base, first in ((BASE_SOUTH, 0), (BASE_NORTH, CELL - REACH)):
            full = dot(flip, rows[first + k])
            put(base + k * ROW_BLK, *pack_hi(full))
            inner.append(full[REACH * BATCH:(CELL - REACH) * BATCH])
        put(BASE_POLE + k * POLE_BLK, *pack_hi(jnp.where(lat == 0, *inner)))
    pl.when(has_up)(to_up.start)
    pl.when(has_down)(to_down.start)
    pl.when(at_pole)(polar.start)

    loads[2].wait()
    for i in range(REACH, CELL - REACH):
        put(BASE_EDGE + i * EDGE_BLK, *pack_hi(dot(flip_edge, pad_row(i))))
    e_mid.start()

    for load in loads[3:]:
        load.wait()
    fill_embed(wpad_ref, wg_ref, par_ref[0][0:1])
    wgu_ref[...] = wgu_ref[...] * bf16(0.5)

    def rows_at(j):
        return pl.ds(j * ROWS if isinstance(j, int) else pl.multiple_of(j * ROWS, ROWS), ROWS)

    def embed_step(j, p, entering=True, leaving=(True, True, True)):
        q = 1 - p
        if leaving[1]:
            y_ref[p] = dot(hid_ref[p], wo_ref[0])
        if entering:
            pre_ref[p] = dot(xpad_ref[rows_at(j), :], wpad_ref[...])
        if leaving[0]:
            hid_ref[q] = swish(pre_ref[q])
        if leaving[2]:
            vg_ref[rows_at(j - 3), :] = norm(y_ref[q] + par_ref[0][1:2], par_ref[0]).astype(bf16)

    def update_step(j, p, entering=True, leaving=(True, True, True)):
        q = 1 - p
        if leaving[1]:
            y_ref[2 + p] = dot(hid_ref[2 + p], wo_ref[5])
        if entering:
            vg = vg_ref[rows_at(j), :]
            pre_ref[2 + p] = dot(vg, wgu_ref[...])
            vgt_ref[pl.ds(j * CELL, CELL)] = dot(flip, vg).astype(bf16).reshape(CELL, BATCH, LAT)
        if leaving[0]:
            hid_ref[2 + q] = swish(pre_ref[2 + q] + 0.5 * par_ref[5][0:1])
        if leaving[2]:
            upd = norm(y_ref[2 + q] + par_ref[5][1:2], par_ref[5])
            gout_ref[j - 3] = (vg_ref[rows_at(j - 3), :].astype(f32) + upd).astype(bf16).reshape(BATCH, CELL, LAT)

    def fill(step):
        step(0, 0, True, (False, False, False))
        step(1, 1, True, (True, False, False))
        step(2, 0, True, (True, True, False))

    def drain(step):
        step(CELL, 0, False, (True, True, True))
        step(CELL + 1, 1, False, (False, True, True))
        step(CELL + 2, 0, False, (False, False, True))

    def run(step, first, trips):
        def some(k, carry):
            for u in range(UNROLL):
                step(first + k * UNROLL + u, (first + u) % 2)
            return carry

        lax.fori_loop(0, trips, some, 0)

    fill(embed_step)
    run(embed_step, 3, 12 // UNROLL)
    embed_step(CELL - 1, 1)
    drain(embed_step)
    fill(update_step)
    run(update_step, 3, 4 // UNROLL)
    e_top.wait_recv()
    e_low.wait_recv()
    pl.when(has_up)(fwd_up.start)
    pl.when(has_down)(fwd_down.start)
    run(update_step, 7, 8 // UNROLL)
    update_step(CELL - 1, 1)
    drain(update_step)

    code_ref[...] = slot_lists(send_ref[...], mask_ref[...], lat, lon)
    par = par_ref[1]
    vm = finish(0.5 * (dot_t(mesh_ref[...], wm_ref[...]) + par[0:1]), wo_ref[1], par).astype(bf16)
    vm_ref[...] = vm.astype(f32)
    par = par_ref[2]
    el = finish(0.5 * (jnp.concatenate([dot_t(edge_ref[n], we_ref[...]) for n in range(NODES)], axis=0) + par[0:1]), wo_ref[2], par).astype(bf16)
    par = par_ref[3]
    el_ref[...] = el.astype(f32) + par[3:4]
    vm_proj = dot(vm, wmsg_ref[2 * LAT:]) + par[0:1]
    lp = dot(el, wmsg_ref[:LAT]).reshape(NODES, SLOTS, LAT) + vm_proj[:, None, :]
    lp_ref[...] = 0.5 * lp.reshape(NSLOT, LAT)

    pl.when(at_pole)(polar.wait_recv)

    @pl.when(has_down)
    def _():
        to_up.wait_recv()
        fwd_up.wait_recv()

    @pl.when(has_up)
    def _():
        to_down.wait_recv()
        fwd_down.wait_recv()

    for first, last in ((0, BASE_EDGE + REACH * EDGE_BLK), (BASE_EDGE + (CELL - REACH) * EDGE_BLK, BLOCKS)):
        rx_out_ref[first:last] = rx_ref[first * BATCH:last * BATCH].reshape(last - first, BATCH, LANES)
    e_mid.wait_recv()
    first, last = BASE_EDGE + REACH * EDGE_BLK, BASE_EDGE + (CELL - REACH) * EDGE_BLK
    rx_out_ref[first:last] = rx_ref[first * BATCH:last * BATCH].reshape(last - first, BATCH, LANES)
    e_top.wait_send()
    e_low.wait_send()
    e_mid.wait_send()
    pl.when(at_pole)(polar.wait_send)

    @pl.when(has_up)
    def _():
        to_up.wait_send()
        fwd_up.wait_send()

    @pl.when(has_down)
    def _():
        to_down.wait_send()
        fwd_down.wait_send()


def slot_kernel(lists_ref, vgt_ref, gout_ref, rx_ref, lp_ref, el_ref, vm_ref, wg_ref, wmsg_ref, wnode_ref, wo_ref, par_ref,
                mesh_ref, grid_ref, wpad_ref, wmid_ref, raw_ref, lhs_ref, pre_ref, hid_ref, y_ref, far_vg_ref, acc_ref, base_ref, code_ref, sem):
    fetch = pltpu.make_async_copy(lists_ref, code_ref, sem.at[CELL])
    fetch.start()
    copies = [pltpu.make_async_copy(gout_ref.at[i], grid_ref.at[:, i], sem.at[i]) for i in range(CELL)]
    for copy in copies:
        copy.start()
    fill_embed(wpad_ref, wg_ref, par_ref[0][0:1])
    wmid_ref[...] = wmsg_ref[LAT:2 * LAT] * bf16(0.5)
    acc_ref[...] = jnp.zeros_like(acc_ref)

    vm = vm_ref[...]
    base_ref[...] = dot(vm.astype(bf16), wnode_ref[:LAT]) + par_ref[4][0:1]
    fetch.wait()
    n_all, n_far, n_near = [code_ref[3, LIST - 3 + k] for k in range(3)]

    def block(ref, index):
        return ref[index]

    par = par_ref[3]

    def embed_step(j, p, entering=True, leaving=(True, True, True)):
        q = 1 - p
        if leaving[1]:
            y_ref[2 + p] = dot(hid_ref[2 + p], wo_ref[0])
        if entering:
            for u in range(GROUP):
                halo = code_ref[3, j * GROUP + u]
                lo, hi = halo & 0x1FF, halo >> 16
                dst = slice(u * BATCH, (u + 1) * BATCH)
                raw_ref[p, dst, :LANES] = block(rx_ref, lo)
                high = block(rx_ref, hi & 0x1FF).astype(f32)
                high = jnp.where(hi >= 1 << 9, pltpu.roll(high, HALF, 1), high)
                raw_ref[p, dst, LANES:] = high.astype(bf16)
            pre_ref[2 + p] = dot(raw_ref[p], wpad_ref[...])
        if leaving[0]:
            hid_ref[2 + q] = swish(pre_ref[2 + q])
        if leaving[2]:
            vg = norm(y_ref[2 + q] + par_ref[0][1:2], par_ref[0])
            far_vg_ref[pl.ds((j - 3) * GROUP, GROUP)] = vg.astype(bf16).reshape(GROUP, BATCH, LAT)

    def message_step(j, p, near_only=False, entering=True, leaving=(True, True, True)):
        q = 1 - p
        now, old, oldest = [jnp.maximum(FRONT + (j - k) * GROUP, 0) for k in (0, 1, 3)]
        if leaving[1]:
            y_ref[p] = dot(hid_ref[p], wo_ref[3])
        if entering:
            for u in range(GROUP):
                sender = block(vgt_ref, code_ref[1, now + u])
                if not near_only:
                    far = code_ref[2, now + u]
                    sender = jnp.where(far >= 1 << 9, block(far_vg_ref, far & 0x1FF), sender)
                lhs_ref[p, u * BATCH:(u + 1) * BATCH] = sender
            pre_ref[p] = dot(lhs_ref[p], wmid_ref[...])
        if leaving[0]:
            for u in range(GROUP):
                at = slice(u * BATCH, (u + 1) * BATCH)
                hid_ref[q, at] = swish(pre_ref[q, at] + lp_ref[pl.ds(code_ref[0, old + u] & 0x1FF, 1), :])
        if leaving[2]:
            for u in range(GROUP):
                word = code_ref[0, oldest + u]
                t, node = word & 0x1FF, word >> 16
                upd = scale(y_ref[q, u * BATCH:(u + 1) * BATCH] + par[1:2]) * par[2:3]
                new = (upd + el_ref[pl.ds(t, 1), :]).astype(bf16).astype(f32)
                acc_ref[u % 4, node] = acc_ref[u % 4, node] + new

    embed_steps = jnp.maximum((n_far + 2 * GROUP - 1) // (2 * GROUP) * 2, 4)
    beside = embed_steps + 4
    late = jnp.where(n_far > 0, jnp.maximum(beside - n_near // GROUP, 0), 0)
    groups = (n_all + GROUP - 1) // GROUP + late
    steps = jnp.maximum((groups + 1) // 2 * 2, beside)

    stages = [(False, False, False), (True, False, False), (True, True, False), (True, True, True)]
    for j in range(4):
        message_step(j - late, j % 2, True, True, stages[j])
        embed_step(j, j % 2, True, stages[j])

    def both(k, carry):
        for p in range(2):
            message_step(2 * k + p - late, p, True)
            embed_step(2 * k + p, p)
        return carry

    lax.fori_loop(2, embed_steps // 2, both, 0)
    ends = [(True, True, True), (False, True, True), (False, False, True)]
    for j in range(4):
        message_step(embed_steps + j - late, j % 2, True)
        if j < 3:
            embed_step(embed_steps + j, j % 2, False, ends[j])

    def many(count, start):
        def body(k, carry):
            for u in range(count):
                message_step(start + count * k + u - late, u % 2)
            return carry
        return body

    rest = steps - beside
    fours = rest // 4
    lax.fori_loop(0, fours, many(4, beside), 0)
    lax.fori_loop(0, rest // 2 - 2 * fours, many(2, beside + 4 * fours), 0)
    for j in range(3):
        message_step(steps + j - late, j % 2, False, False, ends[j])

    n_rows = NODES * BATCH
    par = par_ref[4]
    agg = ((acc_ref[0, :NODES] + acc_ref[1, :NODES]) + (acc_ref[2, :NODES] + acc_ref[3, :NODES])).reshape(n_rows, LAT).astype(bf16)
    base = base_ref[...]
    pre = dot(agg, wnode_ref[LAT:]).reshape(NODES, BATCH, LAT) + base[:, None, :]
    upd = finish(0.5 * pre.reshape(n_rows, LAT), wo_ref[4], par)
    out = (upd.reshape(NODES, BATCH, LAT) + vm[:, None, :]).reshape(n_rows, LAT).astype(bf16)
    mesh_ref[...] = dot(flip_matrix(n_rows, BATCH), out).astype(bf16).reshape(BATCH, NODES, LAT)
    for copy in copies:
        copy.wait()


def solution(mesh):
    n_lat, n_lon = mesh.shape['lat'], mesh.shape['lon']

    def cell_step(grid_in, mesh_in, edge_in, senders, edge_mask, w_grid, w_mesh, w_edge, w_msg, w_node, w_gupd, w_out, bias_gain):
        vmem = pl.BlockSpec(memory_space=pltpu.VMEM)
        hbm = pl.BlockSpec(memory_space=pltpu.HBM)
        loaded = [grid_in, mesh_in.T, edge_in.transpose(0, 2, 1), senders, edge_mask, w_grid, w_mesh, w_edge, w_msg, w_gupd, w_out, bias_gain]
        pin = lambda x: pltpu.with_memory_space_constraint(x, pltpu.HBM)
        own = pl.pallas_call(
            functools.partial(own_kernel, n_lat, n_lon),
            name='own',
            out_shape=[
                pltpu.VMEM((CELL * CELL, BATCH, LAT), bf16),
                pltpu.VMEM((CELL, BATCH, CELL, LAT), bf16),
                pltpu.VMEM((BLOCKS, BATCH, LANES), bf16),
                pltpu.VMEM((NSLOT, LAT), f32),
                pltpu.VMEM((NSLOT, LAT), f32),
                pltpu.VMEM((NODES, LAT), f32),
                pltpu.VMEM((4, LIST), i32),
            ],
            in_specs=[hbm] * 12,
            out_specs=[vmem] * 7,
            scratch_shapes=[
                *[pltpu.VMEM(a.shape, a.dtype) for a in loaded],
                pltpu.VMEM((ROWS * CELL, 256), bf16),
                pltpu.VMEM((256, LAT), bf16),
                pltpu.VMEM((4, ROWS, LAT), f32),
                pltpu.VMEM((4, ROWS, LAT), bf16),
                pltpu.VMEM((4, ROWS, LAT), f32),
                pltpu.VMEM((CELL * ROWS, LAT), bf16),
                pltpu.VMEM((BLOCKS * BATCH, LANES), bf16),
                pltpu.VMEM((BLOCKS * BATCH, LANES), bf16),
                pltpu.SemaphoreType.DMA((14,)),
                pltpu.SemaphoreType.DMA((8,)),
                pltpu.SemaphoreType.DMA((8,)),
            ],
            compiler_params=pltpu.CompilerParams(vmem_limit_bytes=28 << 20, collective_id=0, has_side_effects=True),
            cost_estimate=pl.CostEstimate(flops=10 * 10**9, bytes_accessed=16 << 20, transcendentals=0),
        )(*map(pin, loaded))
        vgt, gout, rx, lp, el, vm, code = own

        mesh_out, grid_out = pl.pallas_call(
            slot_kernel,
            name='slots',
            out_shape=[jax.ShapeDtypeStruct((BATCH, NODES, LAT), bf16), jax.ShapeDtypeStruct((BATCH, CELL, CELL, LAT), bf16)],
            in_specs=[vmem] * 12,
            out_specs=[vmem, hbm],
            scratch_shapes=[
                pltpu.VMEM((256, LAT), bf16),
                pltpu.VMEM((LAT, LAT), bf16),
                pltpu.VMEM((2, ROWS, 256), bf16),
                pltpu.VMEM((2, ROWS, LAT), bf16),
                pltpu.VMEM((4, ROWS, LAT), f32),
                pltpu.VMEM((4, ROWS, LAT), bf16),
                pltpu.VMEM((4, ROWS, LAT), f32),
                pltpu.VMEM((NSLOT + 3 * GROUP, BATCH, LAT), bf16),
                pltpu.VMEM((4, NODES + 1, BATCH, LAT), f32),
                pltpu.VMEM((NODES, LAT), f32),
                pltpu.SMEM((4, LIST), i32),
                pltpu.SemaphoreType.DMA((CELL + 1,)),
            ],
            compiler_params=pltpu.CompilerParams(vmem_limit_bytes=24 << 20),
            cost_estimate=pl.CostEstimate(flops=10 * 10**9, bytes_accessed=16 << 20, transcendentals=0),
        )(code, vgt, gout, rx, lp, el, vm, w_grid, w_msg, w_node, w_out, bias_gain)
        return mesh_out, grid_out

    grid_spec = P('dp', 'lat', 'lon', None)
    node_spec = P(('lat', 'lon'), None)
    slot_spec = P(('lat', 'lon'), None, None)
    rep = P()
    in_specs = (grid_spec, node_spec, slot_spec, node_spec, node_spec) + (rep,) * 8
    out_specs = (P('dp', ('lat', 'lon'), None), grid_spec)
    return jax.shard_map(cell_step, mesh=mesh, in_specs=in_specs, out_specs=out_specs, check_vma=False)
```

```python
import functools

import jax
import jax.numpy as jnp
from jax import lax
from jax.experimental import pallas as pl
from jax.experimental.pallas import tpu as pltpu
from jax.sharding import PartitionSpec as P

REACH = 3
LN_EPS = 1e-5
CELL = 16
BATCH = 16
CIN = 186
LAT = 512
HALF = 64
LANES = 128
NODES = 8
SLOTS = 48
NSLOT = NODES * SLOTS
GROUP = 16
ROWS = GROUP * BATCH
EDGE_PTS, POLE_PTS, ROW_PTS = 2 * REACH, CELL - 2 * REACH, CELL
EDGE_BLK, POLE_BLK, ROW_BLK = EDGE_PTS * 3 // 2, POLE_PTS * 3 // 2, ROW_PTS * 3 // 2
BASE_EDGE = 0
BASE_POLE = BASE_EDGE + CELL * EDGE_BLK
BASE_NORTH = BASE_POLE + REACH * POLE_BLK
BASE_SOUTH = BASE_NORTH + REACH * ROW_BLK
BASE_CN = BASE_SOUTH + REACH * ROW_BLK
BASE_CS = BASE_CN + REACH * EDGE_BLK
BLOCKS = BASE_CS + REACH * EDGE_BLK
LIST = 512
FRONT = 3 * GROUP
bf16, f32, i32 = jnp.bfloat16, jnp.float32, jnp.int32
MESH = pl.DeviceIdType.MESH


def dot(a, b):
    return jnp.dot(a, b, preferred_element_type=f32)


def dot_t(a, b):
    return lax.dot_general(a, b, (((0,), (0,)), ((), ())), preferred_element_type=f32)


def swish(h):
    return (h + h * jnp.tanh(h)).astype(bf16)


def scale(y):
    y = y - jnp.mean(y, axis=-1, keepdims=True)
    var = jnp.mean(y * y, axis=-1, keepdims=True)
    return y * lax.rsqrt(var + LN_EPS)


def norm(y, par):
    return scale(y) * par[2:3] + par[3:4]


def finish(half_pre, w2, par):
    return norm(dot(swish(half_pre), w2) + par[1:2], par)


def pack_hi(y):
    half = y.shape[0] // 2
    hi = y[:, LANES:]
    return y[:, :LANES].astype(bf16), (hi[:half] + pltpu.roll(hi[half:], HALF, 1)).astype(bf16)


def fill_embed(wpad_ref, wg_ref, b1):
    tile = CIN // BATCH * BATCH
    wpad_ref[tile:] = jnp.zeros((256 - tile, LAT), bf16)
    wpad_ref[:CIN] = wg_ref[...]
    b_hi = b1.astype(bf16)
    b_mid = (b1 - b_hi.astype(f32)).astype(bf16)
    b_lo = (b1 - b_hi.astype(f32) - b_mid.astype(f32)).astype(bf16)
    row = lax.broadcasted_iota(i32, (BATCH, LAT), 0) + tile
    edge = wpad_ref[tile:tile + BATCH].astype(f32)
    for k, part in enumerate((b_hi, b_mid, b_lo)):
        edge = jnp.where(row == CIN + k, part.astype(f32), edge)
    wpad_ref[tile:tile + BATCH] = edge.astype(bf16)
    wpad_ref[...] = wpad_ref[...] * bf16(0.5)


def slot_lists(senders, live, lat, lon):
    row, col = senders >> 5, senders & 31
    r = row - lat * CELL
    c = col & (CELL - 1)
    own_lon = (col >> 4) == lon
    in_band = (r >= 0) & (r < CELL)
    local = in_band & own_lon
    is_edge = (c < REACH) | (c >= CELL - REACH)
    pole = in_band & jnp.logical_not(is_edge)
    e = jnp.where(c < REACH, c, c - (CELL - EDGE_PTS))
    north = r < 0
    band_base = jnp.where(north, jnp.where(own_lon, BASE_NORTH, BASE_CN), jnp.where(own_lon, BASE_SOUTH, BASE_CS))
    base = jnp.where(in_band, jnp.where(pole, BASE_POLE, BASE_EDGE), band_base)
    pole_line = jnp.where(lat == 0, r, r - (CELL - REACH))
    line = jnp.where(in_band, jnp.where(pole, pole_line, r), jnp.where(north, r + REACH, r - CELL))
    q = jnp.where(pole, c - REACH, jnp.where(own_lon, c, e))
    half = jnp.where(pole, POLE_PTS // 2, jnp.where(own_lon, ROW_PTS // 2, EDGE_PTS // 2))
    start = base + line * (half * 3)
    upper = jnp.where(q >= half, 1, 0)
    lo = start + q
    hi = start + half * 2 + q - upper * half
    n_slots = senders.shape[1]

    def ahead(flag):
        value = flag.astype(f32)
        earlier = lax.broadcasted_iota(i32, (n_slots, n_slots), 0) < lax.broadcasted_iota(i32, (n_slots, n_slots), 1)
        inside = dot(value.astype(bf16), jnp.where(earlier, 1.0, 0.0).astype(bf16))
        total = jnp.broadcast_to(jnp.sum(value, axis=1, keepdims=True), (senders.shape[0], LANES)).astype(bf16)
        earlier = lax.broadcasted_iota(i32, (NODES, NODES), 1) < lax.broadcasted_iota(i32, (NODES, NODES), 0)
        return inside + dot(jnp.where(earlier, 1.0, 0.0).astype(bf16), total)[:, :n_slots]

    active = live == 1
    far = active & jnp.logical_not(local)
    eye = lax.broadcasted_iota(i32, (n_slots, n_slots), 0) == lax.broadcasted_iota(i32, (n_slots, n_slots), 1)
    point = lax.broadcasted_iota(i32, (n_slots, LIST), 1).astype(f32)
    wanted = jnp.where(far, lo, LIST - 1).astype(f32)
    hits = []
    for n in range(NODES):
        column = jnp.sum(jnp.where(eye, wanted[n:n + 1], 0.0), axis=1, keepdims=True)
        hits.append(jnp.where(point == column, 1.0, 0.0))
    used = jnp.sum(functools.reduce(jnp.maximum, hits), axis=0, keepdims=True)
    lanes = lax.broadcasted_iota(i32, (NODES, LIST), 1)
    used = jnp.where((jnp.broadcast_to(used, (NODES, LIST)) > 0) & (lanes < LIST - 1), 1.0, 0.0)
    earlier = lax.broadcasted_iota(i32, (LIST, LIST), 0) < lax.broadcasted_iota(i32, (LIST, LIST), 1)
    rank = dot(used.astype(bf16), jnp.where(earlier, 1.0, 0.0).astype(bf16))[0:1]
    far_at = []
    for hit in hits:
        column = jnp.sum(hit * rank, axis=1, keepdims=True)
        far_at.append(jnp.sum(jnp.where(eye, column, 0.0), axis=0, keepdims=True))
    far_at = jnp.concatenate(far_at, axis=0)
    near = active & local
    n_near = jnp.sum(near.astype(f32))
    all_at = jnp.where(active, jnp.where(local, ahead(near), ahead(far) + n_near) + FRONT, LIST - 1.0)
    to_far = jnp.where(far, far_at, LIST - 1.0)
    slot_id = lax.broadcasted_iota(i32, senders.shape, 1)

    def gather(places, fields):
        total = jnp.zeros((8, LIST), f32)
        for n in range(NODES):
            column = jnp.sum(jnp.where(eye, places[n:n + 1], 0.0), axis=1, keepdims=True)
            rows = [f[n:n + 1].astype(f32) for f in fields]
            rows = jnp.concatenate(rows + [jnp.zeros((8 - len(rows), n_slots), f32)], axis=0).astype(bf16)
            total = total + dot(rows, jnp.where(point == column, 1.0, 0.0).astype(bf16))
        return total

    one = jnp.ones(senders.shape, f32)
    node = lax.broadcasted_iota(i32, senders.shape, 0)
    near_row = jnp.where(local, r * CELL + c, 0)
    got = gather(all_at, [slot_id, node, near_row, jnp.where(far, far_at, 0.0), far.astype(f32), one]).astype(i32)
    lane = lax.broadcasted_iota(i32, (1, LIST), 1)
    valid = (got[5:6] == 1) & (lane < LIST - 1)
    n_all = jnp.sum(active.astype(f32)).astype(i32)
    n_far = jnp.sum(used[0:1]).astype(i32)
    edge_row = jnp.where(valid, got[1:2] * SLOTS + got[0:1], 0) | (jnp.where(valid, got[1:2], NODES) << 16)
    near_block = jnp.where(valid, got[2:3], 0)
    far_block = jnp.where(valid, got[3:4] + (got[4:5] << 9), 0)
    got = gather(to_far, [lo >> 4, lo & 15, hi >> 4, hi & 15, upper, one])
    got = (got / jnp.maximum(got[5:6], 1.0) + 0.5).astype(i32)
    valid = lane < n_far
    halo = jnp.where(valid, (got[0:1] * 16 + got[1:2]) | ((got[2:3] * 16 + got[3:4] + (got[4:5] << 9)) << 16), 0)
    for k, count in enumerate((n_all, n_far, n_near.astype(i32))):
        halo = jnp.where(lane == LIST - 3 + k, count, halo)
    return jnp.concatenate([edge_row, near_block, far_block, halo], axis=0)


def flip_matrix(rows, inner):
    a = lax.broadcasted_iota(i32, (rows, rows), 0)
    b = lax.broadcasted_iota(i32, (rows, rows), 1)
    outer = rows // inner
    return jnp.where(a // outer + a % outer * inner == b, 1.0, 0.0).astype(bf16)


def own_kernel(n_lat, n_lon, x_hbm, mesh_hbm, edge_hbm, send_hbm, mask_hbm, wg_hbm, wm_hbm, we_hbm, wmsg_hbm, wgu_hbm, wo_hbm, par_hbm,
               vgt_ref, gout_ref, rx_out_ref, lp_ref, el_ref, vm_ref, code_ref,
               x_ref, mesh_ref, edge_ref, send_ref, mask_ref, wg_ref, wm_ref, we_ref, wmsg_ref, wgu_ref, wo_ref, par_ref, xpad_ref, wpad_ref, pre_ref, hid_ref, y_ref, vg_ref, tx_ref, rx_ref,
               in_sem, send_sem, recv_sem):
    dp = lax.axis_index('dp')
    lon = lax.axis_index('lon')
    lat = lax.axis_index('lat')
    across = (dp, (lon + 1) % n_lon, lat)
    up = (dp, lon, lat - 1)
    down = (dp, lon, lat + 1)
    has_up = lat > 0
    has_down = lat < n_lat - 1
    at_pole = jnp.logical_or(lat == 0, lat == n_lat - 1)

    loads = [(x_hbm.at[:, :REACH], x_ref.at[:, :REACH]), (x_hbm.at[:, CELL - REACH:], x_ref.at[:, CELL - REACH:]),
             (x_hbm.at[:, REACH:CELL - REACH], x_ref.at[:, REACH:CELL - REACH]), (wg_hbm, wg_ref), (par_hbm, par_ref), (wo_hbm, wo_ref), (wgu_hbm, wgu_ref), (wm_hbm, wm_ref),
             (we_hbm, we_ref), (wmsg_hbm, wmsg_ref), (mesh_hbm, mesh_ref), (edge_hbm, edge_ref), (send_hbm, send_ref), (mask_hbm, mask_ref)]
    loads = [pltpu.make_async_copy(a, b, in_sem.at[k]) for k, (a, b) in enumerate(loads)]
    for load in loads:
        load.start()

    barrier = pltpu.get_barrier_semaphore()
    pl.semaphore_signal(barrier, inc=1, device_id=across, device_id_type=MESH)

    @pl.when(has_up)
    def _():
        pl.semaphore_signal(barrier, inc=1, device_id=up, device_id_type=MESH)

    @pl.when(has_down)
    def _():
        pl.semaphore_signal(barrier, inc=1, device_id=down, device_id_type=MESH)

    def send(k, src_ref, src, dst, count, to):
        return pltpu.make_async_remote_copy(
            src_ref=src_ref.at[pl.ds(src * BATCH, count * BATCH)], dst_ref=rx_ref.at[pl.ds(dst * BATCH, count * BATCH)],
            send_sem=send_sem.at[k], recv_sem=recv_sem.at[k], device_id=to, device_id_type=MESH)

    e_top = send(0, tx_ref, BASE_EDGE, BASE_EDGE, REACH * EDGE_BLK, across)
    e_low = send(1, tx_ref, BASE_EDGE + (CELL - REACH) * EDGE_BLK, BASE_EDGE + (CELL - REACH) * EDGE_BLK, REACH * EDGE_BLK, across)
    e_mid = send(2, tx_ref, BASE_EDGE + REACH * EDGE_BLK, BASE_EDGE + REACH * EDGE_BLK, (CELL - 2 * REACH) * EDGE_BLK, across)
    polar = send(3, tx_ref, BASE_POLE, BASE_POLE, REACH * POLE_BLK, across)
    to_up = send(4, tx_ref, BASE_SOUTH, BASE_SOUTH, REACH * ROW_BLK, up)
    to_down = send(5, tx_ref, BASE_NORTH, BASE_NORTH, REACH * ROW_BLK, down)
    fwd_up = send(6, rx_ref, BASE_EDGE, BASE_CS, REACH * EDGE_BLK, up)
    fwd_down = send(7, rx_ref, BASE_EDGE + (CELL - REACH) * EDGE_BLK, BASE_CN, REACH * EDGE_BLK, down)

    flip = flip_matrix(ROWS, CELL)
    flip_edge = jnp.concatenate([flip[:REACH * BATCH], flip[(CELL - REACH) * BATCH:]], axis=0)
    lane = lax.broadcasted_iota(i32, (ROWS, LANES), 1) + LANES
    ones = jnp.where((lane >= CIN) & (lane < CIN + 3), 1.0, 0.0).astype(bf16)
    loads[0].wait()

    def put(row, lo, hi):
        n = lo.shape[0]
        tx_ref[row * BATCH:row * BATCH + n] = lo
        tx_ref[row * BATCH + n:row * BATCH + n * 3 // 2] = hi

    def pad_row(i):
        at = slice(i * ROWS, (i + 1) * ROWS)
        xpad_ref[at, LANES:] = ones
        xpad_ref[at, :CIN] = x_ref[:, i].reshape(ROWS, CIN)
        return xpad_ref[at, :]

    rows = {i: pad_row(i) for i in range(REACH)}
    for i in range(REACH):
        put(BASE_EDGE + i * EDGE_BLK, *pack_hi(dot(flip_edge, rows[i])))
    pl.semaphore_wait(barrier, 1 + has_up.astype(i32) + has_down.astype(i32))
    e_top.start()
    loads[1].wait()
    for i in range(CELL - REACH, CELL):
        rows[i] = pad_row(i)
        put(BASE_EDGE + i * EDGE_BLK, *pack_hi(dot(flip_edge, rows[i])))
    e_low.start()
    for k in range(REACH):
        inner = []
        for base, first in ((BASE_SOUTH, 0), (BASE_NORTH, CELL - REACH)):
            full = dot(flip, rows[first + k])
            put(base + k * ROW_BLK, *pack_hi(full))
            inner.append(full[REACH * BATCH:(CELL - REACH) * BATCH])
        put(BASE_POLE + k * POLE_BLK, *pack_hi(jnp.where(lat == 0, *inner)))
    pl.when(has_up)(to_up.start)
    pl.when(has_down)(to_down.start)
    pl.when(at_pole)(polar.start)

    loads[2].wait()
    for i in range(REACH, CELL - REACH):
        put(BASE_EDGE + i * EDGE_BLK, *pack_hi(dot(flip_edge, pad_row(i))))
    e_mid.start()

    for load in loads[3:]:
        load.wait()
    fill_embed(wpad_ref, wg_ref, par_ref[0][0:1])
    wgu_ref[...] = wgu_ref[...] * bf16(0.5)

    def rows_at(j):
        return pl.ds(j * ROWS if isinstance(j, int) else pl.multiple_of(j * ROWS, ROWS), ROWS)

    def embed_step(j, p, entering=True, leaving=(True, True, True)):
        q = 1 - p
        if leaving[1]:
            y_ref[p] = dot(hid_ref[p], wo_ref[0])
        if entering:
            pre_ref[p] = dot(xpad_ref[rows_at(j), :], wpad_ref[...])
        if leaving[0]:
            hid_ref[q] = swish(pre_ref[q])
        if leaving[2]:
            vg_ref[rows_at(j - 3), :] = norm(y_ref[q] + par_ref[0][1:2], par_ref[0]).astype(bf16)

    def update_step(j, p, entering=True, leaving=(True, True, True)):
        q = 1 - p
        if leaving[1]:
            y_ref[2 + p] = dot(hid_ref[2 + p], wo_ref[5])
        if entering:
            vg = vg_ref[rows_at(j), :]
            pre_ref[2 + p] = dot(vg, wgu_ref[...])
            vgt_ref[pl.ds(j * CELL, CELL)] = dot(flip, vg).astype(bf16).reshape(CELL, BATCH, LAT)
        if leaving[0]:
            hid_ref[2 + q] = swish(pre_ref[2 + q] + 0.5 * par_ref[5][0:1])
        if leaving[2]:
            upd = norm(y_ref[2 + q] + par_ref[5][1:2], par_ref[5])
            gout_ref[j - 3] = (vg_ref[rows_at(j - 3), :].astype(f32) + upd).astype(bf16).reshape(BATCH, CELL, LAT)

    def fill(step):
        step(0, 0, True, (False, False, False))
        step(1, 1, True, (True, False, False))
        step(2, 0, True, (True, True, False))

    def drain(step):
        step(CELL, 0, False, (True, True, True))
        step(CELL + 1, 1, False, (False, True, True))
        step(CELL + 2, 0, False, (False, False, True))

    def run(step, first, trips, unroll):
        def some(k, carry):
            for u in range(unroll):
                step(first + k * unroll + u, (first + u) % 2)
            return carry

        lax.fori_loop(0, trips, some, 0)

    fill(embed_step)
    run(embed_step, 3, 2, 6)
    embed_step(CELL - 1, 1)
    drain(embed_step)
    fill(update_step)
    run(update_step, 3, 1, 4)
    e_top.wait_recv()
    e_low.wait_recv()
    pl.when(has_up)(fwd_up.start)
    pl.when(has_down)(fwd_down.start)
    run(update_step, 7, 2, 4)
    update_step(CELL - 1, 1)
    drain(update_step)

    code_ref[...] = slot_lists(send_ref[...], mask_ref[...], lat, lon)
    par = par_ref[1]
    vm = finish(0.5 * (dot_t(mesh_ref[...], wm_ref[...]) + par[0:1]), wo_ref[1], par).astype(bf16)
    vm_ref[...] = vm.astype(f32)
    par = par_ref[2]
    el = finish(0.5 * (jnp.concatenate([dot_t(edge_ref[n], we_ref[...]) for n in range(NODES)], axis=0) + par[0:1]), wo_ref[2], par).astype(bf16)
    par = par_ref[3]
    el_ref[...] = el.astype(f32) + par[3:4]
    vm_proj = dot(vm, wmsg_ref[2 * LAT:]) + par[0:1]
    lp = dot(el, wmsg_ref[:LAT]).reshape(NODES, SLOTS, LAT) + vm_proj[:, None, :]
    lp_ref[...] = 0.5 * lp.reshape(NSLOT, LAT)

    pl.when(at_pole)(polar.wait_recv)

    @pl.when(has_down)
    def _():
        to_up.wait_recv()
        fwd_up.wait_recv()

    @pl.when(has_up)
    def _():
        to_down.wait_recv()
        fwd_down.wait_recv()

    for first, last in ((0, BASE_EDGE + REACH * EDGE_BLK), (BASE_EDGE + (CELL - REACH) * EDGE_BLK, BLOCKS)):
        rx_out_ref[first:last] = rx_ref[first * BATCH:last * BATCH].reshape(last - first, BATCH, LANES)
    e_mid.wait_recv()
    first, last = BASE_EDGE + REACH * EDGE_BLK, BASE_EDGE + (CELL - REACH) * EDGE_BLK
    rx_out_ref[first:last] = rx_ref[first * BATCH:last * BATCH].reshape(last - first, BATCH, LANES)
    e_top.wait_send()
    e_low.wait_send()
    e_mid.wait_send()
    pl.when(at_pole)(polar.wait_send)

    @pl.when(has_up)
    def _():
        to_up.wait_send()
        fwd_up.wait_send()

    @pl.when(has_down)
    def _():
        to_down.wait_send()
        fwd_down.wait_send()


def slot_kernel(lists_ref, vgt_ref, gout_ref, rx_ref, lp_ref, el_ref, vm_ref, wg_ref, wmsg_ref, wnode_ref, wo_ref, par_ref,
                mesh_ref, grid_ref, wpad_ref, wmid_ref, raw_ref, lhs_ref, pre_ref, hid_ref, y_ref, far_vg_ref, acc_ref, base_ref, code_ref, sem):
    fetch = pltpu.make_async_copy(lists_ref, code_ref, sem.at[CELL])
    fetch.start()
    copies = [pltpu.make_async_copy(gout_ref.at[i], grid_ref.at[:, i], sem.at[i]) for i in range(CELL)]
    for copy in copies:
        copy.start()
    fill_embed(wpad_ref, wg_ref, par_ref[0][0:1])
    wmid_ref[...] = wmsg_ref[LAT:2 * LAT] * bf16(0.5)
    acc_ref[...] = jnp.zeros_like(acc_ref)

    vm = vm_ref[...]
    base_ref[...] = dot(vm.astype(bf16), wnode_ref[:LAT]) + par_ref[4][0:1]
    fetch.wait()
    n_all, n_far, n_near = [code_ref[3, LIST - 3 + k] for k in range(3)]

    def block(ref, index):
        return ref[index]

    par = par_ref[3]

    def embed_step(j, p, entering=True, leaving=(True, True, True)):
        q = 1 - p
        if leaving[1]:
            y_ref[2 + p] = dot(hid_ref[2 + p], wo_ref[0])
        if entering:
            for u in range(GROUP):
                halo = code_ref[3, j * GROUP + u]
                lo, hi = halo & 0x1FF, halo >> 16
                dst = slice(u * BATCH, (u + 1) * BATCH)
                raw_ref[p, dst, :LANES] = block(rx_ref, lo)
                high = block(rx_ref, hi & 0x1FF).astype(f32)
                high = jnp.where(hi >= 1 << 9, pltpu.roll(high, HALF, 1), high)
                raw_ref[p, dst, LANES:] = high.astype(bf16)
            pre_ref[2 + p] = dot(raw_ref[p], wpad_ref[...])
        if leaving[0]:
            hid_ref[2 + q] = swish(pre_ref[2 + q])
        if leaving[2]:
            vg = norm(y_ref[2 + q] + par_ref[0][1:2], par_ref[0])
            far_vg_ref[pl.ds((j - 3) * GROUP, GROUP)] = vg.astype(bf16).reshape(GROUP, BATCH, LAT)

    def message_step(j, p, near_only=False, entering=True, leaving=(True, True, True)):
        q = 1 - p
        now, old, oldest = [jnp.maximum(FRONT + (j - k) * GROUP, 0) for k in (0, 1, 3)]
        if leaving[1]:
            y_ref[p] = dot(hid_ref[p], wo_ref[3])
        if entering:
            for u in range(GROUP):
                sender = block(vgt_ref, code_ref[1, now + u])
                if not near_only:
                    far = code_ref[2, now + u]
                    sender = jnp.where(far >= 1 << 9, block(far_vg_ref, far & 0x1FF), sender)
                lhs_ref[p, u * BATCH:(u + 1) * BATCH] = sender
            pre_ref[p] = dot(lhs_ref[p], wmid_ref[...])
        if leaving[0]:
            for u in range(GROUP):
                at = slice(u * BATCH, (u + 1) * BATCH)
                hid_ref[q, at] = swish(pre_ref[q, at] + lp_ref[pl.ds(code_ref[0, old + u] & 0x1FF, 1), :])
        if leaving[2]:
            for u in range(GROUP):
                word = code_ref[0, oldest + u]
                t, node = word & 0x1FF, word >> 16
                upd = scale(y_ref[q, u * BATCH:(u + 1) * BATCH] + par[1:2]) * par[2:3]
                new = (upd + el_ref[pl.ds(t, 1), :]).astype(bf16).astype(f32)
                acc_ref[u % 4, node] = acc_ref[u % 4, node] + new

    embed_steps = jnp.maximum((n_far + 2 * GROUP - 1) // (2 * GROUP) * 2, 4)
    beside = embed_steps + 4
    late = jnp.where(n_far > 0, jnp.maximum(beside - n_near // GROUP, 0), 0)
    groups = (n_all + GROUP - 1) // GROUP + late
    steps = jnp.maximum((groups + 1) // 2 * 2, beside)

    stages = [(False, False, False), (True, False, False), (True, True, False), (True, True, True)]
    for j in range(4):
        message_step(j - late, j % 2, True, True, stages[j])
        embed_step(j, j % 2, True, stages[j])

    def both(k, carry):
        for p in range(2):
            message_step(2 * k + p - late, p, True)
            embed_step(2 * k + p, p)
        return carry

    lax.fori_loop(2, embed_steps // 2, both, 0)
    ends = [(True, True, True), (False, True, True), (False, False, True)]
    for j in range(4):
        message_step(embed_steps + j - late, j % 2, True)
        if j < 3:
            embed_step(embed_steps + j, j % 2, False, ends[j])

    def many(count, start):
        def body(k, carry):
            for u in range(count):
                message_step(start + count * k + u - late, u % 2)
            return carry
        return body

    rest = steps - beside
    fours = rest // 4
    lax.fori_loop(0, fours, many(4, beside), 0)
    lax.fori_loop(0, rest // 2 - 2 * fours, many(2, beside + 4 * fours), 0)
    for j in range(3):
        message_step(steps + j - late, j % 2, False, False, ends[j])

    n_rows = NODES * BATCH
    par = par_ref[4]
    agg = ((acc_ref[0, :NODES] + acc_ref[1, :NODES]) + (acc_ref[2, :NODES] + acc_ref[3, :NODES])).reshape(n_rows, LAT).astype(bf16)
    base = base_ref[...]
    pre = dot(agg, wnode_ref[LAT:]).reshape(NODES, BATCH, LAT) + base[:, None, :]
    upd = finish(0.5 * pre.reshape(n_rows, LAT), wo_ref[4], par)
    out = (upd.reshape(NODES, BATCH, LAT) + vm[:, None, :]).reshape(n_rows, LAT).astype(bf16)
    mesh_ref[...] = dot(flip_matrix(n_rows, BATCH), out).astype(bf16).reshape(BATCH, NODES, LAT)
    for copy in copies:
        copy.wait()


def solution(mesh):
    n_lat, n_lon = mesh.shape['lat'], mesh.shape['lon']

    def cell_step(grid_in, mesh_in, edge_in, senders, edge_mask, w_grid, w_mesh, w_edge, w_msg, w_node, w_gupd, w_out, bias_gain):
        vmem = pl.BlockSpec(memory_space=pltpu.VMEM)
        hbm = pl.BlockSpec(memory_space=pltpu.HBM)
        loaded = [grid_in, mesh_in.T, edge_in.transpose(0, 2, 1), senders, edge_mask, w_grid, w_mesh, w_edge, w_msg, w_gupd, w_out, bias_gain]
        pin = lambda x: pltpu.with_memory_space_constraint(x, pltpu.HBM)
        own = pl.pallas_call(
            functools.partial(own_kernel, n_lat, n_lon),
            name='own',
            out_shape=[
                pltpu.VMEM((CELL * CELL, BATCH, LAT), bf16),
                pltpu.VMEM((CELL, BATCH, CELL, LAT), bf16),
                pltpu.VMEM((BLOCKS, BATCH, LANES), bf16),
                pltpu.VMEM((NSLOT, LAT), f32),
                pltpu.VMEM((NSLOT, LAT), f32),
                pltpu.VMEM((NODES, LAT), f32),
                pltpu.VMEM((4, LIST), i32),
            ],
            in_specs=[hbm] * 12,
            out_specs=[vmem] * 7,
            scratch_shapes=[
                *[pltpu.VMEM(a.shape, a.dtype) for a in loaded],
                pltpu.VMEM((ROWS * CELL, 256), bf16),
                pltpu.VMEM((256, LAT), bf16),
                pltpu.VMEM((4, ROWS, LAT), f32),
                pltpu.VMEM((4, ROWS, LAT), bf16),
                pltpu.VMEM((4, ROWS, LAT), f32),
                pltpu.VMEM((CELL * ROWS, LAT), bf16),
                pltpu.VMEM((BLOCKS * BATCH, LANES), bf16),
                pltpu.VMEM((BLOCKS * BATCH, LANES), bf16),
                pltpu.SemaphoreType.DMA((14,)),
                pltpu.SemaphoreType.DMA((8,)),
                pltpu.SemaphoreType.DMA((8,)),
            ],
            compiler_params=pltpu.CompilerParams(vmem_limit_bytes=36 << 20, collective_id=0, has_side_effects=True),
            cost_estimate=pl.CostEstimate(flops=10 * 10**9, bytes_accessed=16 << 20, transcendentals=0),
        )(*map(pin, loaded))
        vgt, gout, rx, lp, el, vm, code = own

        mesh_out, grid_out = pl.pallas_call(
            slot_kernel,
            name='slots',
            out_shape=[jax.ShapeDtypeStruct((BATCH, NODES, LAT), bf16), jax.ShapeDtypeStruct((BATCH, CELL, CELL, LAT), bf16)],
            in_specs=[vmem] * 12,
            out_specs=[vmem, hbm],
            scratch_shapes=[
                pltpu.VMEM((256, LAT), bf16),
                pltpu.VMEM((LAT, LAT), bf16),
                pltpu.VMEM((2, ROWS, 256), bf16),
                pltpu.VMEM((2, ROWS, LAT), bf16),
                pltpu.VMEM((4, ROWS, LAT), f32),
                pltpu.VMEM((4, ROWS, LAT), bf16),
                pltpu.VMEM((4, ROWS, LAT), f32),
                pltpu.VMEM((NSLOT + 3 * GROUP, BATCH, LAT), bf16),
                pltpu.VMEM((4, NODES + 1, BATCH, LAT), f32),
                pltpu.VMEM((NODES, LAT), f32),
                pltpu.SMEM((4, LIST), i32),
                pltpu.SemaphoreType.DMA((CELL + 1,)),
            ],
            compiler_params=pltpu.CompilerParams(vmem_limit_bytes=24 << 20),
            cost_estimate=pl.CostEstimate(flops=10 * 10**9, bytes_accessed=16 << 20, transcendentals=0),
        )(code, vgt, gout, rx, lp, el, vm, w_grid, w_msg, w_node, w_out, bias_gain)
        return mesh_out, grid_out

    grid_spec = P('dp', 'lat', 'lon', None)
    node_spec = P(('lat', 'lon'), None)
    slot_spec = P(('lat', 'lon'), None, None)
    rep = P()
    in_specs = (grid_spec, node_spec, slot_spec, node_spec, node_spec) + (rep,) * 8
    out_specs = (P('dp', ('lat', 'lon'), None), grid_spec)
    return jax.shard_map(cell_step, mesh=mesh, in_specs=in_specs, out_specs=out_specs, check_vma=False)
```
